32 devices in a mesh: dp: 4 (over y, z), tp: 8 (over x, core).
Axes of the slice: x: 4, y: 2, z: 2, core: 2. Of those that a mesh axis runs over, the one named last changes fastest.
The devices are a block of a 4x4x8 slice.
Arguments:
- hidden: bfloat16 [4, 2048, 2048], P('dp', 'tp'), parts along dimension 0
- positions: int32 [4, 2048], P('dp'), parts along dimension 0
- norm_w: float32 [2048], replicated
- w_query: bfloat16 [2048, 2048], P(None, 'tp')
- w_key: bfloat16 [2048, 256], replicated
- w_value: bfloat16 [2048, 256], replicated
- w_out: bfloat16 [2048, 2048], P('tp')
- grad_out: bfloat16 [4, 2048, 2048], P('dp', 'tp'), parts along dimension 0
Outputs:
- output 1: bfloat16 [4, 2048, 2048], P('dp', 'tp'), parts along dimension 0
- output 2: bfloat16 [4, 2048, 2048], P('dp', 'tp'), parts along dimension 0
- output 3: float32 [8192, 2048], P('dp', 'tp'), parts along dimension 0
- output 4: float32 [8192, 2048], P(('dp', 'tp')), parts along dimension 0
- output 5: float32 [8192, 256], P('dp'), parts along dimension 0
- output 6: float32 [8192, 256], P('dp'), parts along dimension 0
- output 7: float32 [8192], P('dp'), parts along dimension 0
There are 4 independent parts. The reference program is written for one: setup_inputs(seed, part) draws one part's arguments, and reference() takes and returns one part's arrays. A program takes and returns all parts, laid end to end along the dimension named above; an argument that names none is the same for every part.
All inputs are finite; a program needn't handle non-finite values.
Results may differ from the reference program's by a relative error of at most 0.02.
Values are sent between devices in bfloat16 or wider.
A program may use at most 768 MiB of HBM per device.

```python
import jax
import jax.numpy as jnp
from jax import lax

BATCH = 1
SEQ = 2048
D_MODEL = 2048
HEADS = 8
HEAD = 256


def setup_inputs(seed: int = 0, part: int = 0) -> dict:
    part_key = jax.random.fold_in(jax.random.key(seed), part)
    part_keys = jax.random.split(part_key, 4)
    shared_keys = jax.random.split(jax.random.key(seed + 1), 5)
    width = HEADS * HEAD
    hidden = jax.random.normal(part_keys[0], (BATCH, SEQ, D_MODEL), jnp.float32)
    increments = jax.random.randint(part_keys[1], (BATCH, SEQ), 1, 4, dtype=jnp.int32)
    starts = jax.random.randint(part_keys[2], (BATCH, 1), 0, 64, dtype=jnp.int32)
    positions = jnp.cumsum(increments, axis=1) - increments[:, :1] + starts
    grad_out = jax.random.normal(part_keys[3], (BATCH, SEQ, D_MODEL), jnp.float32)
    norm_w = 0.5 * jax.random.normal(shared_keys[0], (D_MODEL,), jnp.float32)
    w_query = jax.random.normal(shared_keys[1], (D_MODEL, width), jnp.float32) * D_MODEL ** -0.5
    w_key = jax.random.normal(shared_keys[2], (D_MODEL, HEAD), jnp.float32) * D_MODEL ** -0.5
    w_value = jax.random.normal(shared_keys[3], (D_MODEL, HEAD), jnp.float32) * D_MODEL ** -0.5
    out_gain = (SEQ ** 0.5) / 8.0 * width ** -0.5
    w_out = jax.random.normal(shared_keys[4], (width, D_MODEL), jnp.float32) * out_gain
    return {'hidden': hidden.astype(jnp.bfloat16), 'positions': positions.astype(jnp.int32), 'norm_w': norm_w, 'w_query': w_query.astype(jnp.bfloat16), 'w_key': w_key.astype(jnp.bfloat16), 'w_value': w_value.astype(jnp.bfloat16), 'w_out': w_out.astype(jnp.bfloat16), 'grad_out': grad_out.astype(jnp.bfloat16)}


def rope_tables(positions):
    half = HEAD // 2
    inv_freq = 10000.0 ** (-2.0 * jnp.arange(half, dtype=jnp.float32) / HEAD)
    angle = positions.astype(jnp.float32)[..., None] * inv_freq
    return jnp.cos(angle), jnp.sin(angle)


def apply_rope(vector, cos_t, sin_t):
    half = HEAD // 2
    first = vector[..., :half]
    second = vector[..., half:]
    return jnp.concatenate([first * cos_t - second * sin_t, second * cos_t + first * sin_t], axis=-1)


def block_forward(hidden, positions, norm_w, w_query, w_key, w_value, w_out):
    hidden_f = hidden.astype(jnp.float32)
    inv_rms = lax.rsqrt(jnp.mean(hidden_f * hidden_f, axis=-1, keepdims=True) + 1e-6)
    normed_act = (hidden_f * inv_rms * (1.0 + norm_w)).astype(jnp.bfloat16)
    tokens = normed_act.reshape(BATCH * SEQ, D_MODEL)
    query = jnp.dot(tokens, w_query, preferred_element_type=jnp.float32).astype(jnp.bfloat16).reshape(BATCH, SEQ, HEADS, HEAD)
    key_proj = jnp.dot(tokens, w_key, preferred_element_type=jnp.float32).astype(jnp.bfloat16).reshape(BATCH, SEQ, HEAD)
    value_proj = jnp.dot(tokens, w_value, preferred_element_type=jnp.float32).astype(jnp.bfloat16).reshape(BATCH, SEQ, HEAD)
    cos_t, sin_t = rope_tables(positions)
    q_rot = (apply_rope(query.astype(jnp.float32), cos_t[:, :, None], sin_t[:, :, None]) * HEAD ** -0.5).astype(jnp.bfloat16)
    k_rot = apply_rope(key_proj.astype(jnp.float32), cos_t, sin_t).astype(jnp.bfloat16)
    scores = jnp.einsum('bqhd,bkd->bhqk', q_rot.astype(jnp.float32), k_rot.astype(jnp.float32))
    causal = jnp.arange(SEQ)[:, None] >= jnp.arange(SEQ)[None, :]
    attn_probs = jax.nn.softmax(jnp.where(causal, scores, -1e30), axis=-1)
    attended = jnp.einsum('bhqk,bkd->bqhd', attn_probs.astype(jnp.bfloat16).astype(jnp.float32), value_proj.astype(jnp.float32)).astype(jnp.bfloat16)
    projected = jnp.dot(attended.reshape(BATCH * SEQ, HEADS * HEAD), w_out, preferred_element_type=jnp.float32).reshape(BATCH, SEQ, D_MODEL)
    return (hidden_f + projected).astype(jnp.bfloat16)


def reference(hidden, positions, norm_w, w_query, w_key, w_value, w_out, grad_out):
    def bound_forward(hidden_in, norm_in, query_in, key_in, value_in, out_in):
        return block_forward(hidden_in, positions, norm_in, query_in, key_in, value_in, out_in)
    output, pullback = jax.vjp(bound_forward, hidden, norm_w, w_query, w_key, w_value, w_out)
    grad_hidden, grad_norm_w, grad_w_query, grad_w_key, grad_w_value, grad_w_out = pullback(grad_out)
    return (output, grad_hidden.astype(jnp.bfloat16), grad_w_query.astype(jnp.float32), grad_w_out.astype(jnp.float32), grad_w_key.astype(jnp.float32), grad_w_value.astype(jnp.float32), grad_norm_w.astype(jnp.float32))
```

```python
import functools

import jax
import jax.numpy as jnp
from jax import lax
from jax.experimental import pallas as pl
from jax.experimental.pallas import tpu as pltpu
from jax.sharding import PartitionSpec as P

MESH = pl.DeviceIdType.MESH
F32 = jnp.float32
BF16 = jnp.bfloat16
TILE = 512
COLS = 512
VMEM_LIMIT = 63 * 1024 * 1024


def dot_nn(a, b):
    return lax.dot_general(a, b, (((1,), (0,)), ((), ())), preferred_element_type=F32)


def dot_nt(a, b):
    return lax.dot_general(a, b, (((1,), (1,)), ((), ())), preferred_element_type=F32)


def dot_tn(a, b):
    return lax.dot_general(a, b, (((0,), (0,)), ((), ())), preferred_element_type=F32)


def rope(u, cos_t, sin_t):
    half = u.shape[-1] // 2
    first, second = u[:, :half], u[:, half:]
    return jnp.concatenate([first * cos_t - second * sin_t, second * cos_t + first * sin_t], axis=-1)


class Place:
    def __init__(self, size):
        n = size // 2
        self.me = lax.axis_index('tp')
        self.core = lax.rem(self.me, 2)
        self.chip = lax.div(self.me, 2)
        self.chip_r = lax.rem(self.chip + 1, n)
        self.chip_l = lax.rem(self.chip + n - 1, n)
        self.chip_o = lax.rem(self.chip + 2, n)
        self.right = self.chip_r * 2 + self.core
        self.left = self.chip_l * 2 + self.core
        self.sib = self.chip * 2 + 1 - self.core


def remote(src, dst, ssem, rsem, to):
    return pltpu.make_async_remote_copy(src_ref=src, dst_ref=dst, send_sem=ssem, recv_sem=rsem,
                                        device_id={'tp': to}, device_id_type=MESH)


def rows_of(start, size):
    return pl.ds(pl.multiple_of(start, min(size, 128)), size)


class Gather:
    def __init__(self, place, full, block, ssem, rsem):
        self.p, self.full, self.block, self.ssem, self.rsem = place, full, block, ssem, rsem
        p = place
        half = block // 2
        regions = []
        for core in (p.core, 1 - p.core):
            for chip in (p.chip_l, p.chip_r, p.chip_o):
                for h in (0, 1):
                    regions.append(rows_of((chip * 2 + core) * block + h * half, half))
        own_other = rows_of(p.sib * block, block)
        self.regions = regions[:6] + [own_other] + regions[6:]
        self.own = [rows_of(p.me * block + h * half, half) for h in (0, 1)]
        self.own_all = rows_of(p.me * block, block)

    def _send(self, sem, src, rows, rsem, to):
        copy = remote(src, self.full.at[rows], self.ssem.at[sem], self.rsem.at[rsem], to)
        copy.start()

    def start(self, src=None):
        p, half = self.p, self.block // 2
        parts = [self.full.at[r] for r in self.own] if src is None else [src.at[pl.ds(h * half, half)] for h in (0, 1)]
        whole = self.full.at[self.own_all] if src is None else src
        self._send(0, parts[0], self.own[0], 0, p.right)
        self._send(3, parts[1], self.own[1], 3, p.left)
        self._send(1, parts[1], self.own[1], 1, p.right)
        self._send(2, parts[0], self.own[0], 2, p.left)
        self._send(6, whole, self.own_all, 6, p.sib)

    def recv(self, *which):
        for k in which:
            ref = self.full.at[self.regions[k]]
            remote(ref, ref, self.ssem.at[k], self.rsem.at[k], self.p.sib).wait_recv()

    def relay(self):
        self._send(4, self.full.at[self.regions[0]], self.regions[0], 4, self.p.right)
        self._send(5, self.full.at[self.regions[3]], self.regions[3], 5, self.p.left)

    def forward(self, *which):
        for k in which:
            self._send(7 + k, self.full.at[self.regions[k]], self.regions[k], 7 + k, self.p.sib)

    def finish(self):
        for k in range(13):
            ref = self.full.at[self.own_all if k == 6 else self.own[0]]
            remote(ref, ref, self.ssem.at[k], self.rsem.at[k], self.p.sib).wait_send()


class Scatter:
    def __init__(self, place, block, width, tile, dtype, prod, d2d, sums, top, bot, from_l, from_r, ssem, rsem,
                 stage=None, source=None):
        self.__dict__.update(locals())
        self.half = block // 2

    def row(self, chip, core, h=0):
        return (chip * 2 + core) * self.block + h * self.half

    def tiles(self, fn):
        if self.width == self.tile:
            fn(pl.ds(0, self.width))
        else:
            @pl.loop(0, self.width // self.tile)
            def _(n):
                fn(pl.ds(pl.multiple_of(n * self.tile, self.tile), self.tile))

    def chip_send(self):
        p = self.place
        for k, chip in enumerate((p.chip_o, p.chip_r, p.chip_l, p.chip)):
            row = self.row(chip, 1 - p.core)
            if self.source is None:
                slot = k % 2
                if k >= 2:
                    ref = self.stage.at[slot]
                    remote(ref, ref, self.ssem.at[k - 2], self.rsem.at[0], p.sib).wait_send()

                def fill(cols, row=row, slot=slot):
                    self.stage[slot, :, cols] = self.prod(row, self.block, cols).astype(self.dtype)
                self.tiles(fill)
                src = self.stage.at[slot]
            else:
                src = self.source.at[rows_of(row, self.block)]
            remote(src, self.d2d.at[k], self.ssem.at[k], self.rsem.at[k], p.sib).start()

    def chip_recv(self, k):
        ref = self.d2d.at[k]
        remote(ref, ref, self.ssem.at[k], self.rsem.at[k], self.place.sib).wait_recv()

    def far(self):
        p, half = self.place, self.half
        self.chip_recv(0)

        def fill(cols):
            total = self.prod(self.row(p.chip_o, p.core), self.block, cols) + self.d2d[0, :, cols].astype(F32)
            self.sums[0, :, cols] = total.astype(self.dtype)
        self.tiles(fill)
        remote(self.sums.at[0, pl.ds(0, half)], self.top, self.ssem.at[4], self.rsem.at[4], p.right).start()
        remote(self.sums.at[0, pl.ds(half, half)], self.bot, self.ssem.at[5], self.rsem.at[5], p.left).start()

    def near_half(self, k, h, chip, extra, dst, sem, to):
        half = self.half
        rows = pl.ds(h * half, half)

        def fill(cols):
            total = self.prod(self.row(chip, self.place.core, h), half, cols) + self.d2d[k, rows, cols].astype(F32)
            if extra is not None:
                total = total + extra[:, cols].astype(F32)
            self.sums[k, rows, cols] = total.astype(self.dtype)
        self.tiles(fill)
        remote(self.sums.at[k, rows], dst.at[rows], self.ssem.at[sem], self.rsem.at[sem], to).start()

    def near_first(self):
        p = self.place
        self.chip_recv(1)
        self.near_half(1, 1, p.chip_r, None, self.from_l, 6, p.right)
        self.chip_recv(2)
        self.near_half(2, 0, p.chip_l, None, self.from_r, 8, p.left)

    def near_second(self):
        p = self.place
        remote(self.top, self.top, self.ssem.at[4], self.rsem.at[4], p.right).wait_recv()
        self.near_half(1, 0, p.chip_r, self.top, self.from_l, 7, p.right)
        remote(self.bot, self.bot, self.ssem.at[5], self.rsem.at[5], p.left).wait_recv()
        self.near_half(2, 1, p.chip_l, self.bot, self.from_r, 9, p.left)

    def last(self, fn):
        p, half = self.place, self.half
        self.chip_recv(3)
        for sem, ref, h in ((6, self.from_l, 1), (7, self.from_l, 0), (8, self.from_r, 0), (9, self.from_r, 1)):
            part = ref.at[pl.ds(h * half, half)]
            remote(part, part, self.ssem.at[sem], self.rsem.at[sem], p.sib).wait_recv()

        def fill(cols):
            total = self.prod(self.row(p.chip, p.core), self.block, cols) + self.d2d[3, :, cols].astype(F32)
            fn(cols, total + self.from_l[:, cols].astype(F32) + self.from_r[:, cols].astype(F32))
        self.tiles(fill)

    def chip_done(self):
        for k in (range(4) if self.source is not None else (2, 3)):
            ref = self.d2d.at[k]
            remote(ref, ref, self.ssem.at[k], self.rsem.at[k], self.place.sib).wait_send()

    def ring_done(self):
        for k in range(4, 10):
            remote(self.top, self.top, self.ssem.at[k], self.rsem.at[k], self.place.sib).wait_send()


def gather_kernel(size, x_ref, dout_ref, gain_ref, angle_ref, wq_hbm, wk_hbm, wv_hbm,
                  a_out, dout_out, q_ref, k_ref, v_ref, o_ref, lse_ref, cos_ref, sin_ref,
                  a_full, wbuf, s_scr, m_scr, l_scr, acc_scr, lsem, ssem_a, rsem_a, ssem_d, rsem_d):
    p = Place(size)
    block = x_ref.shape[0]
    seq, head = q_ref.shape
    scale = head ** -0.5
    weights = [pltpu.make_async_copy(w, wbuf.at[i], lsem.at[i]) for i, w in enumerate((wq_hbm, wk_hbm, wv_hbm))]
    for w in weights:
        w.start()
    act = Gather(p, a_full, block, ssem_a, rsem_a)
    grad = Gather(p, dout_out, block, ssem_d, rsem_d)
    own_grad = pltpu.make_async_copy(dout_ref, dout_out.at[grad.own_all], lsem.at[3])
    own_grad.start()

    barrier = pltpu.get_barrier_semaphore()
    for peer in (p.left, p.right, p.sib):
        pl.semaphore_signal(barrier, inc=1, device_id={'tp': peer}, device_id_type=MESH)

    @pl.loop(0, block // 64)
    def _(n):
        rows = pl.ds(pl.multiple_of(n * 64, 64), 64)
        x_f = x_ref[rows, :].astype(F32)
        inv = lax.rsqrt(jnp.mean(x_f * x_f, axis=-1, keepdims=True) + 1e-6)
        a_full[rows_of(p.me * block + n * 64, 64), :] = (x_f * inv * gain_ref[...]).astype(BF16)

    pl.semaphore_wait(barrier, 3)
    act.start()

    @pl.loop(0, seq // 64)
    def _(n):
        rows = pl.ds(pl.multiple_of(n * 64, 64), 64)
        angle = angle_ref[rows, :]
        cos_ref[rows, :] = jnp.cos(angle)
        sin_ref[rows, :] = jnp.sin(angle)

    for w in weights:
        w.wait()

    def project(first, second):
        @pl.loop(0, 2)
        def _(n):
            rows = rows_of((first + n * (second - first)) * block, block)
            a = a_full[rows, :]
            cos_t, sin_t = cos_ref[rows, :], sin_ref[rows, :]
            query = dot_nn(a, wbuf[0]).astype(BF16).astype(F32)
            q_ref[rows, :] = (rope(query, cos_t, sin_t) * scale).astype(BF16)
            key = dot_nn(a, wbuf[1]).astype(BF16).astype(F32)
            k_ref[rows, :] = rope(key, cos_t, sin_t).astype(BF16)
            v_ref[rows, :] = dot_nn(a, wbuf[2]).astype(BF16)

    act.recv(6)
    project(p.me, p.sib)
    act.recv(0, 3)
    act.relay()
    grad.start(dout_ref)
    act.forward(0, 3)
    act.recv(1, 2)
    act.forward(1, 2)
    project(p.left, p.right)
    act.recv(7, 8, 9, 10)
    project(p.chip_l * 2 + 1 - p.core, p.chip_r * 2 + 1 - p.core)
    act.recv(4, 5)
    act.forward(4, 5)
    act.recv(11, 12)
    project(p.chip_o * 2 + p.core, p.chip_o * 2 + 1 - p.core)
    a_copy = pltpu.make_async_copy(a_full, a_out, lsem.at[4])
    a_copy.start()
    grad.recv(0, 3)
    grad.relay()
    grad.forward(0, 3)

    row_ids = lax.broadcasted_iota(jnp.int32, (TILE, TILE), 0)
    col_ids = lax.broadcasted_iota(jnp.int32, (TILE, TILE), 1)

    @pl.loop(0, seq // TILE)
    def _(i):
        rows = pl.ds(pl.multiple_of(i * TILE, TILE), TILE)
        m_scr[...] = jnp.full(m_scr.shape, -1e30, F32)
        l_scr[...] = jnp.zeros(l_scr.shape, F32)
        acc_scr[...] = jnp.zeros(acc_scr.shape, F32)

        @pl.loop(0, i + 1)
        def _(j):
            cols = pl.ds(pl.multiple_of(j * TILE, TILE), TILE)
            s = dot_nt(q_ref[rows, :], k_ref[cols, :])
            s = jnp.where(row_ids + (i - j) * TILE >= col_ids, s, -1e30)
            s_scr[j] = s
            m_old = m_scr[:, :1]
            m_new = jnp.maximum(m_old, jnp.max(s, axis=-1, keepdims=True))
            l_new = l_scr[:, :1] * jnp.exp(m_old - m_new) + jnp.sum(jnp.exp(s - m_new), axis=-1, keepdims=True)
            m_scr[...] = jnp.broadcast_to(m_new, m_scr.shape)
            l_scr[...] = jnp.broadcast_to(l_new, l_scr.shape)

        lse = m_scr[...] + jnp.log(l_scr[...])
        lse_ref[rows, :] = lse

        @pl.loop(0, i + 1)
        def _(j):
            cols = pl.ds(pl.multiple_of(j * TILE, TILE), TILE)
            prob = jnp.exp(s_scr[j] - lse_ref[rows, :1]).astype(BF16)
            acc_scr[...] += dot_nn(prob, v_ref[cols, :])

        o_ref[rows, :] = acc_scr[...].astype(BF16)

    grad.recv(1, 2)
    grad.forward(1, 2)
    grad.recv(4, 5)
    grad.forward(4, 5)
    grad.recv(6, 7, 8, 9, 10, 11, 12)
    act.finish()
    grad.finish()
    own_grad.wait()
    a_copy.wait()


def reduce_kernel(size, x_ref, dout_ref, gain_ref, q_ref, k_ref, v_ref, o_ref, lse_ref, cos_ref, sin_ref,
                  wo_ref, wq_ref, wk_ref, wv_ref, a_hbm, grad_hbm,
                  out_ref, dx_ref, dwq_out, dwo_out, dwk_out, dwv_out, dw_ref,
                  big, dq_ref, dkv_ref, dkv_full, dq_acc, stage, sums, d2d_a, top_a, bot_a, fl_a, fr_a,
                  d2d_b, top_b, bot_b, fl_b, fr_b, d2d_c, sums_c, top_c, bot_c, fl_c, fr_c,
                  wide, tiles, dw_me, dw_all, lsem, tsem, ss_a, rs_a, ss_b, rs_b, ss_c, rs_c, ss_g, rs_g, ss_w, rs_w):
    p = Place(size)
    block, width = x_ref.shape
    seq, head = q_ref.shape
    scale = head ** -0.5
    load_grad = pltpu.make_async_copy(grad_hbm, big, lsem.at[0])
    load_grad.start()

    barrier = pltpu.get_barrier_semaphore()
    peers = [lax.rem(p.me + d, size) for d in range(1, size)]
    for peer in peers:
        pl.semaphore_signal(barrier, inc=1, device_id={'tp': peer}, device_id_type=MESH)
    pl.semaphore_wait(barrier, size - 1)

    out_rs = Scatter(p, block, width, COLS, BF16,
                     lambda row, n, cols: dot_nn(o_ref[rows_of(row, n), :], wo_ref[:, cols]),
                     d2d_a, sums, top_a, bot_a, fl_a, fr_a, ss_a, rs_a, stage=stage)
    da_rs = Scatter(p, block, width, COLS, BF16,
                    lambda row, n, cols: dot_nt(dq_ref[rows_of(row, n), :], wq_ref[cols, :]),
                    d2d_b, sums, top_b, bot_b, fl_b, fr_b, ss_b, rs_b, stage=stage)
    kv_rs = Scatter(p, block, 2 * head, 2 * head, F32,
                    lambda row, n, cols: dkv_ref[rows_of(row, n), cols],
                    d2d_c, sums_c, top_c, bot_c, fl_c, fr_c, ss_c, rs_c, source=dkv_ref)
    kv_ag = Gather(p, dkv_full, block, ss_g, rs_g)

    out_rs.chip_send()
    out_rs.far()
    out_rs.near_first()
    out_rs.chip_done()
    dkv_ref[...] = jnp.zeros(dkv_ref.shape, F32)
    load_grad.wait()

    row_ids = lax.broadcasted_iota(jnp.int32, (TILE, TILE), 0)
    col_ids = lax.broadcasted_iota(jnp.int32, (TILE, TILE), 1)

    def backward(lo, hi):
        @pl.loop(lo, hi)
        def _(i):
            rows = pl.ds(pl.multiple_of(i * TILE, TILE), TILE)
            do_f = dot_nt(big[rows, :], wo_ref[...])
            do = do_f.astype(BF16)
            row_dot = jnp.sum(do.astype(F32) * o_ref[rows, :].astype(F32), axis=-1, keepdims=True)
            dq_acc[...] = jnp.zeros(dq_acc.shape, F32)
            q = q_ref[rows, :]

            @pl.loop(0, i + 1)
            def _(j):
                cols = pl.ds(pl.multiple_of(j * TILE, TILE), TILE)
                s = dot_nt(q, k_ref[cols, :])
                prob = jnp.exp(s - lse_ref[rows, :1])
                prob = jnp.where(row_ids + (i - j) * TILE >= col_ids, prob, 0.0)
                dkv_ref[cols, head:] += dot_tn(prob.astype(BF16), do)
                dprob = dot_nt(do, v_ref[cols, :])
                ds = (prob * (dprob - row_dot)).astype(BF16)
                dkv_ref[cols, :head] += dot_tn(ds, q)
                dq_acc[...] += dot_nn(ds, k_ref[cols, :])

            dq_ref[rows, :] = rope(dq_acc[...] * scale, cos_ref[rows, :], -sin_ref[rows, :]).astype(BF16)

    steps = seq // TILE
    backward(0, steps // 2)
    out_rs.near_second()
    backward(steps // 2, steps)

    kv_rs.chip_send()
    da_rs.chip_send()
    kv_rs.far()
    kv_rs.near_first()
    out_rs.ring_done()
    da_rs.far()
    da_rs.near_first()

    @pl.loop(0, width // COLS)
    def _(n):
        cols = pl.ds(pl.multiple_of(n * COLS, COLS), COLS)
        wide[:, cols] = dot_tn(o_ref[...], big[:, cols])
    wo_copy = pltpu.make_async_copy(wide, dwo_out, lsem.at[1])
    wo_copy.start()
    load_act = pltpu.make_async_copy(a_hbm, big, lsem.at[2])
    load_act.start()

    def finish_out(cols, total):
        out_ref[:, cols] = (x_ref[:, cols].astype(F32) + total).astype(BF16)
    out_rs.last(finish_out)

    kv_rs.near_second()
    own = rows_of(p.me * block, block)

    def finish_kv(cols, total):
        dkv_full[own, :head] = rope(total[:, :head], cos_ref[own, :], -sin_ref[own, :]).astype(BF16)
        dkv_full[own, head:] = total[:, head:].astype(BF16)
    kv_rs.last(finish_kv)
    kv_ag.start()
    da_rs.near_second()

    load_act.wait()
    slots = width // COLS

    def weight_grad(lhs, dst, drain):
        @pl.loop(0, slots)
        def _(n):
            if drain:
                pltpu.make_async_copy(tiles.at[n], dst.at[pl.ds(pl.multiple_of(n * COLS, COLS), COLS)], tsem.at[n]).wait()
            cols = pl.ds(pl.multiple_of(n * COLS, COLS), COLS)
            tiles[n] = dot_tn(lhs(), big[:, cols]).T
            pltpu.make_async_copy(tiles.at[n], dst.at[cols], tsem.at[n]).start()

    weight_grad(lambda: dq_ref[...], dwq_out, False)
    kv_ag.recv(0, 3)
    kv_ag.relay()
    kv_ag.forward(0, 3)
    kv_ag.recv(1, 2)
    kv_ag.forward(1, 2)
    kv_ag.recv(4, 5)
    kv_ag.forward(4, 5)
    kv_ag.recv(6, 7, 8, 9, 10, 11, 12)
    weight_grad(lambda: dkv_full[:, :head], dwk_out, True)
    weight_grad(lambda: dkv_full[:, head:], dwv_out, True)

    wo_copy.wait()

    def finish_da(cols, total):
        wide[:, cols] = (total + dot_nt(dkv_full[own, :head], wk_ref[cols, :])
                         + dot_nt(dkv_full[own, head:], wv_ref[cols, :]))
    da_rs.last(finish_da)

    dw_me[...] = jnp.zeros(dw_me.shape, F32)

    @pl.loop(0, block // 32)
    def _(n):
        rows = pl.ds(pl.multiple_of(n * 32, 32), 32)
        x_f = x_ref[rows, :].astype(F32)
        inv = lax.rsqrt(jnp.mean(x_f * x_f, axis=-1, keepdims=True) + 1e-6)
        normed = x_f * inv
        da = wide[rows, :]
        dw_me[...] += jnp.sum(da * normed, axis=0, keepdims=True)
        gn = da * gain_ref[...]
        dx_ref[rows, :] = (dout_ref[rows, :].astype(F32)
                           + inv * (gn - normed * jnp.mean(gn * normed, axis=-1, keepdims=True))).astype(BF16)

    lanes = 128
    for t in range(width // lanes):
        dw_all[0, t:t + 1, :] = dw_me[:, t * lanes:(t + 1) * lanes]
    for d in range(1, size):
        remote(dw_all.at[0], dw_all.at[d], ss_w.at[d], rs_w.at[d], peers[d - 1]).start()
    for d in range(1, size):
        remote(dw_all.at[d], dw_all.at[d], ss_w.at[d], rs_w.at[d], p.sib).wait_recv()
    dw_ref[...] = jnp.sum(dw_all[...], axis=0)

    for d in range(1, size):
        remote(dw_all.at[0], dw_all.at[0], ss_w.at[d], rs_w.at[d], p.sib).wait_send()
    kv_rs.chip_done()
    kv_rs.ring_done()
    da_rs.chip_done()
    da_rs.ring_done()
    kv_ag.finish()
    for n in range(slots):
        pltpu.make_async_copy(tiles.at[n], dwv_out.at[pl.ds(n * COLS, COLS)], tsem.at[n]).wait()


def local_block(size, hidden, positions, norm_w, w_query, w_key, w_value, w_out, grad_out):
    _, block, width = hidden.shape
    seq = positions.shape[1]
    head = w_key.shape[1]
    half = head // 2
    x, dout = hidden[0], grad_out[0]
    gain = (1.0 + norm_w)[None, :]
    inv_freq = 10000.0 ** (-2.0 * jnp.arange(half, dtype=F32) / head)
    angle = positions[0].astype(F32)[:, None] * inv_freq
    vm = pl.BlockSpec(memory_space=pltpu.VMEM)
    hbm = pl.BlockSpec(memory_space=pl.ANY)
    dma = pltpu.SemaphoreType.DMA
    shape = jax.ShapeDtypeStruct
    V = pltpu.VMEM

    a_full, dout_full, q, k, v, o, lse, cos_t, sin_t = pl.pallas_call(
        functools.partial(gather_kernel, size),
        out_shape=[shape((seq, width), BF16)] * 2 + [shape((seq, head), BF16)] * 4
        + [shape((seq, 128), F32), shape((seq, half), F32), shape((seq, half), F32)],
        in_specs=[vm] * 4 + [hbm] * 3,
        out_specs=[hbm] * 2 + [vm] * 7,
        scratch_shapes=[V((seq, width), BF16), V((3, width, head), BF16), V((seq // TILE, TILE, TILE), F32),
                        V((TILE, 128), F32), V((TILE, 128), F32), V((TILE, head), F32),
                        dma((5,)), dma((13,)), dma((13,)), dma((13,)), dma((13,))],
        compiler_params=pltpu.CompilerParams(collective_id=0, has_side_effects=True, vmem_limit_bytes=VMEM_LIMIT),
        name='gather_forward',
    )(x, dout, gain, angle, w_query, w_key, w_value)

    half_block = block // 2

    def ring_bufs(cols, dtype):
        return [V((4, block, cols), dtype), V((half_block, cols), dtype), V((half_block, cols), dtype),
                V((block, cols), dtype), V((block, cols), dtype)]
    kv_bufs = ring_bufs(2 * head, F32)
    out, dx, dwq, dwo, dwk, dwv, dw = pl.pallas_call(
        functools.partial(reduce_kernel, size),
        out_shape=[shape((block, width), BF16)] * 2
        + [shape((width, head), F32), shape((head, width), F32), shape((width, head), F32), shape((width, head), F32),
           shape((width // 128, 128), F32)],
        in_specs=[vm] * 14 + [hbm] * 2,
        out_specs=[vm] * 2 + [hbm] * 4 + [vm],
        scratch_shapes=[V((seq, width), BF16), V((seq, head), BF16), V((seq, 2 * head), F32), V((seq, 2 * head), BF16),
                        V((TILE, head), F32), V((2, block, width), BF16), V((3, block, width), BF16)]
        + ring_bufs(width, BF16) + ring_bufs(width, BF16)
        + [kv_bufs[0], V((3, block, 2 * head), F32)] + kv_bufs[1:]
        + [V((head, width), F32), V((width // COLS, COLS, head), F32), V((1, width), F32), V((size, width // 128, 128), F32),
           dma((3,)), dma((width // COLS,))] + [dma((10,))] * 6 + [dma((13,))] * 2 + [dma((size,))] * 2,
        compiler_params=pltpu.CompilerParams(collective_id=1, has_side_effects=True, vmem_limit_bytes=VMEM_LIMIT),
        name='reduce_backward',
    )(x, dout, gain, q, k, v, o, lse, cos_t, sin_t, w_out, w_query, w_key, w_value, a_full, dout_full)
    return out[None], dx[None], dwq, dwo, dwk, dwv, dw.reshape(width)


def solution(mesh):
    specs_in = (P('dp', 'tp', None), P('dp', None), P(None), P(None, 'tp'), P(None, None), P(None, None), P('tp', None), P('dp', 'tp', None))
    specs_out = (P('dp', 'tp', None), P('dp', 'tp', None), P('dp', 'tp'), P(('dp', 'tp'), None), P('dp', None), P('dp', None), P('dp'))
    return jax.shard_map(functools.partial(local_block, mesh.shape['tp']), mesh=mesh, in_specs=specs_in, out_specs=specs_out, check_vma=False)
```

```python
import functools

import jax
import jax.numpy as jnp
from jax import lax
from jax.experimental import pallas as pl
from jax.experimental.pallas import tpu as pltpu
from jax.sharding import PartitionSpec as P

MESH = pl.DeviceIdType.MESH
F32 = jnp.float32
BF16 = jnp.bfloat16
TILE = 512
COLS = 512
VMEM_LIMIT = 63 * 1024 * 1024


def dot_nn(a, b):
    return lax.dot_general(a, b, (((1,), (0,)), ((), ())), preferred_element_type=F32)


def dot_nt(a, b):
    return lax.dot_general(a, b, (((1,), (1,)), ((), ())), preferred_element_type=F32)


def dot_tn(a, b):
    return lax.dot_general(a, b, (((0,), (0,)), ((), ())), preferred_element_type=F32)


def rope(u, cos_t, sin_t):
    half = u.shape[-1] // 2
    first, second = u[:, :half], u[:, half:]
    return jnp.concatenate([first * cos_t - second * sin_t, second * cos_t + first * sin_t], axis=-1)


class Place:
    def __init__(self, size, stride):
        n = size // 2
        group = lax.axis_index('dp')
        z, y = lax.rem(group, 2), lax.rem(lax.div(group, stride), 2)
        self.group_z = group + 1 - 2 * z
        self.group_y = group + stride * (1 - 2 * y)
        self.part = 2 * y + z
        self.part_z, self.part_y, self.part_d = 2 * y + 1 - z, 2 * (1 - y) + z, 3 - self.part
        self.me = lax.axis_index('tp')
        self.core = lax.rem(self.me, 2)
        self.chip = lax.div(self.me, 2)
        self.chip_r = lax.rem(self.chip + 1, n)
        self.chip_l = lax.rem(self.chip + n - 1, n)
        self.chip_o = lax.rem(self.chip + 2, n)
        self.right = self.chip_r * 2 + self.core
        self.left = self.chip_l * 2 + self.core
        self.sib = self.chip * 2 + 1 - self.core


def remote(src, dst, ssem, rsem, to):
    return pltpu.make_async_remote_copy(src_ref=src, dst_ref=dst, send_sem=ssem, recv_sem=rsem,
                                        device_id={'tp': to}, device_id_type=MESH)


def rows_of(start, size):
    return pl.ds(pl.multiple_of(start, min(size, 128)), size)


class Gather:
    def __init__(self, place, at, ssem, rsem):
        self.at, self.p, self.ssem, self.rsem = at, place, ssem, rsem
        p = place
        self.own = [at(p.chip, p.core, h) for h in (0, 1)]
        self.own_all = at(p.chip, p.core, None)
        regions = []
        for core in (p.core, 1 - p.core):
            for chip in (p.chip_l, p.chip_r, p.chip_o):
                regions += [at(chip, core, 0), at(chip, core, 1)]
        self.regions = regions[:6] + [at(p.chip, 1 - p.core, None)] + regions[6:]

    def _send(self, sem, src, dst, rsem, to):
        remote(src, dst, self.ssem.at[sem], self.rsem.at[rsem], to).start()

    def start(self, parts=None, whole=None):
        p = self.p
        parts = self.own if parts is None else parts
        whole = self.own_all if whole is None else whole
        self._send(0, parts[0], self.own[0], 0, p.right)
        self._send(3, parts[1], self.own[1], 3, p.left)
        self._send(1, parts[1], self.own[1], 1, p.right)
        self._send(2, parts[0], self.own[0], 2, p.left)
        self._send(6, whole, self.own_all, 6, p.sib)

    def recv(self, *which):
        for k in which:
            ref = self.regions[k]
            remote(ref, ref, self.ssem.at[k], self.rsem.at[k], self.p.sib).wait_recv()

    def _forward_only(self, *which):
        for k in which:
            self._send(7 + k, self.regions[k], self.regions[k], 7 + k, self.p.sib)

    def _forward(self, *which):
        self.recv(*which)
        self._forward_only(*which)

    def first(self):
        self.recv(0, 3)
        self._send(4, self.regions[0], self.regions[0], 4, self.p.right)
        self._send(5, self.regions[3], self.regions[3], 5, self.p.left)
        self._forward_only(0, 3)

    def second(self):
        self._forward(1, 2)

    def third(self):
        self._forward(4, 5)

    def sibling(self):
        self.recv(6)

    def sibling_near(self):
        self.recv(7, 8, 9, 10)

    def sibling_far(self):
        self.recv(11, 12)

    def finish(self):
        for k in range(13):
            ref = self.own_all if k == 6 else self.own[0]
            remote(ref, ref, self.ssem.at[k], self.rsem.at[k], self.p.sib).wait_send()


class Share:
    def __init__(self, place, full, rows, ssem, rsem):
        self.p, self.full, self.rows, self.ssem, self.rsem = place, full, rows, ssem, rsem

    def at(self, part, h=None, other=False):
        core = 1 - self.p.core if other else self.p.core
        if h is None:
            return self.full.at[:, core, part]
        return self.full.at[:, core, part, pl.ds(h * self.rows, self.rows)]

    def _send(self, k, ref, **to):
        pltpu.make_async_remote_copy(src_ref=ref, dst_ref=ref, send_sem=self.ssem.at[k], recv_sem=self.rsem.at[k],
                                     device_id=to, device_id_type=MESH).start()

    def _recv(self, k, ref):
        remote(ref, ref, self.ssem.at[k], self.rsem.at[k], self.p.sib).wait_recv()

    def start(self):
        p = self.p
        self._send(0, self.at(p.part), dp=p.group_z)
        self._send(1, self.at(p.part), dp=p.group_y)

    def relay(self):
        p = self.p
        self._recv(0, self.at(p.part_z))
        self._send(2, self.at(p.part_z, 0), dp=p.group_y)
        self._recv(1, self.at(p.part_y))
        self._send(3, self.at(p.part_y, 1), dp=p.group_z)
        self._send(4, self.at(p.part_z), tp=p.sib)
        self._send(5, self.at(p.part_y), tp=p.sib)

    def forward(self):
        p = self.p
        for h in (0, 1):
            self._recv(2 + h, self.at(p.part_d, h))
            self._send(6 + h, self.at(p.part_d, h), tp=p.sib)

    def finish(self):
        p = self.p
        for k, h in enumerate((None, None, 0, 0, None, None, 0, 0)):
            ref = self.at(p.part, h)
            remote(ref, ref, self.ssem.at[k], self.rsem.at[k], p.sib).wait_send()
        self._recv(4, self.at(p.part_z, None, True))
        self._recv(5, self.at(p.part_y, None, True))
        self._recv(6, self.at(p.part_d, 0, True))
        self._recv(7, self.at(p.part_d, 1, True))


class Exchange:
    def __init__(self, place, block, src, dst, relays, ssem, rsem):
        self.p, self.block, self.src, self.dst, self.relays, self.ssem, self.rsem = place, block, src, dst, relays, ssem, rsem

    def _send(self, sem, src, dst, rsem, to):
        remote(src, dst, self.ssem.at[sem], self.rsem.at[rsem], to).start()

    def part(self, chip, core):
        return self.src.at[rows_of((chip * 2 + core) * self.block, self.block)]

    def start(self):
        p = self.p
        slot = self.dst.at[p.me]
        self._send(0, self.part(p.chip_o, 0), self.relays.at[0], 0, p.right)
        self._send(1, self.part(p.chip_o, 1), self.relays.at[1], 1, p.left)
        for core in (0, 1):
            self._send(2 + core, self.part(p.chip_r, core), slot, 2 + p.core, p.chip_r * 2 + core)
            self._send(4 + core, self.part(p.chip_l, core), slot, 4 + p.core, p.chip_l * 2 + core)
        self._send(8, self.part(p.chip, 1 - p.core), slot, 8, p.sib)
        self.dst[p.me] = self.src[rows_of(p.me * self.block, self.block), :]

    def _recv(self, k, ref):
        remote(ref, ref, self.ssem.at[k], self.rsem.at[k], self.p.sib).wait_recv()

    def relay(self):
        p = self.p
        self._recv(0, self.relays.at[0])
        self._send(6, self.relays.at[0], self.dst.at[p.left], 6 + p.core, p.chip_r * 2)
        self._recv(1, self.relays.at[1])
        self._send(7, self.relays.at[1], self.dst.at[p.right], 6 + p.core, p.chip_l * 2 + 1)

    def recv(self):
        p = self.p
        for core in (0, 1):
            self._recv(2 + core, self.dst.at[p.chip_l * 2 + core])
            self._recv(4 + core, self.dst.at[p.chip_r * 2 + core])
            self._recv(6 + core, self.dst.at[p.chip_o * 2 + core])
        self._recv(8, self.dst.at[p.sib])

    def finish(self):
        for k in range(9):
            ref = self.relays.at[0]
            remote(ref, ref, self.ssem.at[k], self.rsem.at[k], self.p.sib).wait_send()


class Scatter:
    def __init__(self, place, block, src, d2d, sums, top, bot, from_l, from_r, ssem, rsem):
        self.__dict__.update(locals())
        self.half = block // 2

    def rows(self, chip, core, h=None):
        row = (chip * 2 + core) * self.block
        return rows_of(row, self.block) if h is None else rows_of(row + h * self.half, self.half)

    def _send(self, k, src, dst, to):
        remote(src, dst, self.ssem.at[k], self.rsem.at[k], to).start()

    def _recv(self, k, ref):
        remote(ref, ref, self.ssem.at[k], self.rsem.at[k], self.place.sib).wait_recv()

    def chip_send(self):
        p = self.place
        for k, chip in enumerate((p.chip_o, p.chip_r, p.chip_l, p.chip)):
            self._send(k, self.src.at[self.rows(chip, 1 - p.core)], self.d2d.at[k], p.sib)

    def far(self):
        p, half = self.place, self.half
        self._recv(0, self.d2d.at[0])
        self.sums[0] = self.src[self.rows(p.chip_o, p.core), :] + self.d2d[0]
        self._send(4, self.sums.at[0, pl.ds(0, half)], self.top, p.right)
        self._send(5, self.sums.at[0, pl.ds(half, half)], self.bot, p.left)

    def near_half(self, k, h, chip, extra, dst, sem, to):
        rows = pl.ds(h * self.half, self.half)
        total = self.src[self.rows(chip, self.place.core, h), :] + self.d2d[k, rows, :]
        self.sums[k, rows, :] = total if extra is None else total + extra[...]
        self._send(sem, self.sums.at[k, rows], dst.at[rows], to)

    def near_first(self):
        p = self.place
        self._recv(1, self.d2d.at[1])
        self.near_half(1, 1, p.chip_r, None, self.from_l, 6, p.right)
        self._recv(2, self.d2d.at[2])
        self.near_half(2, 0, p.chip_l, None, self.from_r, 8, p.left)

    def near_second(self):
        p = self.place
        self._recv(4, self.top)
        self.near_half(1, 0, p.chip_r, self.top, self.from_l, 7, p.right)
        self._recv(5, self.bot)
        self.near_half(2, 1, p.chip_l, self.bot, self.from_r, 9, p.left)

    def last(self):
        p, half = self.place, self.half
        self._recv(3, self.d2d.at[3])
        for k, ref, h in ((6, self.from_l, 1), (7, self.from_l, 0), (8, self.from_r, 0), (9, self.from_r, 1)):
            self._recv(k, ref.at[pl.ds(h * half, half)])
        return self.src[self.rows(p.chip, p.core), :] + self.d2d[3] + self.from_l[...] + self.from_r[...]

    def finish(self):
        for k in range(10):
            ref = self.d2d.at[0] if k < 4 else self.top
            remote(ref, ref, self.ssem.at[k], self.rsem.at[k], self.place.sib).wait_send()


def block_kernel(size, stride, x_ref, dout_ref, gain_ref, angle_ref, wq_hbm, wk_hbm, wv_hbm, wo_hbm,
                 out_ref, dx_ref, dwo_out, dw_ref, a_out, dq_out, dkv_out, wo_full, wq_full,
                 act_full, big, wbuf, wo, wqt, q_ref, k_ref, v_ref, o_ref, dq_ref, dkv_ref, dkv_full, o_all, dq_all,
                 relay_o, relay_q, lse_ref, cos_ref, sin_ref, m_scr, l_scr, acc,
                 d2d, sums, top, bot, from_l, from_r, wide, dw_me, dw_all, lsem,
                 ss_a, rs_a, ss_d, rs_d, ss_wo, rs_wo, ss_wq, rs_wq, ss_kv, rs_kv, ss_yo, rs_yo, ss_yq, rs_yq,
                 ss_o, rs_o, ss_q, rs_q, ss_r, rs_r, ss_w, rs_w):
    p = Place(size, stride)
    block, width = x_ref.shape
    seq, head = q_ref.shape
    chips = size // 2
    half = block // 2
    parts, part_rows = wo.shape[:2]
    scale = head ** -0.5
    wo_rows = lambda: wo[...].reshape(head, width)

    barrier = pltpu.get_barrier_semaphore()
    peers = [lax.rem(p.me + d, size) for d in range(1, size)]
    for to in [{'tp': peer} for peer in peers] + [{'dp': p.group_z}, {'dp': p.group_y}]:
        pl.semaphore_signal(barrier, inc=1, device_id=to, device_id_type=MESH)

    loads = [pltpu.make_async_copy(src, dst, lsem.at[i]) for i, (src, dst) in enumerate(
        ((wq_hbm, wbuf.at[0]), (wo_hbm, wo), (wk_hbm, wbuf.at[1]), (wv_hbm, wbuf.at[2])))]
    for copy in loads:
        copy.start()

    def weight_at(full):
        quarter = part_rows // 2

        def at(chip, core, h):
            if h is None:
                return full.at[chip, core, p.part]
            return full.at[chip, core, p.part, pl.ds(h * quarter, quarter)]
        return at

    def rows_at(full):
        def at(chip, core, h):
            row = (chip * 2 + core) * block
            return full.at[rows_of(row, block) if h is None else rows_of(row + h * half, half)]
        return at

    def grad_at(chip, core, h):
        return big.at[chip, core] if h is None else big.at[chip, core, pl.ds(h * (parts // 2), parts // 2)]

    act = Gather(p, rows_at(act_full), ss_a, rs_a)
    grad = Gather(p, grad_at, ss_d, rs_d)
    wo_g = Gather(p, weight_at(wo_full), ss_wo, rs_wo)
    wq_g = Gather(p, weight_at(wq_full), ss_wq, rs_wq)
    kv_g = Gather(p, rows_at(dkv_full), ss_kv, rs_kv)
    wo_s = Share(p, wo_full, part_rows // 2, ss_yo, rs_yo)
    wq_s = Share(p, wq_full, part_rows // 2, ss_yq, rs_yq)
    o_x = Exchange(p, block, o_ref, o_all, relay_o, ss_o, rs_o)
    dq_x = Exchange(p, block, dq_ref, dq_all, relay_q, ss_q, rs_q)
    kv_r = Scatter(p, block, dkv_ref, d2d, sums, top, bot, from_l, from_r, ss_r, rs_r)

    def start_weight(g, shard, sem):
        quarter = part_rows // 2
        own = pltpu.make_async_copy(shard.at[p.part], g.own_all, lsem.at[sem])
        own.start()
        g.start([shard.at[p.part, pl.ds(h * quarter, quarter)] for h in (0, 1)], shard.at[p.part])
        return own

    loads[1].wait()
    loads[0].wait()
    pl.semaphore_wait(barrier, size + 1)
    own_wo = start_weight(wo_g, wo, 4)

    @pl.loop(0, parts)
    def _(n):
        rows = pl.ds(pl.multiple_of(n * COLS, COLS), COLS)
        flipped = wbuf[0, rows, :].T
        for g in range(parts):
            wqt[g, :, rows] = flipped[g * part_rows:(g + 1) * part_rows, :]
    own_wq = start_weight(wq_g, wqt, 5)

    @pl.loop(0, block // 64)
    def _(n):
        rows = pl.ds(pl.multiple_of(n * 64, 64), 64)
        x_f = x_ref[rows, :].astype(F32)
        inv = lax.rsqrt(jnp.mean(x_f * x_f, axis=-1, keepdims=True) + 1e-6)
        act_full[rows_of(p.me * block + n * 64, 64), :] = (x_f * inv * gain_ref[...]).astype(BF16)

    for g in (wo_g, wq_g):
        g.first()
    act.start()

    @pl.loop(0, seq // 64)
    def _(n):
        rows = pl.ds(pl.multiple_of(n * 64, 64), 64)
        angle = angle_ref[rows, :]
        cos_ref[rows, :] = jnp.cos(angle)
        sin_ref[rows, :] = jnp.sin(angle)

    loads[2].wait()
    loads[3].wait()

    def project(first, second):
        @pl.loop(0, 2)
        def _(n):
            rows = rows_of((first + n * (second - first)) * block, block)
            a = act_full[rows, :]
            cos_t, sin_t = cos_ref[rows, :], sin_ref[rows, :]
            query = dot_nn(a, wbuf[0]).astype(BF16).astype(F32)
            q_ref[rows, :] = (rope(query, cos_t, sin_t) * scale).astype(BF16)
            key = dot_nn(a, wbuf[1]).astype(BF16).astype(F32)
            k_ref[rows, :] = rope(key, cos_t, sin_t).astype(BF16)
            v_ref[rows, :] = dot_nn(a, wbuf[2]).astype(BF16)

    for g, s, own in ((wo_g, wo_s, own_wo), (wq_g, wq_s, own_wq)):
        g.second()
        g.third()
        own.wait()
        s.start()

    act.sibling()
    project(p.me, p.sib)
    act.first()
    grad.start([dout_ref.at[pl.ds(h * (parts // 2), parts // 2)] for h in (0, 1)], dout_ref)
    big[p.chip, p.core] = dout_ref[...]
    act.second()
    project(p.left, p.right)
    act.sibling_near()
    project(p.chip_l * 2 + 1 - p.core, p.chip_r * 2 + 1 - p.core)
    act.third()
    act.sibling_far()
    project(p.chip_o * 2 + p.core, p.chip_o * 2 + 1 - p.core)
    a_copy = pltpu.make_async_copy(act_full, a_out, lsem.at[6])
    a_copy.start()

    row_ids = lax.broadcasted_iota(jnp.int32, (TILE, TILE), 0)
    col_ids = lax.broadcasted_iota(jnp.int32, (TILE, TILE), 1)

    def tile_rows(j):
        return pl.ds(pl.multiple_of(j * TILE, TILE), TILE)

    @pl.loop(0, seq // TILE)
    def _(i):
        rows = tile_rows(i)
        m_scr[...] = jnp.full(m_scr.shape, -1e30, F32)
        l_scr[...] = jnp.zeros(l_scr.shape, F32)
        acc[...] = jnp.zeros(acc.shape, F32)

        @pl.loop(0, i + 1)
        def _(j):
            s = dot_nt(q_ref[rows, :], k_ref[tile_rows(j), :])
            s = jnp.where(row_ids + (i - j) * TILE >= col_ids, s, -1e30)
            dkv_ref[tile_rows(j), :] = s
            m_old = m_scr[:, :1]
            m_new = jnp.maximum(m_old, jnp.max(s, axis=-1, keepdims=True))
            l_new = l_scr[:, :1] * jnp.exp(m_old - m_new) + jnp.sum(jnp.exp(s - m_new), axis=-1, keepdims=True)
            m_scr[...] = jnp.broadcast_to(m_new, m_scr.shape)
            l_scr[...] = jnp.broadcast_to(l_new, l_scr.shape)

        lse_ref[rows, :] = m_scr[...] + jnp.log(l_scr[...])

        @pl.loop(0, i + 1)
        def _(j):
            prob = jnp.exp(dkv_ref[tile_rows(j), :] - lse_ref[rows, :1]).astype(BF16)
            acc[...] += dot_nn(prob, v_ref[tile_rows(j), :])

        o_ref[rows, :] = acc[...].astype(BF16)

    dkv_ref[...] = jnp.zeros(dkv_ref.shape, F32)

    def backward(first, second, count):
        @pl.loop(0, count)
        def _(n):
            i = first + n * (second - first)
            rows = tile_rows(i)
            do = dot_nt(big[i].reshape(TILE, width), wo_rows()).astype(BF16)
            row_dot = jnp.sum(do.astype(F32) * o_ref[rows, :].astype(F32), axis=-1, keepdims=True)
            acc[...] = jnp.zeros(acc.shape, F32)
            q = q_ref[rows, :]

            @pl.loop(0, i + 1)
            def _(j):
                cols = tile_rows(j)
                s = dot_nt(q, k_ref[cols, :])
                prob = jnp.exp(s - lse_ref[rows, :1])
                prob = jnp.where(row_ids + (i - j) * TILE >= col_ids, prob, 0.0)
                dkv_ref[cols, head:] += dot_tn(prob.astype(BF16), do)
                dprob = dot_nt(do, v_ref[cols, :])
                ds = (prob * (dprob - row_dot)).astype(BF16)
                dkv_ref[cols, :head] += dot_tn(ds, q)
                acc[...] += dot_nn(ds, k_ref[cols, :])

            dq_ref[rows, :] = rope(acc[...] * scale, cos_ref[rows, :], -sin_ref[rows, :]).astype(BF16)

    grad.sibling()
    backward(p.chip, p.chip, 1)
    grad.first()
    o_x.start()
    for s in (wo_s, wq_s):
        s.relay()
    grad.second()
    grad.sibling_near()
    backward(p.chip_l, p.chip_r, 2)
    grad.third()
    grad.sibling_far()
    backward(p.chip_o, p.chip_o, 1)
    dq_copy = pltpu.make_async_copy(dq_ref, dq_out, lsem.at[7])
    dq_copy.start()

    kv_r.chip_send()
    o_x.relay()
    kv_r.far()
    kv_r.near_first()
    dq_x.start()
    for s in (wo_s, wq_s):
        s.forward()

    def col_tiles(fn):
        @pl.loop(0, width // COLS)
        def _(n):
            fn(pl.ds(pl.multiple_of(n * COLS, COLS), COLS))

    def big_cols(cols):
        return big[:, :, :, :, cols].reshape(seq, COLS)

    def weight_o(cols):
        wide[:, cols] = dot_tn(o_ref[...], big_cols(cols))
    col_tiles(weight_o)
    wo_copy = pltpu.make_async_copy(wide, dwo_out, lsem.at[1])
    wo_copy.start()

    kv_r.near_second()
    grad.finish()
    wo_g.sibling()
    wo_g.sibling_near()
    wo_g.sibling_far()
    wo_s.finish()
    load_wo = pltpu.make_async_copy(wo_full, big, lsem.at[2])
    load_wo.start()
    dq_x.relay()
    o_x.recv()
    load_wo.wait()

    def finish_out(cols):
        total = dot_nn(jnp.concatenate([o_all[h] for h in range(size)], axis=-1), big_cols(cols))
        out_ref[:, cols] = (x_ref[:, cols].astype(F32) + total).astype(BF16)
    col_tiles(finish_out)

    wq_g.sibling()
    wq_g.sibling_near()
    wq_g.sibling_far()
    wq_s.finish()
    load_wq = pltpu.make_async_copy(wq_full, big, lsem.at[3])
    load_wq.start()

    own = rows_of(p.me * block, block)
    total = kv_r.last()
    dkv_full[own, :head] = rope(total[:, :head], cos_ref[own, :], -sin_ref[own, :]).astype(BF16)
    dkv_full[own, head:] = total[:, head:].astype(BF16)
    kv_g.start()
    dq_x.recv()
    wo_copy.wait()
    load_wq.wait()

    def finish_da(cols):
        total = dot_nn(jnp.concatenate([dq_all[h] for h in range(size)], axis=-1), big_cols(cols))
        wide[:, cols] = (total + dot_nt(dkv_full[own, :head], wbuf[1, cols, :])
                         + dot_nt(dkv_full[own, head:], wbuf[2, cols, :]))
    col_tiles(finish_da)
    kv_g.first()

    dw_me[...] = jnp.zeros(dw_me.shape, F32)
    sub = 32

    @pl.loop(0, block // sub)
    def _(n):
        rows = pl.ds(pl.multiple_of(n * sub, sub), sub)
        x_f = x_ref[rows, :].astype(F32)
        inv = lax.rsqrt(jnp.mean(x_f * x_f, axis=-1, keepdims=True) + 1e-6)
        normed = x_f * inv
        da = wide[rows, :]
        dw_me[...] += jnp.sum(da * normed, axis=0, keepdims=True)
        gn = da * gain_ref[...]
        per = part_rows // sub
        dout = dout_ref[n // per, pl.ds(pl.multiple_of(lax.rem(n, per) * sub, sub), sub), :].astype(F32)
        dx_ref[rows, :] = (dout + inv * (gn - normed * jnp.mean(gn * normed, axis=-1, keepdims=True))).astype(BF16)

    lanes = 128
    for t in range(width // lanes):
        dw_all[0, t:t + 1, :] = dw_me[:, t * lanes:(t + 1) * lanes]
    for d in range(1, size):
        remote(dw_all.at[0], dw_all.at[d], ss_w.at[d], rs_w.at[d], peers[d - 1]).start()
    kv_g.second()
    kv_g.third()
    for d in range(1, size):
        remote(dw_all.at[d], dw_all.at[d], ss_w.at[d], rs_w.at[d], p.sib).wait_recv()
    dw_ref[...] = jnp.sum(dw_all[...], axis=0)
    kv_g.sibling()
    kv_g.sibling_near()
    kv_g.sibling_far()
    kv_copy = pltpu.make_async_copy(dkv_full, dkv_out, lsem.at[2])
    kv_copy.start()

    for d in range(1, size):
        remote(dw_all.at[0], dw_all.at[0], ss_w.at[d], rs_w.at[d], p.sib).wait_send()
    for g in (act, wo_g, wq_g, kv_g, kv_r, o_x, dq_x):
        g.finish()
    a_copy.wait()
    dq_copy.wait()
    kv_copy.wait()


def weight_kernel(a_ref, dq_ref, dkv_ref, dwq_ref, dwk_ref, dwv_ref):
    head = dq_ref.shape[1]
    a = a_ref[...]
    dwq_ref[...] = dot_tn(dq_ref[...], a).T
    dwk_ref[...] = dot_tn(dkv_ref[:, :head], a).T
    dwv_ref[...] = dot_tn(dkv_ref[:, head:], a).T


def local_block(size, stride, hidden, positions, norm_w, w_query, w_key, w_value, w_out, grad_out):
    _, block, width = hidden.shape
    seq = positions.shape[1]
    head = w_key.shape[1]
    half = head // 2
    chips, parts = size // 2, 4
    part_rows = block // parts
    x, dout = hidden[0], grad_out[0].reshape(parts, part_rows, width)
    gain = (1.0 + norm_w)[None, :]
    inv_freq = 10000.0 ** (-2.0 * jnp.arange(half, dtype=F32) / head)
    angle = positions[0].astype(F32)[:, None] * inv_freq
    vm = pl.BlockSpec(memory_space=pltpu.VMEM)
    hbm = pl.BlockSpec(memory_space=pl.ANY)
    dma = pltpu.SemaphoreType.DMA
    shape = jax.ShapeDtypeStruct
    V = pltpu.VMEM
    full = (chips, 2, parts, part_rows, width)
    kv = 2 * head

    out, dx, dwo, dw, act, dq, dkv, _, _ = pl.pallas_call(
        functools.partial(block_kernel, size, stride),
        out_shape=[shape((block, width), BF16)] * 2 + [shape((head, width), F32), shape((width // 128, 128), F32),
                                                       shape((seq, width), BF16), shape((seq, head), BF16),
                                                       shape((seq, kv), BF16), shape(full, BF16), shape(full, BF16)],
        in_specs=[vm] * 4 + [hbm] * 4,
        out_specs=[vm, vm, hbm, vm] + [hbm] * 5,
        scratch_shapes=[V((seq, width), BF16), V(full, BF16), V((3, width, head), BF16), V((parts, part_rows, width), BF16),
                        V((parts, part_rows, width), BF16)] + [V((seq, head), BF16)] * 5
        + [V((seq, kv), F32), V((seq, kv), BF16), V((size, block, head), BF16), V((size, block, head), BF16),
           V((2, block, head), BF16), V((2, block, head), BF16), V((seq, 128), F32), V((seq, half), F32), V((seq, half), F32),
           V((TILE, 128), F32), V((TILE, 128), F32), V((TILE, head), F32),
           V((4, block, kv), F32), V((3, block, kv), F32), V((block // 2, kv), F32), V((block // 2, kv), F32),
           V((block, kv), F32), V((block, kv), F32), V((head, width), F32), V((1, width), F32),
           V((size, width // 128, 128), F32), dma((8,))]
        + [dma((13,))] * 10 + [dma((8,))] * 4 + [dma((9,))] * 4 + [dma((10,))] * 2 + [dma((size,))] * 2,
        compiler_params=pltpu.CompilerParams(collective_id=0, has_side_effects=True, vmem_limit_bytes=VMEM_LIMIT),
        name='attention_block',
    )(x, dout, gain, angle, w_query, w_key, w_value, w_out.reshape(parts, part_rows, width))

    dwq, dwk, dwv = pl.pallas_call(
        weight_kernel,
        grid=(width // COLS,),
        out_shape=[shape((width, head), F32)] * 3,
        in_specs=[pl.BlockSpec((seq, COLS), lambda n: (0, n)), pl.BlockSpec((seq, head), lambda n: (0, 0)),
                  pl.BlockSpec((seq, kv), lambda n: (0, 0))],
        out_specs=[pl.BlockSpec((COLS, head), lambda n: (n, 0))] * 3,
        name='weight_grads',
    )(act, dq, dkv)
    return out[None], dx[None], dwq, dwo, dwk, dwv, dw.reshape(width)


def solution(mesh):
    specs_in = (P('dp', 'tp', None), P('dp', None), P(None), P(None, 'tp'), P(None, None), P(None, None), P('tp', None), P('dp', 'tp', None))
    specs_out = (P('dp', 'tp', None), P('dp', 'tp', None), P('dp', 'tp'), P(('dp', 'tp'), None), P('dp', None), P('dp', None), P('dp'))
    column = [tuple(d.coords) for d in mesh.devices[:, 0]]
    stride = sum(c[1] == column[0][1] for c in column)
    local = functools.partial(local_block, mesh.shape['tp'], stride)
    return jax.shard_map(local, mesh=mesh, in_specs=specs_in, out_specs=specs_out, check_vma=False)
```

```python
import functools

import jax
import jax.numpy as jnp
from jax import lax
from jax.experimental import pallas as pl
from jax.experimental.pallas import tpu as pltpu
from jax.sharding import PartitionSpec as P

MESH = pl.DeviceIdType.MESH
F32 = jnp.float32
BF16 = jnp.bfloat16
TILE = 512
COLS = 512
VMEM_LIMIT = 63 * 1024 * 1024


def dot_nn(a, b):
    return lax.dot_general(a, b, (((1,), (0,)), ((), ())), preferred_element_type=F32)


def dot_nt(a, b):
    return lax.dot_general(a, b, (((1,), (1,)), ((), ())), preferred_element_type=F32)


def dot_tn(a, b):
    return lax.dot_general(a, b, (((0,), (0,)), ((), ())), preferred_element_type=F32)


def rope(u, cos_t, sin_t):
    half = u.shape[-1] // 2
    first, second = u[:, :half], u[:, half:]
    return jnp.concatenate([first * cos_t - second * sin_t, second * cos_t + first * sin_t], axis=-1)


class Place:
    def __init__(self, size, stride):
        n = size // 2
        group = lax.axis_index('dp')
        z, y = lax.rem(group, 2), lax.rem(lax.div(group, stride), 2)
        self.group_z = group + 1 - 2 * z
        self.group_y = group + stride * (1 - 2 * y)
        self.part = 2 * y + z
        self.part_z, self.part_y, self.part_d = 2 * y + 1 - z, 2 * (1 - y) + z, 3 - self.part
        self.me = lax.axis_index('tp')
        self.core = lax.rem(self.me, 2)
        self.chip = lax.div(self.me, 2)
        self.chip_r = lax.rem(self.chip + 1, n)
        self.chip_l = lax.rem(self.chip + n - 1, n)
        self.chip_o = lax.rem(self.chip + 2, n)
        self.right = self.chip_r * 2 + self.core
        self.left = self.chip_l * 2 + self.core
        self.sib = self.chip * 2 + 1 - self.core


def remote(src, dst, ssem, rsem, to):
    return pltpu.make_async_remote_copy(src_ref=src, dst_ref=dst, send_sem=ssem, recv_sem=rsem,
                                        device_id={'tp': to}, device_id_type=MESH)


def rows_of(start, size):
    return pl.ds(pl.multiple_of(start, min(size, 128)), size)


class Gather:
    def __init__(self, place, at, ssem, rsem):
        self.at, self.p, self.ssem, self.rsem = at, place, ssem, rsem
        p = place
        self.own = [at(p.chip, p.core, h) for h in (0, 1)]
        self.own_all = at(p.chip, p.core, None)
        regions = []
        for core in (p.core, 1 - p.core):
            for chip in (p.chip_l, p.chip_r, p.chip_o):
                regions += [at(chip, core, 0), at(chip, core, 1)]
        self.regions = regions[:6] + [at(p.chip, 1 - p.core, None)] + regions[6:]

    def _send(self, sem, src, dst, rsem, to):
        remote(src, dst, self.ssem.at[sem], self.rsem.at[rsem], to).start()

    def start(self, parts=None, whole=None):
        p = self.p
        parts = self.own if parts is None else parts
        whole = self.own_all if whole is None else whole
        self._send(0, parts[0], self.own[0], 0, p.right)
        self._send(3, parts[1], self.own[1], 3, p.left)
        self._send(1, parts[1], self.own[1], 1, p.right)
        self._send(2, parts[0], self.own[0], 2, p.left)
        self._send(6, whole, self.own_all, 6, p.sib)

    def recv(self, *which):
        for k in which:
            ref = self.regions[k]
            remote(ref, ref, self.ssem.at[k], self.rsem.at[k], self.p.sib).wait_recv()

    def _forward_only(self, *which):
        for k in which:
            self._send(7 + k, self.regions[k], self.regions[k], 7 + k, self.p.sib)

    def _forward(self, *which):
        self.recv(*which)
        self._forward_only(*which)

    def first(self):
        self.recv(0, 3)
        self._send(4, self.regions[0], self.regions[0], 4, self.p.right)
        self._send(5, self.regions[3], self.regions[3], 5, self.p.left)
        self._forward_only(0, 3)

    def second(self):
        self._forward(1, 2)

    def third(self):
        self._forward(4, 5)

    def sibling(self):
        self.recv(6)

    def sibling_near(self):
        self.recv(7, 8, 9, 10)

    def sibling_far(self):
        self.recv(11, 12)

    def finish(self):
        for k in range(13):
            ref = self.own_all if k == 6 else self.own[0]
            remote(ref, ref, self.ssem.at[k], self.rsem.at[k], self.p.sib).wait_send()


class Share:
    def __init__(self, place, full, rows, ssem, rsem):
        self.p, self.full, self.rows, self.ssem, self.rsem = place, full, rows, ssem, rsem

    def at(self, part, h=None, other=False):
        core = 1 - self.p.core if other else self.p.core
        if h is None:
            return self.full.at[:, core, part]
        return self.full.at[:, core, part, pl.ds(h * self.rows, self.rows)]

    def _send(self, k, ref, **to):
        pltpu.make_async_remote_copy(src_ref=ref, dst_ref=ref, send_sem=self.ssem.at[k], recv_sem=self.rsem.at[k],
                                     device_id=to, device_id_type=MESH).start()

    def _recv(self, k, ref):
        remote(ref, ref, self.ssem.at[k], self.rsem.at[k], self.p.sib).wait_recv()

    def start(self):
        p = self.p
        self._send(0, self.at(p.part), dp=p.group_z)
        self._send(1, self.at(p.part), dp=p.group_y)

    def relay(self):
        p = self.p
        self._recv(0, self.at(p.part_z))
        self._send(2, self.at(p.part_z, 0), dp=p.group_y)
        self._recv(1, self.at(p.part_y))
        self._send(3, self.at(p.part_y, 1), dp=p.group_z)
        self._send(4, self.at(p.part_z), tp=p.sib)
        self._send(5, self.at(p.part_y), tp=p.sib)

    def forward(self):
        p = self.p
        for h in (0, 1):
            self._recv(2 + h, self.at(p.part_d, h))
            self._send(6 + h, self.at(p.part_d, h), tp=p.sib)

    def finish(self):
        p = self.p
        for k, h in enumerate((None, None, 0, 0, None, None, 0, 0)):
            ref = self.at(p.part, h)
            remote(ref, ref, self.ssem.at[k], self.rsem.at[k], p.sib).wait_send()
        self._recv(4, self.at(p.part_z, None, True))
        self._recv(5, self.at(p.part_y, None, True))
        self._recv(6, self.at(p.part_d, 0, True))
        self._recv(7, self.at(p.part_d, 1, True))


class Exchange:
    def __init__(self, place, block, src, dst, relays, ssem, rsem):
        self.p, self.block, self.src, self.dst, self.relays, self.ssem, self.rsem = place, block, src, dst, relays, ssem, rsem

    def _send(self, sem, src, dst, rsem, to):
        remote(src, dst, self.ssem.at[sem], self.rsem.at[rsem], to).start()

    def part(self, chip, core):
        return self.src.at[rows_of((chip * 2 + core) * self.block, self.block)]

    def start(self):
        p = self.p
        slot = self.dst.at[p.me]
        self._send(0, self.part(p.chip_o, 0), self.relays.at[0], 0, p.right)
        self._send(1, self.part(p.chip_o, 1), self.relays.at[1], 1, p.left)
        for core in (0, 1):
            self._send(2 + core, self.part(p.chip_r, core), slot, 2 + p.core, p.chip_r * 2 + core)
            self._send(4 + core, self.part(p.chip_l, core), slot, 4 + p.core, p.chip_l * 2 + core)
        self._send(8, self.part(p.chip, 1 - p.core), slot, 8, p.sib)
        self.dst[p.me] = self.src[rows_of(p.me * self.block, self.block), :]

    def _recv(self, k, ref):
        remote(ref, ref, self.ssem.at[k], self.rsem.at[k], self.p.sib).wait_recv()

    def relay(self):
        p = self.p
        self._recv(0, self.relays.at[0])
        self._send(6, self.relays.at[0], self.dst.at[p.left], 6 + p.core, p.chip_r * 2)
        self._recv(1, self.relays.at[1])
        self._send(7, self.relays.at[1], self.dst.at[p.right], 6 + p.core, p.chip_l * 2 + 1)

    def recv(self):
        p = self.p
        for core in (0, 1):
            self._recv(2 + core, self.dst.at[p.chip_l * 2 + core])
            self._recv(4 + core, self.dst.at[p.chip_r * 2 + core])
            self._recv(6 + core, self.dst.at[p.chip_o * 2 + core])
        self._recv(8, self.dst.at[p.sib])

    def finish(self):
        for k in range(9):
            ref = self.relays.at[0]
            remote(ref, ref, self.ssem.at[k], self.rsem.at[k], self.p.sib).wait_send()


class Scatter:
    def __init__(self, place, block, src, d2d, sums, top, bot, from_l, from_r, ssem, rsem):
        self.__dict__.update(locals())
        self.half = block // 2

    def rows(self, chip, core, h=None):
        row = (chip * 2 + core) * self.block
        return rows_of(row, self.block) if h is None else rows_of(row + h * self.half, self.half)

    def _send(self, k, src, dst, to):
        remote(src, dst, self.ssem.at[k], self.rsem.at[k], to).start()

    def _recv(self, k, ref):
        remote(ref, ref, self.ssem.at[k], self.rsem.at[k], self.place.sib).wait_recv()

    def chip_send(self):
        p = self.place
        for k, chip in enumerate((p.chip_o, p.chip_r, p.chip_l, p.chip)):
            self._send(k, self.src.at[self.rows(chip, 1 - p.core)], self.d2d.at[k], p.sib)

    def far(self):
        p, half = self.place, self.half
        self._recv(0, self.d2d.at[0])
        self.sums[0] = self.src[self.rows(p.chip_o, p.core), :] + self.d2d[0]
        self._send(4, self.sums.at[0, pl.ds(0, half)], self.top, p.right)
        self._send(5, self.sums.at[0, pl.ds(half, half)], self.bot, p.left)

    def near_half(self, k, h, chip, extra, dst, sem, to):
        rows = pl.ds(h * self.half, self.half)
        total = self.src[self.rows(chip, self.place.core, h), :] + self.d2d[k, rows, :]
        self.sums[k, rows, :] = total if extra is None else total + extra[...]
        self._send(sem, self.sums.at[k, rows], dst.at[rows], to)

    def near_first(self):
        p = self.place
        self._recv(1, self.d2d.at[1])
        self.near_half(1, 1, p.chip_r, None, self.from_l, 6, p.right)
        self._recv(2, self.d2d.at[2])
        self.near_half(2, 0, p.chip_l, None, self.from_r, 8, p.left)

    def near_second(self):
        p = self.place
        self._recv(4, self.top)
        self.near_half(1, 0, p.chip_r, self.top, self.from_l, 7, p.right)
        self._recv(5, self.bot)
        self.near_half(2, 1, p.chip_l, self.bot, self.from_r, 9, p.left)

    def last(self):
        p, half = self.place, self.half
        self._recv(3, self.d2d.at[3])
        for k, ref, h in ((6, self.from_l, 1), (7, self.from_l, 0), (8, self.from_r, 0), (9, self.from_r, 1)):
            self._recv(k, ref.at[pl.ds(h * half, half)])
        return self.src[self.rows(p.chip, p.core), :] + self.d2d[3] + self.from_l[...] + self.from_r[...]

    def finish(self):
        for k in range(10):
            ref = self.d2d.at[0] if k < 4 else self.top
            remote(ref, ref, self.ssem.at[k], self.rsem.at[k], self.place.sib).wait_send()


def block_kernel(size, stride, norm_ref, pos_ref, freq_ref, x_hbm, dout_hbm, wq_hbm, wk_hbm, wv_hbm, wo_hbm,
                 out_ref, dx_ref, dwo_out, dw_ref, a_out, dq_out, dkv_out, wo_full, wq_full,
                 x_ref, dout_ref, gain_ref, act_full, big, wbuf, wo, wqt, q_ref, k_ref, v_ref, o_ref, dq_ref, dkv_ref, dkv_full, o_all, dq_all,
                 relay_o, relay_q, lse_ref, cos_ref, sin_ref, m_scr, l_scr, acc,
                 d2d, sums, top, bot, from_l, from_r, wide, dw_me, dw_all, lsem,
                 ss_a, rs_a, ss_d, rs_d, ss_wo, rs_wo, ss_wq, rs_wq, ss_kv, rs_kv, ss_yo, rs_yo, ss_yq, rs_yq,
                 ss_o, rs_o, ss_q, rs_q, ss_r, rs_r, ss_w, rs_w):
    p = Place(size, stride)
    block, width = x_ref.shape
    seq, head = q_ref.shape
    chips = size // 2
    half = block // 2
    parts, part_rows = wo.shape[:2]
    scale = head ** -0.5
    wo_rows = lambda: wo[...].reshape(head, width)

    barrier = pltpu.get_barrier_semaphore()
    peers = [lax.rem(p.me + d, size) for d in range(1, size)]
    for to in [{'tp': peer} for peer in peers] + [{'dp': p.group_z}, {'dp': p.group_y}]:
        pl.semaphore_signal(barrier, inc=1, device_id=to, device_id_type=MESH)

    load_x, load_wq, load_wo, load_dout, *load_kv = [pltpu.make_async_copy(src, dst, lsem.at[i]) for i, (src, dst) in enumerate(
        ((x_hbm, x_ref), (wq_hbm, wbuf.at[0]), (wo_hbm, wo), (dout_hbm, dout_ref), (wk_hbm, wbuf.at[1]), (wv_hbm, wbuf.at[2])))]
    for copy in (load_x, load_wq, load_wo, load_dout, *load_kv):
        copy.start()
    lanes = 128
    groups = [slice(t * lanes, (t + 1) * lanes) for t in range(width // lanes)]
    for t, cols in enumerate(groups):
        gain_ref[:, cols] = 1.0 + norm_ref[t:t + 1, :]

    def weight_at(full):
        quarter = part_rows // 2

        def at(chip, core, h):
            if h is None:
                return full.at[chip, core, p.part]
            return full.at[chip, core, p.part, pl.ds(h * quarter, quarter)]
        return at

    def rows_at(full):
        def at(chip, core, h):
            row = (chip * 2 + core) * block
            return full.at[rows_of(row, block) if h is None else rows_of(row + h * half, half)]
        return at

    def grad_at(chip, core, h):
        return big.at[chip, core] if h is None else big.at[chip, core, pl.ds(h * (parts // 2), parts // 2)]

    act = Gather(p, rows_at(act_full), ss_a, rs_a)
    grad = Gather(p, grad_at, ss_d, rs_d)
    wo_g = Gather(p, weight_at(wo_full), ss_wo, rs_wo)
    wq_g = Gather(p, weight_at(wq_full), ss_wq, rs_wq)
    kv_g = Gather(p, rows_at(dkv_full), ss_kv, rs_kv)
    wo_s = Share(p, wo_full, part_rows // 2, ss_yo, rs_yo)
    wq_s = Share(p, wq_full, part_rows // 2, ss_yq, rs_yq)
    o_x = Exchange(p, block, o_ref, o_all, relay_o, ss_o, rs_o)
    dq_x = Exchange(p, block, dq_ref, dq_all, relay_q, ss_q, rs_q)
    kv_r = Scatter(p, block, dkv_ref, d2d, sums, top, bot, from_l, from_r, ss_r, rs_r)

    def start_weight(g, shard, src, sem):
        quarter = part_rows // 2
        g.start([src.at[p.part, pl.ds(h * quarter, quarter)] for h in (0, 1)], src.at[p.part])
        own = pltpu.make_async_copy(shard.at[p.part], g.own_all, lsem.at[sem])
        own.start()
        return own

    pl.semaphore_wait(barrier, size + 1)
    load_wo.wait()
    own_wo = start_weight(wo_g, wo, wo_hbm, 6)
    load_wq.wait()

    @pl.loop(0, width // COLS)
    def _(n):
        rows = pl.ds(pl.multiple_of(n * COLS, COLS), COLS)
        flipped = wbuf[0, rows, :].T
        for g in range(parts):
            wqt[g, :, rows] = flipped[g * part_rows:(g + 1) * part_rows, :]
    own_wq = start_weight(wq_g, wqt, wqt, 7)

    load_x.wait()

    @pl.loop(0, block // 64)
    def _(n):
        rows = pl.ds(pl.multiple_of(n * 64, 64), 64)
        x_f = x_ref[rows, :].astype(F32)
        inv = lax.rsqrt(jnp.mean(x_f * x_f, axis=-1, keepdims=True) + 1e-6)
        act_full[rows_of(p.me * block + n * 64, 64), :] = (x_f * inv * gain_ref[...]).astype(BF16)

    for g in (wo_g, wq_g):
        g.first()
    act.start()

    @pl.loop(0, seq // lanes)
    def _(n):
        rows = pl.ds(pl.multiple_of(n * lanes, lanes), lanes)
        angle = jnp.broadcast_to(pos_ref[:, rows].astype(F32), (lanes, lanes)).T * freq_ref[...]
        cos_ref[rows, :] = jnp.cos(angle)
        sin_ref[rows, :] = jnp.sin(angle)

    load_dout.wait()
    big[p.chip, p.core] = dout_ref[...]
    for copy in load_kv:
        copy.wait()

    def project(first, second):
        @pl.loop(0, 2)
        def _(n):
            rows = rows_of((first + n * (second - first)) * block, block)
            a = act_full[rows, :]
            cos_t, sin_t = cos_ref[rows, :], sin_ref[rows, :]
            query = dot_nn(a, wbuf[0]).astype(BF16).astype(F32)
            q_ref[rows, :] = (rope(query, cos_t, sin_t) * scale).astype(BF16)
            key = dot_nn(a, wbuf[1]).astype(BF16).astype(F32)
            k_ref[rows, :] = rope(key, cos_t, sin_t).astype(BF16)
            v_ref[rows, :] = dot_nn(a, wbuf[2]).astype(BF16)

    for g, s, own in ((wo_g, wo_s, own_wo), (wq_g, wq_s, own_wq)):
        g.second()
        g.third()
        own.wait()
        s.start()

    act.sibling()
    project(p.me, p.sib)
    act.first()
    grad.start([dout_ref.at[pl.ds(h * (parts // 2), parts // 2)] for h in (0, 1)], dout_ref)
    act.second()
    project(p.left, p.right)
    act.sibling_near()
    project(p.chip_l * 2 + 1 - p.core, p.chip_r * 2 + 1 - p.core)
    act.third()
    act.sibling_far()
    project(p.chip_o * 2 + p.core, p.chip_o * 2 + 1 - p.core)
    a_copy = pltpu.make_async_copy(act_full, a_out, lsem.at[8])
    a_copy.start()

    row_ids = lax.broadcasted_iota(jnp.int32, (TILE, TILE), 0)
    col_ids = lax.broadcasted_iota(jnp.int32, (TILE, TILE), 1)

    def tile_rows(j):
        return pl.ds(pl.multiple_of(j * TILE, TILE), TILE)

    def lane_groups(v):
        return [v[:, t * lanes:(t + 1) * lanes] for t in range(TILE // lanes)]

    def spread(v):
        return jnp.concatenate([v] * (TILE // lanes), axis=-1)

    diagonal = row_ids >= col_ids

    @pl.loop(0, seq // TILE)
    def _(i):
        rows = tile_rows(i)
        m_scr[...] = jnp.full(m_scr.shape, -1e30, F32)

        def score(j, s):
            dkv_ref[tile_rows(j), :] = s
            m_scr[...] = functools.reduce(jnp.maximum, lane_groups(s), m_scr[...])

        @pl.loop(0, i)
        def _(j):
            score(j, dot_nt(q_ref[rows, :], k_ref[tile_rows(j), :]))

        score(i, jnp.where(diagonal, dot_nt(q_ref[rows, :], k_ref[rows, :]), -1e30))
        m_scr[...] = jnp.broadcast_to(jnp.max(m_scr[...], axis=-1, keepdims=True), m_scr.shape)
        l_scr[...] = jnp.zeros(l_scr.shape, F32)
        acc[...] = jnp.zeros(acc.shape, F32)

        @pl.loop(0, i + 1)
        def _(j):
            prob = jnp.exp(dkv_ref[tile_rows(j), :] - spread(m_scr[...]))
            l_scr[...] = functools.reduce(jnp.add, lane_groups(prob), l_scr[...])
            acc[...] += dot_nn(prob.astype(BF16), v_ref[tile_rows(j), :])

        total = jnp.sum(l_scr[...], axis=-1, keepdims=True)
        lse_ref[rows, :] = m_scr[...] + jnp.log(total)
        o_ref[rows, :] = (acc[...] / total).astype(BF16)

    dkv_ref[...] = jnp.zeros(dkv_ref.shape, F32)

    def backward(first, second, count):
        @pl.loop(0, count)
        def _(n):
            i = first + n * (second - first)
            rows = tile_rows(i)
            do = dot_nt(big[i].reshape(TILE, width), wo_rows()).astype(BF16)
            row_dot = jnp.sum(do.astype(F32) * o_ref[rows, :].astype(F32), axis=-1, keepdims=True)
            m_scr[...] = jnp.broadcast_to(row_dot, m_scr.shape)
            acc[...] = jnp.zeros(acc.shape, F32)
            q = q_ref[rows, :]

            def inner(j, masked):
                cols = tile_rows(j)
                prob = jnp.exp(dot_nt(q, k_ref[cols, :]) - spread(lse_ref[rows, :]))
                if masked:
                    prob = jnp.where(diagonal, prob, 0.0)
                dkv_ref[cols, head:] += dot_tn(prob.astype(BF16), do)
                ds = (prob * (dot_nt(do, v_ref[cols, :]) - spread(m_scr[...]))).astype(BF16)
                dkv_ref[cols, :head] += dot_tn(ds, q)
                acc[...] += dot_nn(ds, k_ref[cols, :])

            @pl.loop(0, i)
            def _(j):
                inner(j, False)
            inner(i, True)

            dq_ref[rows, :] = rope(acc[...] * scale, cos_ref[rows, :], -sin_ref[rows, :]).astype(BF16)

    grad.sibling()
    backward(p.chip, p.chip, 1)
    grad.first()
    o_x.start()
    for s in (wo_s, wq_s):
        s.relay()
    grad.second()
    grad.sibling_near()
    backward(p.chip_l, p.chip_r, 2)
    grad.third()
    grad.sibling_far()
    backward(p.chip_o, p.chip_o, 1)
    dq_copy = pltpu.make_async_copy(dq_ref, dq_out, lsem.at[9])
    dq_copy.start()

    kv_r.chip_send()
    o_x.relay()
    kv_r.far()
    kv_r.near_first()
    for s in (wo_s, wq_s):
        s.forward()

    def col_tiles(fn):
        @pl.loop(0, width // COLS)
        def _(n):
            fn(pl.ds(pl.multiple_of(n * COLS, COLS), COLS))

    def big_cols(cols):
        return big[:, :, :, :, cols].reshape(seq, COLS)

    def weight_o(cols):
        wide[:, cols] = dot_tn(o_ref[...], big_cols(cols))
    col_tiles(weight_o)
    wo_copy = pltpu.make_async_copy(wide, dwo_out, lsem.at[1])
    wo_copy.start()

    kv_r.near_second()
    dq_x.start()
    grad.finish()
    wo_g.sibling()
    wo_g.sibling_near()
    wo_g.sibling_far()
    wo_s.finish()
    load_wo = pltpu.make_async_copy(wo_full, big, lsem.at[2])
    load_wo.start()
    o_x.recv()
    load_wo.wait()

    def finish_out(cols):
        total = dot_nn(jnp.concatenate([o_all[h] for h in range(size)], axis=-1), big_cols(cols))
        out_ref[:, cols] = (x_ref[:, cols].astype(F32) + total).astype(BF16)
    col_tiles(finish_out)

    wq_g.sibling()
    wq_g.sibling_near()
    wq_g.sibling_far()
    wq_s.finish()
    load_wq = pltpu.make_async_copy(wq_full, big, lsem.at[3])
    load_wq.start()

    own = rows_of(p.me * block, block)
    total = kv_r.last()
    dkv_full[own, :head] = rope(total[:, :head], cos_ref[own, :], -sin_ref[own, :]).astype(BF16)
    dkv_full[own, head:] = total[:, head:].astype(BF16)
    dq_x.relay()
    kv_g.start()
    dq_x.recv()
    wo_copy.wait()
    load_wq.wait()

    def finish_da(cols):
        total = dot_nn(jnp.concatenate([dq_all[h] for h in range(size)], axis=-1), big_cols(cols))
        wide[:, cols] = (total + dot_nt(dkv_full[own, :head], wbuf[1, cols, :])
                         + dot_nt(dkv_full[own, head:], wbuf[2, cols, :]))
    col_tiles(finish_da)
    kv_g.first()

    dw_me[...] = jnp.zeros(dw_me.shape, F32)
    sub = 32

    @pl.loop(0, block // sub)
    def _(n):
        rows = pl.ds(pl.multiple_of(n * sub, sub), sub)
        x_f = x_ref[rows, :].astype(F32)
        inv = lax.rsqrt(jnp.mean(x_f * x_f, axis=-1, keepdims=True) + 1e-6)
        normed = x_f * inv
        da = wide[rows, :]
        dw_me[...] += jnp.sum(da * normed, axis=0, keepdims=True)
        gn = da * gain_ref[...]
        per = part_rows // sub
        dout = dout_ref[n // per, pl.ds(pl.multiple_of(lax.rem(n, per) * sub, sub), sub), :].astype(F32)
        dx_ref[rows, :] = (dout + inv * (gn - normed * jnp.mean(gn * normed, axis=-1, keepdims=True))).astype(BF16)

    for t, cols in enumerate(groups):
        dw_all[0, t:t + 1, :] = dw_me[:, cols]
    for d in range(1, size):
        remote(dw_all.at[0], dw_all.at[d], ss_w.at[d], rs_w.at[d], peers[d - 1]).start()
    kv_g.second()
    kv_g.third()
    for d in range(1, size):
        remote(dw_all.at[d], dw_all.at[d], ss_w.at[d], rs_w.at[d], p.sib).wait_recv()
    dw_ref[...] = jnp.sum(dw_all[...], axis=0)
    kv_g.sibling()
    kv_g.sibling_near()
    kv_g.sibling_far()
    kv_copy = pltpu.make_async_copy(dkv_full, dkv_out, lsem.at[2])
    kv_copy.start()

    for d in range(1, size):
        remote(dw_all.at[0], dw_all.at[0], ss_w.at[d], rs_w.at[d], p.sib).wait_send()
    for g in (act, wo_g, wq_g, kv_g, kv_r, o_x, dq_x):
        g.finish()
    a_copy.wait()
    dq_copy.wait()
    kv_copy.wait()


def weight_kernel(a_ref, dq_ref, dkv_ref, out_in, dx_in, dwo_in, dw_in,
                  dwq_ref, dwk_ref, dwv_ref, out_ref, dx_ref, dwo_ref, dw_ref, flipped):
    head = dq_ref.shape[1]

    @pl.when(pl.program_id(0) == 0)
    def _():
        flipped[:head, :] = dq_ref[...].T
        flipped[head:, :] = dkv_ref[...].T

    for src, dst in ((out_in, out_ref), (dx_in, dx_ref), (dwo_in, dwo_ref), (dw_in, dw_ref)):
        dst[...] = src[...]
    for n, dst in enumerate((dwq_ref, dwk_ref, dwv_ref)):
        dst[...] = dot_nn(flipped[n * head:(n + 1) * head, :], a_ref[...]).T


def local_block(size, stride, hidden, positions, norm_w, w_query, w_key, w_value, w_out, grad_out):
    _, block, width = hidden.shape
    seq = positions.shape[1]
    head = w_key.shape[1]
    half = head // 2
    chips, parts = size // 2, 4
    part_rows = block // parts
    lanes = 128
    x, dout = hidden[0], grad_out[0].reshape(parts, part_rows, width)
    inv_freq = (10000.0 ** (-2.0 * jnp.arange(half, dtype=F32) / head))[None, :]
    vm = pl.BlockSpec(memory_space=pltpu.VMEM)
    hbm = pl.BlockSpec(memory_space=pl.ANY)
    dma = pltpu.SemaphoreType.DMA
    shape = jax.ShapeDtypeStruct
    V = pltpu.VMEM
    full = (chips, 2, parts, part_rows, width)
    kv = 2 * head

    out, dx, dwo, dw, act, dq, dkv, _, _ = pl.pallas_call(
        functools.partial(block_kernel, size, stride),
        out_shape=[shape((block, width), BF16)] * 2 + [shape((head, width), F32), shape((width // 128, 128), F32),
                                                       shape((seq, width), BF16), shape((seq, head), BF16),
                                                       shape((seq, kv), BF16), shape(full, BF16), shape(full, BF16)],
        in_specs=[vm] * 3 + [hbm] * 6,
        out_specs=[vm, vm, hbm, vm] + [hbm] * 5,
        scratch_shapes=[V((block, width), BF16), V((parts, part_rows, width), BF16), V((1, width), F32),
                        V((seq, width), BF16), V(full, BF16), V((3, width, head), BF16), V((parts, part_rows, width), BF16),
                        V((parts, part_rows, width), BF16)] + [V((seq, head), BF16)] * 5
        + [V((seq, kv), F32), V((seq, kv), BF16), V((size, block, head), BF16), V((size, block, head), BF16),
           V((2, block, head), BF16), V((2, block, head), BF16), V((seq, 128), F32), V((seq, half), F32), V((seq, half), F32),
           V((TILE, 128), F32), V((TILE, 128), F32), V((TILE, head), F32),
           V((4, block, kv), F32), V((3, block, kv), F32), V((block // 2, kv), F32), V((block // 2, kv), F32),
           V((block, kv), F32), V((block, kv), F32), V((head, width), F32), V((1, width), F32),
           V((size, width // 128, 128), F32), dma((10,))]
        + [dma((13,))] * 10 + [dma((8,))] * 4 + [dma((9,))] * 4 + [dma((10,))] * 2 + [dma((size,))] * 2,
        compiler_params=pltpu.CompilerParams(collective_id=0, has_side_effects=True, vmem_limit_bytes=VMEM_LIMIT),
        name='attention_block',
    )(norm_w.reshape(width // lanes, lanes), positions, inv_freq, x, dout, w_query, w_key, w_value,
      w_out.reshape(parts, part_rows, width))

    steps = width // COLS
    whole = lambda *dims: pl.BlockSpec(dims, lambda n: (0, 0))
    rows = lambda *dims: pl.BlockSpec(dims, lambda n: (n, 0))
    small = (width // lanes, lanes)
    passed = [rows(block // steps, width), rows(block // steps, width), rows(head // steps, width), whole(*small)]
    dwq, dwk, dwv, out, dx, dwo, dw = pl.pallas_call(
        weight_kernel,
        grid=(steps,),
        out_shape=[shape((width, head), F32)] * 3 + [shape((block, width), BF16)] * 2 + [shape((head, width), F32), shape(small, F32)],
        in_specs=[pl.BlockSpec((seq, COLS), lambda n: (0, n)), whole(seq, head), whole(seq, kv)] + passed,
        out_specs=[rows(COLS, head)] * 3 + passed,
        scratch_shapes=[V((3 * head, seq), BF16)],
        name='weight_grads',
    )(act, dq, dkv, out, dx, dwo, dw)
    return out[None], dx[None], dwq, dwo, dwk, dwv, dw.reshape(width)


def solution(mesh):
    specs_in = (P('dp', 'tp', None), P('dp', None), P(None), P(None, 'tp'), P(None, None), P(None, None), P('tp', None), P('dp', 'tp', None))
    specs_out = (P('dp', 'tp', None), P('dp', 'tp', None), P('dp', 'tp'), P(('dp', 'tp'), None), P('dp', None), P('dp', None), P('dp'))
    column = [tuple(d.coords) for d in mesh.devices[:, 0]]
    stride = sum(c[1] == column[0][1] for c in column)
    local = functools.partial(local_block, mesh.shape['tp'], stride)
    return jax.shard_map(local, mesh=mesh, in_specs=specs_in, out_specs=specs_out, check_vma=False)
```

```python
import functools

import jax
import jax.numpy as jnp
import numpy as np
from jax import lax
from jax.experimental import pallas as pl
from jax.experimental.pallas import tpu as pltpu
from jax.sharding import PartitionSpec as P

MESH = pl.DeviceIdType.MESH
F32 = jnp.float32
BF16 = jnp.bfloat16
TILE = 512
STRIP = 256
COLS = 512
VMEM_LIMIT = 63 * 1024 * 1024
KEPT = 16 * 1024 * 1024


def dot_nn(a, b):
    return lax.dot_general(a, b, (((1,), (0,)), ((), ())), preferred_element_type=F32)


def dot_nt(a, b):
    return lax.dot_general(a, b, (((1,), (1,)), ((), ())), preferred_element_type=F32)


def dot_tn(a, b):
    return lax.dot_general(a, b, (((0,), (0,)), ((), ())), preferred_element_type=F32)


def rope(u, cos_t, sin_t):
    half = u.shape[-1] // 2
    first, second = u[:, :half], u[:, half:]
    return jnp.concatenate([first * cos_t - second * sin_t, second * cos_t + first * sin_t], axis=-1)


class Place:
    def __init__(self, size, stride):
        n = size // 2
        group = lax.axis_index('dp')
        z, y = lax.rem(group, 2), lax.rem(lax.div(group, stride), 2)
        self.group_z = group + 1 - 2 * z
        self.group_y = group + stride * (1 - 2 * y)
        self.part = 2 * y + z
        self.part_z, self.part_y, self.part_d = 2 * y + 1 - z, 2 * (1 - y) + z, 3 - self.part
        self.me = lax.axis_index('tp')
        self.core = lax.rem(self.me, 2)
        self.chip = lax.div(self.me, 2)
        self.chip_r = lax.rem(self.chip + 1, n)
        self.chip_l = lax.rem(self.chip + n - 1, n)
        self.chip_o = lax.rem(self.chip + 2, n)
        self.right = self.chip_r * 2 + self.core
        self.left = self.chip_l * 2 + self.core
        self.sib = self.chip * 2 + 1 - self.core


def remote(src, dst, ssem, rsem, to):
    return pltpu.make_async_remote_copy(src_ref=src, dst_ref=dst, send_sem=ssem, recv_sem=rsem,
                                        device_id={'tp': to}, device_id_type=MESH)


def rows_of(start, size):
    return pl.ds(pl.multiple_of(start, min(size, 128)), size)


class Gather:
    def __init__(self, place, at, ssem, rsem):
        self.at, self.p, self.ssem, self.rsem = at, place, ssem, rsem
        p = place
        self.own = [at(p.chip, p.core, h) for h in (0, 1)]
        self.own_all = at(p.chip, p.core, None)
        regions = []
        for core in (p.core, 1 - p.core):
            for chip in (p.chip_l, p.chip_r, p.chip_o):
                regions += [at(chip, core, 0), at(chip, core, 1)]
        self.regions = regions[:6] + [at(p.chip, 1 - p.core, None)] + regions[6:]

    def _send(self, sem, src, dst, rsem, to):
        remote(src, dst, self.ssem.at[sem], self.rsem.at[rsem], to).start()

    def start(self, parts=None, whole=None):
        p = self.p
        parts = self.own if parts is None else parts
        whole = self.own_all if whole is None else whole
        self._send(0, parts[0], self.own[0], 0, p.right)
        self._send(3, parts[1], self.own[1], 3, p.left)
        self._send(1, parts[1], self.own[1], 1, p.right)
        self._send(2, parts[0], self.own[0], 2, p.left)
        self._send(6, whole, self.own_all, 6, p.sib)

    def recv(self, *which):
        for k in which:
            ref = self.regions[k]
            remote(ref, ref, self.ssem.at[k], self.rsem.at[k], self.p.sib).wait_recv()

    def _forward_only(self, *which):
        for k in which:
            self._send(7 + k, self.regions[k], self.regions[k], 7 + k, self.p.sib)

    def _forward(self, *which):
        self.recv(*which)
        self._forward_only(*which)

    def first(self):
        self.recv(0, 3)
        self._send(4, self.regions[0], self.regions[0], 4, self.p.right)
        self._send(5, self.regions[3], self.regions[3], 5, self.p.left)
        self._forward_only(0, 3)

    def second(self):
        self._forward(1, 2)

    def third(self):
        self._forward(4, 5)

    def sibling(self):
        self.recv(6)

    def sibling_near(self):
        self.recv(7, 8, 9, 10)

    def sibling_far(self):
        self.recv(11, 12)

    def finish(self):
        for k in range(13):
            ref = self.own_all if k == 6 else self.own[0]
            remote(ref, ref, self.ssem.at[k], self.rsem.at[k], self.p.sib).wait_send()


class Share:
    def __init__(self, place, full, rows, ssem, rsem):
        self.p, self.full, self.rows, self.ssem, self.rsem = place, full, rows, ssem, rsem

    def at(self, part, h=None, other=False):
        core = 1 - self.p.core if other else self.p.core
        if h is None:
            return self.full.at[:, core, part]
        return self.full.at[:, core, part, pl.ds(h * self.rows, self.rows)]

    def _send(self, k, ref, **to):
        pltpu.make_async_remote_copy(src_ref=ref, dst_ref=ref, send_sem=self.ssem.at[k], recv_sem=self.rsem.at[k],
                                     device_id=to, device_id_type=MESH).start()

    def _recv(self, k, ref):
        remote(ref, ref, self.ssem.at[k], self.rsem.at[k], self.p.sib).wait_recv()

    def start(self):
        p = self.p
        self._send(0, self.at(p.part), dp=p.group_z)
        self._send(1, self.at(p.part), dp=p.group_y)

    def relay(self):
        p = self.p
        self._recv(0, self.at(p.part_z))
        self._send(2, self.at(p.part_z, 0), dp=p.group_y)
        self._recv(1, self.at(p.part_y))
        self._send(3, self.at(p.part_y, 1), dp=p.group_z)
        self._send(4, self.at(p.part_z), tp=p.sib)
        self._send(5, self.at(p.part_y), tp=p.sib)

    def forward(self):
        p = self.p
        for h in (0, 1):
            self._recv(2 + h, self.at(p.part_d, h))
            self._send(6 + h, self.at(p.part_d, h), tp=p.sib)

    def finish(self):
        p = self.p
        for k, h in enumerate((None, None, 0, 0, None, None, 0, 0)):
            ref = self.at(p.part, h)
            remote(ref, ref, self.ssem.at[k], self.rsem.at[k], p.sib).wait_send()
        self._recv(4, self.at(p.part_z, None, True))
        self._recv(5, self.at(p.part_y, None, True))
        self._recv(6, self.at(p.part_d, 0, True))
        self._recv(7, self.at(p.part_d, 1, True))


class Exchange:
    def __init__(self, place, block, src, dst, relays, ssem, rsem):
        self.p, self.block, self.src, self.dst, self.relays, self.ssem, self.rsem = place, block, src, dst, relays, ssem, rsem

    def _send(self, sem, src, dst, rsem, to):
        remote(src, dst, self.ssem.at[sem], self.rsem.at[rsem], to).start()

    def part(self, chip, core):
        return self.src.at[rows_of((chip * 2 + core) * self.block, self.block)]

    def start(self):
        p = self.p
        slot = self.dst.at[p.me]
        self._send(0, self.part(p.chip_o, 0), self.relays.at[0], 0, p.right)
        self._send(1, self.part(p.chip_o, 1), self.relays.at[1], 1, p.left)
        for core in (0, 1):
            self._send(2 + core, self.part(p.chip_r, core), slot, 2 + p.core, p.chip_r * 2 + core)
            self._send(4 + core, self.part(p.chip_l, core), slot, 4 + p.core, p.chip_l * 2 + core)
        self._send(8, self.part(p.chip, 1 - p.core), slot, 8, p.sib)
        self.dst[p.me] = self.src[rows_of(p.me * self.block, self.block), :]

    def _recv(self, k, ref):
        remote(ref, ref, self.ssem.at[k], self.rsem.at[k], self.p.sib).wait_recv()

    def relay(self):
        p = self.p
        self._recv(0, self.relays.at[0])
        self._send(6, self.relays.at[0], self.dst.at[p.left], 6 + p.core, p.chip_r * 2)
        self._recv(1, self.relays.at[1])
        self._send(7, self.relays.at[1], self.dst.at[p.right], 6 + p.core, p.chip_l * 2 + 1)

    def recv(self):
        p = self.p
        for core in (0, 1):
            self._recv(2 + core, self.dst.at[p.chip_l * 2 + core])
            self._recv(4 + core, self.dst.at[p.chip_r * 2 + core])
            self._recv(6 + core, self.dst.at[p.chip_o * 2 + core])
        self._recv(8, self.dst.at[p.sib])

    def finish(self):
        for k in range(9):
            ref = self.relays.at[0]
            remote(ref, ref, self.ssem.at[k], self.rsem.at[k], self.p.sib).wait_send()


class Scatter:
    def __init__(self, place, block, src, d2d, sums, top, bot, from_l, from_r, ssem, rsem):
        self.__dict__.update(locals())
        self.half = block // 2

    def rows(self, chip, core, h=None):
        row = (chip * 2 + core) * self.block
        return rows_of(row, self.block) if h is None else rows_of(row + h * self.half, self.half)

    def _send(self, k, src, dst, to):
        remote(src, dst, self.ssem.at[k], self.rsem.at[k], to).start()

    def _recv(self, k, ref):
        remote(ref, ref, self.ssem.at[k], self.rsem.at[k], self.place.sib).wait_recv()

    def chip_send(self):
        p = self.place
        for k, chip in enumerate((p.chip_o, p.chip_r, p.chip_l, p.chip)):
            self._send(k, self.src.at[self.rows(chip, 1 - p.core)], self.d2d.at[k], p.sib)

    def far(self):
        p, half = self.place, self.half
        self._recv(0, self.d2d.at[0])
        self.sums[0] = self.src[self.rows(p.chip_o, p.core), :] + self.d2d[0]
        self._send(4, self.sums.at[0, pl.ds(0, half)], self.top, p.right)
        self._send(5, self.sums.at[0, pl.ds(half, half)], self.bot, p.left)

    def near_half(self, k, h, chip, extra, dst, sem, to):
        rows = pl.ds(h * self.half, self.half)
        total = self.src[self.rows(chip, self.place.core, h), :] + self.d2d[k, rows, :]
        self.sums[k, rows, :] = total if extra is None else total + extra[...]
        self._send(sem, self.sums.at[k, rows], dst.at[rows], to)

    def near_first(self):
        p = self.place
        self._recv(1, self.d2d.at[1])
        self.near_half(1, 1, p.chip_r, None, self.from_l, 6, p.right)
        self._recv(2, self.d2d.at[2])
        self.near_half(2, 0, p.chip_l, None, self.from_r, 8, p.left)

    def near_second(self):
        p = self.place
        self._recv(4, self.top)
        self.near_half(1, 0, p.chip_r, self.top, self.from_l, 7, p.right)
        self._recv(5, self.bot)
        self.near_half(2, 1, p.chip_l, self.bot, self.from_r, 9, p.left)

    def last(self):
        p, half = self.place, self.half
        self._recv(3, self.d2d.at[3])
        for k, ref, h in ((6, self.from_l, 1), (7, self.from_l, 0), (8, self.from_r, 0), (9, self.from_r, 1)):
            self._recv(k, ref.at[pl.ds(h * half, half)])
        return self.src[self.rows(p.chip, p.core), :] + self.d2d[3] + self.from_l[...] + self.from_r[...]

    def finish(self):
        for k in range(10):
            ref = self.d2d.at[0] if k < 4 else self.top
            remote(ref, ref, self.ssem.at[k], self.rsem.at[k], self.place.sib).wait_send()


def block_kernel(size, stride, norm_ref, pos_ref, freq_ref, x_hbm, dout_hbm, wq_hbm, wk_hbm, wv_hbm, wo_hbm,
                 out_ref, dx_ref, dwo_ref, dw_ref, act_full, dq_ref, dkv_full, wo_full, wq_full,
                 x_ref, dout_ref, gain_ref, big, wbuf, wo, wqt, q_ref, k_ref, v_ref, o_ref, dkv_ref, o_all, dq_all,
                 relay_o, relay_q, lse_ref, cos_ref, sin_ref, m_scr, l_scr, acc,
                 d2d, sums, top, bot, from_l, from_r, wide, dw_me, dw_all, lsem,
                 ss_a, rs_a, ss_d, rs_d, ss_wo, rs_wo, ss_wq, rs_wq, ss_kv, rs_kv, ss_yo, rs_yo, ss_yq, rs_yq,
                 ss_o, rs_o, ss_q, rs_q, ss_r, rs_r, ss_w, rs_w):
    p = Place(size, stride)
    block, width = x_ref.shape
    seq, head = q_ref.shape
    chips = size // 2
    half = block // 2
    parts, part_rows = wo.shape[:2]
    scale = head ** -0.5
    wo_rows = lambda: wo[...].reshape(head, width)

    barrier = pltpu.get_barrier_semaphore()
    peers = [lax.rem(p.me + d, size) for d in range(1, size)]
    for to in [{'tp': peer} for peer in peers] + [{'dp': p.group_z}, {'dp': p.group_y}]:
        pl.semaphore_signal(barrier, inc=1, device_id=to, device_id_type=MESH)

    load_x, load_wq, load_wo, load_dout, *load_kv = [pltpu.make_async_copy(src, dst, lsem.at[i]) for i, (src, dst) in enumerate(
        ((x_hbm, x_ref), (wq_hbm, wbuf.at[0]), (wo_hbm, wo), (dout_hbm, dout_ref), (wk_hbm, wbuf.at[1]), (wv_hbm, wbuf.at[2])))]
    for copy in (load_x, load_wq, load_wo, load_dout, *load_kv):
        copy.start()
    lanes = 128
    groups = [slice(t * lanes, (t + 1) * lanes) for t in range(width // lanes)]
    for t, cols in enumerate(groups):
        gain_ref[:, cols] = 1.0 + norm_ref[t:t + 1, :]

    def weight_at(full):
        quarter = part_rows // 2

        def at(chip, core, h):
            if h is None:
                return full.at[chip, core, p.part]
            return full.at[chip, core, p.part, pl.ds(h * quarter, quarter)]
        return at

    def rows_at(full):
        def at(chip, core, h):
            row = (chip * 2 + core) * block
            return full.at[rows_of(row, block) if h is None else rows_of(row + h * half, half)]
        return at

    def grad_at(chip, core, h):
        return big.at[chip, core] if h is None else big.at[chip, core, pl.ds(h * (parts // 2), parts // 2)]

    act = Gather(p, rows_at(act_full), ss_a, rs_a)
    grad = Gather(p, grad_at, ss_d, rs_d)
    wo_g = Gather(p, weight_at(wo_full), ss_wo, rs_wo)
    wq_g = Gather(p, weight_at(wq_full), ss_wq, rs_wq)
    kv_g = Gather(p, rows_at(dkv_full), ss_kv, rs_kv)
    wo_s = Share(p, wo_full, part_rows // 2, ss_yo, rs_yo)
    wq_s = Share(p, wq_full, part_rows // 2, ss_yq, rs_yq)
    o_x = Exchange(p, block, o_ref, o_all, relay_o, ss_o, rs_o)
    dq_x = Exchange(p, block, dq_ref, dq_all, relay_q, ss_q, rs_q)
    kv_r = Scatter(p, block, dkv_ref, d2d, sums, top, bot, from_l, from_r, ss_r, rs_r)

    def start_weight(g, shard, src, sem):
        quarter = part_rows // 2
        g.start([src.at[p.part, pl.ds(h * quarter, quarter)] for h in (0, 1)], src.at[p.part])
        own = pltpu.make_async_copy(shard.at[p.part], g.own_all, lsem.at[sem])
        own.start()
        return own

    pl.semaphore_wait(barrier, size + 1)
    load_wo.wait()
    own_wo = start_weight(wo_g, wo, wo_hbm, 6)
    load_wq.wait()

    @pl.loop(0, width // COLS)
    def _(n):
        rows = pl.ds(pl.multiple_of(n * COLS, COLS), COLS)
        flipped = wbuf[0, rows, :].T
        for g in range(parts):
            wqt[g, :, rows] = flipped[g * part_rows:(g + 1) * part_rows, :]
    own_wq = start_weight(wq_g, wqt, wqt, 7)

    load_x.wait()

    @pl.loop(0, block // 64)
    def _(n):
        rows = pl.ds(pl.multiple_of(n * 64, 64), 64)
        x_f = x_ref[rows, :].astype(F32)
        inv = lax.rsqrt(jnp.mean(x_f * x_f, axis=-1, keepdims=True) + 1e-6)
        act_full[rows_of(p.me * block + n * 64, 64), :] = (x_f * inv * gain_ref[...]).astype(BF16)

    for g in (wo_g, wq_g):
        g.first()
    act.start()

    @pl.loop(0, seq // lanes)
    def _(n):
        rows = pl.ds(pl.multiple_of(n * lanes, lanes), lanes)
        angle = jnp.broadcast_to(pos_ref[:, rows].astype(F32), (lanes, lanes)).T * freq_ref[...]
        cos_ref[rows, :] = jnp.cos(angle)
        sin_ref[rows, :] = jnp.sin(angle)

    load_dout.wait()
    big[p.chip, p.core] = dout_ref[...]
    for copy in load_kv:
        copy.wait()

    def project(first, second):
        @pl.loop(0, 2)
        def _(n):
            rows = rows_of((first + n * (second - first)) * block, block)
            a = act_full[rows, :]
            cos_t, sin_t = cos_ref[rows, :], sin_ref[rows, :]
            query = dot_nn(a, wbuf[0]).astype(BF16).astype(F32)
            q_ref[rows, :] = (rope(query, cos_t, sin_t) * scale).astype(BF16)
            key = dot_nn(a, wbuf[1]).astype(BF16).astype(F32)
            k_ref[rows, :] = rope(key, cos_t, sin_t).astype(BF16)
            v_ref[rows, :] = dot_nn(a, wbuf[2]).astype(BF16)

    for g, s, own in ((wo_g, wo_s, own_wo), (wq_g, wq_s, own_wq)):
        g.second()
        g.third()
        own.wait()
        s.start()

    act.sibling()
    project(p.me, p.sib)
    act.first()
    grad.start([dout_ref.at[pl.ds(h * (parts // 2), parts // 2)] for h in (0, 1)], dout_ref)
    act.second()
    project(p.left, p.right)
    act.sibling_near()
    project(p.chip_l * 2 + 1 - p.core, p.chip_r * 2 + 1 - p.core)
    act.third()
    act.sibling_far()
    project(p.chip_o * 2 + p.core, p.chip_o * 2 + 1 - p.core)

    row_ids = lax.broadcasted_iota(jnp.int32, (TILE, TILE), 0)
    col_ids = lax.broadcasted_iota(jnp.int32, (TILE, TILE), 1)

    def tile_rows(j):
        return pl.ds(pl.multiple_of(j * TILE, TILE), TILE)

    def lane_groups(v):
        return [v[:, t * lanes:(t + 1) * lanes] for t in range(TILE // lanes)]

    def spread(v):
        return jnp.concatenate([v] * (TILE // lanes), axis=-1)

    diagonal = row_ids >= col_ids

    @pl.loop(0, seq // TILE)
    def _(i):
        rows = tile_rows(i)
        m_scr[...] = jnp.full(m_scr.shape, -1e30, F32)

        def score(j, s):
            dkv_ref[tile_rows(j), :] = s
            m_scr[...] = functools.reduce(jnp.maximum, lane_groups(s), m_scr[...])

        @pl.loop(0, i)
        def _(j):
            score(j, dot_nt(q_ref[rows, :], k_ref[tile_rows(j), :]))

        score(i, jnp.where(diagonal, dot_nt(q_ref[rows, :], k_ref[rows, :]), -1e30))
        m_scr[...] = jnp.broadcast_to(jnp.max(m_scr[...], axis=-1, keepdims=True), m_scr.shape)
        l_scr[...] = jnp.zeros(l_scr.shape, F32)
        acc[...] = jnp.zeros(acc.shape, F32)

        @pl.loop(0, i + 1)
        def _(j):
            prob = jnp.exp(dkv_ref[tile_rows(j), :] - spread(m_scr[...]))
            l_scr[...] = functools.reduce(jnp.add, lane_groups(prob), l_scr[...])
            acc[...] += dot_nn(prob.astype(BF16), v_ref[tile_rows(j), :])

        total = jnp.sum(l_scr[...], axis=-1, keepdims=True)
        lse_ref[rows, :] = m_scr[...] + jnp.log(total)
        o_ref[rows, :] = (acc[...] / total).astype(BF16)

    dkv_ref[...] = jnp.zeros(dkv_ref.shape, F32)

    def backward(first, second, count):
        @pl.loop(0, count)
        def _(n):
            i = first + n * (second - first)
            rows = tile_rows(i)
            do = dot_nt(big[i].reshape(TILE, width), wo_rows()).astype(BF16)
            row_dot = jnp.sum(do.astype(F32) * o_ref[rows, :].astype(F32), axis=-1, keepdims=True)
            m_scr[...] = jnp.broadcast_to(row_dot, m_scr.shape)
            acc[...] = jnp.zeros(acc.shape, F32)
            q = q_ref[rows, :]

            def inner(j, masked):
                cols = tile_rows(j)
                prob = jnp.exp(dot_nt(q, k_ref[cols, :]) - spread(lse_ref[rows, :]))
                if masked:
                    prob = jnp.where(diagonal, prob, 0.0)
                dkv_ref[cols, head:] += dot_tn(prob.astype(BF16), do)
                ds = (prob * (dot_nt(do, v_ref[cols, :]) - spread(m_scr[...]))).astype(BF16)
                dkv_ref[cols, :head] += dot_tn(ds, q)
                acc[...] += dot_nn(ds, k_ref[cols, :])

            @pl.loop(0, i)
            def _(j):
                inner(j, False)
            inner(i, True)

            dq_ref[rows, :] = rope(acc[...] * scale, cos_ref[rows, :], -sin_ref[rows, :]).astype(BF16)

    grad.sibling()
    backward(p.chip, p.chip, 1)
    grad.first()
    o_x.start()
    for s in (wo_s, wq_s):
        s.relay()
    act.finish()

    def strip(n):
        return pl.ds(pl.multiple_of(n * STRIP, STRIP), STRIP)

    @pl.loop(0, width // STRIP)
    def _(i):
        @pl.loop(0, i + 1)
        def _(j):
            upper, lower = act_full[strip(j), strip(i)], act_full[strip(i), strip(j)]
            act_full[strip(i), strip(j)] = upper.T
            act_full[strip(j), strip(i)] = lower.T

    grad.second()
    grad.sibling_near()
    backward(p.chip_l, p.chip_r, 2)
    grad.third()
    grad.sibling_far()
    backward(p.chip_o, p.chip_o, 1)

    kv_r.chip_send()
    o_x.relay()
    kv_r.far()
    kv_r.near_first()
    for s in (wo_s, wq_s):
        s.forward()

    def col_tiles(fn):
        @pl.loop(0, width // COLS)
        def _(n):
            fn(pl.ds(pl.multiple_of(n * COLS, COLS), COLS))

    def big_cols(cols):
        return big[:, :, :, :, cols].reshape(seq, COLS)

    def weight_o(cols):
        dwo_ref[:, cols] = dot_tn(o_ref[...], big_cols(cols))
    col_tiles(weight_o)

    kv_r.near_second()
    dq_x.start()
    grad.finish()
    wo_g.sibling()
    wo_g.sibling_near()
    wo_g.sibling_far()
    wo_s.finish()
    load_wo = pltpu.make_async_copy(wo_full, big, lsem.at[2])
    load_wo.start()
    o_x.recv()
    load_wo.wait()

    def finish_out(cols):
        total = dot_nn(jnp.concatenate([o_all[h] for h in range(size)], axis=-1), big_cols(cols))
        out_ref[:, cols] = (x_ref[:, cols].astype(F32) + total).astype(BF16)
    col_tiles(finish_out)

    wq_g.sibling()
    wq_g.sibling_near()
    wq_g.sibling_far()
    wq_s.finish()
    load_wq = pltpu.make_async_copy(wq_full, big, lsem.at[3])
    load_wq.start()

    own = rows_of(p.me * block, block)
    total = kv_r.last()
    dkv_full[own, :head] = rope(total[:, :head], cos_ref[own, :], -sin_ref[own, :]).astype(BF16)
    dkv_full[own, head:] = total[:, head:].astype(BF16)
    dq_x.relay()
    kv_g.start()
    dq_x.recv()
    load_wq.wait()

    def finish_da(cols):
        total = dot_nn(jnp.concatenate([dq_all[h] for h in range(size)], axis=-1), big_cols(cols))
        wide[:, cols] = (total + dot_nt(dkv_full[own, :head], wbuf[1, cols, :])
                         + dot_nt(dkv_full[own, head:], wbuf[2, cols, :]))
    col_tiles(finish_da)
    kv_g.first()

    dw_me[...] = jnp.zeros(dw_me.shape, F32)
    sub = 32

    @pl.loop(0, block // sub)
    def _(n):
        rows = pl.ds(pl.multiple_of(n * sub, sub), sub)
        x_f = x_ref[rows, :].astype(F32)
        inv = lax.rsqrt(jnp.mean(x_f * x_f, axis=-1, keepdims=True) + 1e-6)
        normed = x_f * inv
        da = wide[rows, :]
        dw_me[...] += jnp.sum(da * normed, axis=0, keepdims=True)
        gn = da * gain_ref[...]
        per = part_rows // sub
        dout = dout_ref[n // per, pl.ds(pl.multiple_of(lax.rem(n, per) * sub, sub), sub), :].astype(F32)
        dx_ref[rows, :] = (dout + inv * (gn - normed * jnp.mean(gn * normed, axis=-1, keepdims=True))).astype(BF16)

    for t, cols in enumerate(groups):
        dw_all[0, t:t + 1, :] = dw_me[:, cols]
    for d in range(1, size):
        remote(dw_all.at[0], dw_all.at[d], ss_w.at[d], rs_w.at[d], peers[d - 1]).start()
    kv_g.second()
    kv_g.third()
    for d in range(1, size):
        remote(dw_all.at[d], dw_all.at[d], ss_w.at[d], rs_w.at[d], p.sib).wait_recv()
    dw_ref[...] = jnp.sum(dw_all[...], axis=0)
    kv_g.sibling()
    kv_g.sibling_near()
    kv_g.sibling_far()

    for d in range(1, size):
        remote(dw_all.at[0], dw_all.at[0], ss_w.at[d], rs_w.at[d], p.sib).wait_send()
    for g in (wo_g, wq_g, kv_g, kv_r, o_x, dq_x):
        g.finish()


def weight_kernel(out_in, dx_in, dwo_in, dw_in, a_ref, dq_ref, dkv_ref,
                  dwq_ref, dwk_ref, dwv_ref, out_ref, dx_ref, dwo_ref, dw_ref):
    step = pl.program_id(0)
    head = dq_ref.shape[1]

    def part(rows):
        return pl.ds(pl.multiple_of(step * rows, rows), rows)
    for src, dst in ((out_in, out_ref), (dx_in, dx_ref), (dwo_in, dwo_ref)):
        dst[...] = src[part(dst.shape[0]), :]
    dw_ref[...] = dw_in[...]
    a = a_ref[part(dwq_ref.shape[0]), :]
    dwq_ref[...] = dot_nn(a, dq_ref[...])
    dwk_ref[...] = dot_nn(a, dkv_ref[:, :head])
    dwv_ref[...] = dot_nn(a, dkv_ref[:, head:])


def local_block(size, stride, hidden, positions, norm_w, w_query, w_key, w_value, w_out, grad_out):
    _, block, width = hidden.shape
    seq = positions.shape[1]
    head = w_key.shape[1]
    half = head // 2
    chips, parts = size // 2, 4
    part_rows = block // parts
    lanes = 128
    x, dout = hidden[0], grad_out[0].reshape(parts, part_rows, width)
    inv_freq = (10000.0 ** (-2.0 * np.arange(half) / head)).astype(np.float32)[None, :]
    vm = pl.BlockSpec(memory_space=pltpu.VMEM)
    hbm = pl.BlockSpec(memory_space=pl.ANY)
    dma = pltpu.SemaphoreType.DMA
    shape = jax.ShapeDtypeStruct
    V = pltpu.VMEM
    full = (chips, 2, parts, part_rows, width)
    kv = 2 * head
    small = (width // lanes, lanes)

    *results, _, _ = pl.pallas_call(
        functools.partial(block_kernel, size, stride),
        out_shape=[V((block, width), BF16), V((block, width), BF16), V((head, width), F32), V(small, F32),
                   V((seq, width), BF16), V((seq, head), BF16), V((seq, kv), BF16), shape(full, BF16), shape(full, BF16)],
        in_specs=[vm] * 3 + [hbm] * 6,
        out_specs=[vm] * 7 + [hbm] * 2,
        scratch_shapes=[V((block, width), BF16), V((parts, part_rows, width), BF16), V((1, width), F32),
                        V(full, BF16), V((3, width, head), BF16), V((parts, part_rows, width), BF16),
                        V((parts, part_rows, width), BF16)] + [V((seq, head), BF16)] * 4
        + [V((seq, kv), F32), V((size, block, head), BF16), V((size, block, head), BF16),
           V((2, block, head), BF16), V((2, block, head), BF16), V((seq, 128), F32), V((seq, half), F32), V((seq, half), F32),
           V((TILE, 128), F32), V((TILE, 128), F32), V((TILE, head), F32),
           V((4, block, kv), F32), V((3, block, kv), F32), V((block // 2, kv), F32), V((block // 2, kv), F32),
           V((block, kv), F32), V((block, kv), F32), V((head, width), F32), V((1, width), F32),
           V((size, width // 128, 128), F32), dma((8,))]
        + [dma((13,))] * 10 + [dma((8,))] * 4 + [dma((9,))] * 4 + [dma((10,))] * 2 + [dma((size,))] * 2,
        compiler_params=pltpu.CompilerParams(collective_id=0, has_side_effects=True, vmem_limit_bytes=VMEM_LIMIT - KEPT),
        name='attention_block',
    )(norm_w.reshape(width // lanes, lanes), positions, inv_freq, x, dout, w_query, w_key, w_value,
      w_out.reshape(parts, part_rows, width))

    steps = width // COLS
    whole = lambda *dims: pl.BlockSpec(dims, lambda n: (0, 0))
    rows = lambda *dims: pl.BlockSpec(dims, lambda n: (n, 0))
    passed = [rows(block // steps, width), rows(block // steps, width), rows(head // steps, width), whole(*small)]
    dwq, dwk, dwv, out, dx, dwo, dw = pl.pallas_call(
        weight_kernel,
        grid=(steps,),
        out_shape=[shape((width, head), F32)] * 3 + [shape((block, width), BF16)] * 2 + [shape((head, width), F32), shape(small, F32)],
        in_specs=[vm] * 7,
        out_specs=[rows(COLS, head)] * 3 + passed,
        compiler_params=pltpu.CompilerParams(vmem_limit_bytes=VMEM_LIMIT - KEPT),
        name='weight_grads',
    )(*[pltpu.with_memory_space_constraint(v, V) for v in results])
    return out[None], dx[None], dwq, dwo, dwk, dwv, dw.reshape(width)


def solution(mesh):
    specs_in = (P('dp', 'tp', None), P('dp', None), P(None), P(None, 'tp'), P(None, None), P(None, None), P('tp', None), P('dp', 'tp', None))
    specs_out = (P('dp', 'tp', None), P('dp', 'tp', None), P('dp', 'tp'), P(('dp', 'tp'), None), P('dp', None), P('dp', None), P('dp'))
    column = [tuple(d.coords) for d in mesh.devices[:, 0]]
    stride = sum(c[1] == column[0][1] for c in column)
    local = functools.partial(local_block, mesh.shape['tp'], stride)
    return jax.shard_map(local, mesh=mesh, in_specs=specs_in, out_specs=specs_out, check_vma=False)
```

```python
import functools

import jax
import jax.numpy as jnp
import numpy as np
from jax import lax
from jax.experimental import pallas as pl
from jax.experimental.pallas import tpu as pltpu
from jax.sharding import PartitionSpec as P

MESH = pl.DeviceIdType.MESH
F32 = jnp.float32
BF16 = jnp.bfloat16
TILE = 512
STRIP = 256
COLS = 512
VMEM_LIMIT = 63 * 1024 * 1024
KEPT = 16 * 1024 * 1024


def dot_nn(a, b):
    return lax.dot_general(a, b, (((1,), (0,)), ((), ())), preferred_element_type=F32)


def dot_nt(a, b):
    return lax.dot_general(a, b, (((1,), (1,)), ((), ())), preferred_element_type=F32)


def dot_tn(a, b):
    return lax.dot_general(a, b, (((0,), (0,)), ((), ())), preferred_element_type=F32)


def rope(u, cos_t, sin_t):
    half = u.shape[-1] // 2
    first, second = u[:, :half], u[:, half:]
    return jnp.concatenate([first * cos_t - second * sin_t, second * cos_t + first * sin_t], axis=-1)


class Place:
    def __init__(self, size, stride):
        n = size // 2
        group = lax.axis_index('dp')
        z, y = lax.rem(group, 2), lax.rem(lax.div(group, stride), 2)
        self.group_z = group + 1 - 2 * z
        self.group_y = group + stride * (1 - 2 * y)
        self.part = 2 * y + z
        self.part_z, self.part_y, self.part_d = 2 * y + 1 - z, 2 * (1 - y) + z, 3 - self.part
        self.me = lax.axis_index('tp')
        self.core = lax.rem(self.me, 2)
        self.chip = lax.div(self.me, 2)
        self.chip_r = lax.rem(self.chip + 1, n)
        self.chip_l = lax.rem(self.chip + n - 1, n)
        self.chip_o = lax.rem(self.chip + 2, n)
        self.right = self.chip_r * 2 + self.core
        self.left = self.chip_l * 2 + self.core
        self.sib = self.chip * 2 + 1 - self.core


def remote(src, dst, ssem, rsem, to):
    return pltpu.make_async_remote_copy(src_ref=src, dst_ref=dst, send_sem=ssem, recv_sem=rsem,
                                        device_id={'tp': to}, device_id_type=MESH)


def rows_of(start, size):
    return pl.ds(pl.multiple_of(start, min(size, 128)), size)


class Gather:
    def __init__(self, place, at, ssem, rsem):
        self.at, self.p, self.ssem, self.rsem = at, place, ssem, rsem
        p = place
        self.own = [at(p.chip, p.core, h) for h in (0, 1)]
        self.own_all = at(p.chip, p.core, None)
        regions = []
        for core in (p.core, 1 - p.core):
            for chip in (p.chip_l, p.chip_r, p.chip_o):
                regions += [at(chip, core, 0), at(chip, core, 1)]
        self.regions = regions[:6] + [at(p.chip, 1 - p.core, None)] + regions[6:]

    def _send(self, sem, src, dst, rsem, to):
        remote(src, dst, self.ssem.at[sem], self.rsem.at[rsem], to).start()

    def start(self, parts=None, whole=None):
        p = self.p
        parts = self.own if parts is None else parts
        whole = self.own_all if whole is None else whole
        self._send(0, parts[0], self.own[0], 0, p.right)
        self._send(3, parts[1], self.own[1], 3, p.left)
        self._send(1, parts[1], self.own[1], 1, p.right)
        self._send(2, parts[0], self.own[0], 2, p.left)
        self._send(6, whole, self.own_all, 6, p.sib)

    def recv(self, *which):
        for k in which:
            ref = self.regions[k]
            remote(ref, ref, self.ssem.at[k], self.rsem.at[k], self.p.sib).wait_recv()

    def _forward_only(self, *which):
        for k in which:
            self._send(7 + k, self.regions[k], self.regions[k], 7 + k, self.p.sib)

    def _forward(self, *which):
        self.recv(*which)
        self._forward_only(*which)

    def first(self):
        self.recv(0, 3)
        self._send(4, self.regions[0], self.regions[0], 4, self.p.right)
        self._send(5, self.regions[3], self.regions[3], 5, self.p.left)
        self._forward_only(0, 3)

    def second(self):
        self._forward(1, 2)

    def third(self):
        self._forward(4, 5)

    def sibling(self):
        self.recv(6)

    def sibling_near(self):
        self.recv(7, 8, 9, 10)

    def sibling_far(self):
        self.recv(11, 12)

    def finish(self):
        for k in range(13):
            ref = self.own_all if k == 6 else self.own[0]
            remote(ref, ref, self.ssem.at[k], self.rsem.at[k], self.p.sib).wait_send()


class Share:
    def __init__(self, place, full, rows, ssem, rsem):
        self.p, self.full, self.rows, self.ssem, self.rsem = place, full, rows, ssem, rsem

    def at(self, part, h=None, other=False):
        core = 1 - self.p.core if other else self.p.core
        if h is None:
            return self.full.at[:, core, part]
        return self.full.at[:, core, part, pl.ds(h * self.rows, self.rows)]

    def _send(self, k, ref, **to):
        pltpu.make_async_remote_copy(src_ref=ref, dst_ref=ref, send_sem=self.ssem.at[k], recv_sem=self.rsem.at[k],
                                     device_id=to, device_id_type=MESH).start()

    def _recv(self, k, ref):
        remote(ref, ref, self.ssem.at[k], self.rsem.at[k], self.p.sib).wait_recv()

    def start(self):
        p = self.p
        self._send(0, self.at(p.part), dp=p.group_z)
        self._send(1, self.at(p.part), dp=p.group_y)

    def relay(self):
        p = self.p
        self._recv(0, self.at(p.part_z))
        self._send(2, self.at(p.part_z, 0), dp=p.group_y)
        self._recv(1, self.at(p.part_y))
        self._send(3, self.at(p.part_y, 1), dp=p.group_z)
        self._send(4, self.at(p.part_z), tp=p.sib)
        self._send(5, self.at(p.part_y), tp=p.sib)

    def forward(self):
        p = self.p
        for h in (0, 1):
            self._recv(2 + h, self.at(p.part_d, h))
            self._send(6 + h, self.at(p.part_d, h), tp=p.sib)

    def finish(self):
        p = self.p
        for k, h in enumerate((None, None, 0, 0, None, None, 0, 0)):
            ref = self.at(p.part, h)
            remote(ref, ref, self.ssem.at[k], self.rsem.at[k], p.sib).wait_send()
        self._recv(4, self.at(p.part_z, None, True))
        self._recv(5, self.at(p.part_y, None, True))
        self._recv(6, self.at(p.part_d, 0, True))
        self._recv(7, self.at(p.part_d, 1, True))


class Exchange:
    def __init__(self, place, block, src, dst, relays, ssem, rsem):
        self.p, self.block, self.src, self.dst, self.relays, self.ssem, self.rsem = place, block, src, dst, relays, ssem, rsem

    def _send(self, sem, src, dst, rsem, to):
        remote(src, dst, self.ssem.at[sem], self.rsem.at[rsem], to).start()

    def part(self, chip, core):
        return self.src.at[rows_of((chip * 2 + core) * self.block, self.block)]

    def start(self):
        p = self.p
        slot = self.dst.at[p.me]
        self._send(0, self.part(p.chip_o, 0), self.relays.at[0], 0, p.right)
        self._send(1, self.part(p.chip_o, 1), self.relays.at[1], 1, p.left)
        for core in (0, 1):
            self._send(2 + core, self.part(p.chip_r, core), slot, 2 + p.core, p.chip_r * 2 + core)
            self._send(4 + core, self.part(p.chip_l, core), slot, 4 + p.core, p.chip_l * 2 + core)
        self._send(8, self.part(p.chip, 1 - p.core), slot, 8, p.sib)
        self.dst[p.me] = self.src[rows_of(p.me * self.block, self.block), :]

    def _recv(self, k, ref):
        remote(ref, ref, self.ssem.at[k], self.rsem.at[k], self.p.sib).wait_recv()

    def relay(self):
        p = self.p
        self._recv(0, self.relays.at[0])
        self._send(6, self.relays.at[0], self.dst.at[p.left], 6 + p.core, p.chip_r * 2)
        self._recv(1, self.relays.at[1])
        self._send(7, self.relays.at[1], self.dst.at[p.right], 6 + p.core, p.chip_l * 2 + 1)

    def recv(self):
        p = self.p
        for core in (0, 1):
            self._recv(2 + core, self.dst.at[p.chip_l * 2 + core])
            self._recv(4 + core, self.dst.at[p.chip_r * 2 + core])
            self._recv(6 + core, self.dst.at[p.chip_o * 2 + core])
        self._recv(8, self.dst.at[p.sib])

    def finish(self):
        for k in range(9):
            ref = self.relays.at[0]
            remote(ref, ref, self.ssem.at[k], self.rsem.at[k], self.p.sib).wait_send()


class Scatter:
    def __init__(self, place, block, src, d2d, sums, top, bot, from_l, from_r, ssem, rsem):
        self.__dict__.update(locals())
        self.half = block // 2

    def rows(self, chip, core, h=None):
        row = (chip * 2 + core) * self.block
        return rows_of(row, self.block) if h is None else rows_of(row + h * self.half, self.half)

    def _send(self, k, src, dst, to):
        remote(src, dst, self.ssem.at[k], self.rsem.at[k], to).start()

    def _recv(self, k, ref):
        remote(ref, ref, self.ssem.at[k], self.rsem.at[k], self.place.sib).wait_recv()

    def chip_send(self):
        p = self.place
        for k, chip in enumerate((p.chip_o, p.chip_r, p.chip_l, p.chip)):
            self._send(k, self.src.at[self.rows(chip, 1 - p.core)], self.d2d.at[k], p.sib)

    def far(self):
        p, half = self.place, self.half
        self._recv(0, self.d2d.at[0])
        self.sums[0] = self.src[self.rows(p.chip_o, p.core), :] + self.d2d[0]
        self._send(4, self.sums.at[0, pl.ds(0, half)], self.top, p.right)
        self._send(5, self.sums.at[0, pl.ds(half, half)], self.bot, p.left)

    def near_half(self, k, h, chip, extra, dst, sem, to):
        rows = pl.ds(h * self.half, self.half)
        total = self.src[self.rows(chip, self.place.core, h), :] + self.d2d[k, rows, :]
        self.sums[k, rows, :] = total if extra is None else total + extra[...]
        self._send(sem, self.sums.at[k, rows], dst.at[rows], to)

    def near_first(self):
        p = self.place
        self._recv(1, self.d2d.at[1])
        self.near_half(1, 1, p.chip_r, None, self.from_l, 6, p.right)
        self._recv(2, self.d2d.at[2])
        self.near_half(2, 0, p.chip_l, None, self.from_r, 8, p.left)

    def near_second(self):
        p = self.place
        self._recv(4, self.top)
        self.near_half(1, 0, p.chip_r, self.top, self.from_l, 7, p.right)
        self._recv(5, self.bot)
        self.near_half(2, 1, p.chip_l, self.bot, self.from_r, 9, p.left)

    def last(self):
        p, half = self.place, self.half
        self._recv(3, self.d2d.at[3])
        for k, ref, h in ((6, self.from_l, 1), (7, self.from_l, 0), (8, self.from_r, 0), (9, self.from_r, 1)):
            self._recv(k, ref.at[pl.ds(h * half, half)])
        return self.src[self.rows(p.chip, p.core), :] + self.d2d[3] + self.from_l[...] + self.from_r[...]

    def finish(self):
        for k in range(10):
            ref = self.d2d.at[0] if k < 4 else self.top
            remote(ref, ref, self.ssem.at[k], self.rsem.at[k], self.place.sib).wait_send()


def block_kernel(size, stride, norm_ref, pos_ref, freq_ref, x_hbm, dout_hbm, wq_hbm, wk_hbm, wv_hbm, wo_hbm,
                 out_ref, dx_ref, dwo_ref, dwq_ref, dw_ref, act_full, dkv_full, wo_full, wq_full,
                 x_ref, dout_ref, gain_ref, big, wbuf, wo, wqt, q_ref, k_ref, v_ref, o_ref, dq_ref, dkv_ref, o_all, dq_all,
                 relay_o, relay_q, lse_ref, cos_ref, sin_ref, m_scr, l_scr, acc,
                 d2d, sums, top, bot, from_l, from_r, wide, dw_me, dw_all, lsem,
                 ss_a, rs_a, ss_d, rs_d, ss_wo, rs_wo, ss_wq, rs_wq, ss_kv, rs_kv, ss_yo, rs_yo, ss_yq, rs_yq,
                 ss_o, rs_o, ss_q, rs_q, ss_r, rs_r, ss_w, rs_w):
    p = Place(size, stride)
    block, width = x_ref.shape
    seq, head = q_ref.shape
    chips = size // 2
    half = block // 2
    parts, part_rows = wo.shape[:2]
    scale = head ** -0.5
    wo_rows = lambda: wo[...].reshape(head, width)

    barrier = pltpu.get_barrier_semaphore()
    peers = [lax.rem(p.me + d, size) for d in range(1, size)]
    for to in [{'tp': peer} for peer in peers] + [{'dp': p.group_z}, {'dp': p.group_y}]:
        pl.semaphore_signal(barrier, inc=1, device_id=to, device_id_type=MESH)

    load_x, load_wq, load_wo, load_dout, *load_kv = [pltpu.make_async_copy(src, dst, lsem.at[i]) for i, (src, dst) in enumerate(
        ((x_hbm, x_ref), (wq_hbm, wbuf.at[0]), (wo_hbm, wo), (dout_hbm, dout_ref), (wk_hbm, wbuf.at[1]), (wv_hbm, wbuf.at[2])))]
    for copy in (load_x, load_wq, load_wo, load_dout, *load_kv):
        copy.start()
    lanes = 128
    groups = [slice(t * lanes, (t + 1) * lanes) for t in range(width // lanes)]
    for t, cols in enumerate(groups):
        gain_ref[:, cols] = 1.0 + norm_ref[t:t + 1, :]

    def weight_at(full):
        quarter = part_rows // 2

        def at(chip, core, h):
            if h is None:
                return full.at[chip, core, p.part]
            return full.at[chip, core, p.part, pl.ds(h * quarter, quarter)]
        return at

    def rows_at(full):
        def at(chip, core, h):
            row = (chip * 2 + core) * block
            return full.at[rows_of(row, block) if h is None else rows_of(row + h * half, half)]
        return at

    def grad_at(chip, core, h):
        return big.at[chip, core] if h is None else big.at[chip, core, pl.ds(h * (parts // 2), parts // 2)]

    act = Gather(p, rows_at(act_full), ss_a, rs_a)
    grad = Gather(p, grad_at, ss_d, rs_d)
    wo_g = Gather(p, weight_at(wo_full), ss_wo, rs_wo)
    wq_g = Gather(p, weight_at(wq_full), ss_wq, rs_wq)
    kv_g = Gather(p, rows_at(dkv_full), ss_kv, rs_kv)
    wo_s = Share(p, wo_full, part_rows // 2, ss_yo, rs_yo)
    wq_s = Share(p, wq_full, part_rows // 2, ss_yq, rs_yq)
    o_x = Exchange(p, block, o_ref, o_all, relay_o, ss_o, rs_o)
    dq_x = Exchange(p, block, dq_ref, dq_all, relay_q, ss_q, rs_q)
    kv_r = Scatter(p, block, dkv_ref, d2d, sums, top, bot, from_l, from_r, ss_r, rs_r)

    def start_weight(g, shard, src, sem):
        quarter = part_rows // 2
        g.start([src.at[p.part, pl.ds(h * quarter, quarter)] for h in (0, 1)], src.at[p.part])
        own = pltpu.make_async_copy(shard.at[p.part], g.own_all, lsem.at[sem])
        own.start()
        return own

    pl.semaphore_wait(barrier, size + 1)
    load_wo.wait()
    own_wo = start_weight(wo_g, wo, wo_hbm, 6)
    load_wq.wait()

    @pl.loop(0, width // COLS)
    def _(n):
        rows = pl.ds(pl.multiple_of(n * COLS, COLS), COLS)
        flipped = wbuf[0, rows, :].T
        for g in range(parts):
            wqt[g, :, rows] = flipped[g * part_rows:(g + 1) * part_rows, :]
    own_wq = start_weight(wq_g, wqt, wqt, 7)

    load_x.wait()

    @pl.loop(0, block // 64)
    def _(n):
        rows = pl.ds(pl.multiple_of(n * 64, 64), 64)
        x_f = x_ref[rows, :].astype(F32)
        inv = lax.rsqrt(jnp.mean(x_f * x_f, axis=-1, keepdims=True) + 1e-6)
        act_full[rows_of(p.me * block + n * 64, 64), :] = (x_f * inv * gain_ref[...]).astype(BF16)

    for g in (wo_g, wq_g):
        g.first()
    act.start()

    @pl.loop(0, seq // lanes)
    def _(n):
        rows = pl.ds(pl.multiple_of(n * lanes, lanes), lanes)
        angle = jnp.broadcast_to(pos_ref[:, rows].astype(F32), (lanes, lanes)).T * freq_ref[...]
        cos_ref[rows, :] = jnp.cos(angle)
        sin_ref[rows, :] = jnp.sin(angle)

    load_dout.wait()
    big[p.chip, p.core] = dout_ref[...]
    for copy in load_kv:
        copy.wait()

    def project(first, second):
        @pl.loop(0, 2)
        def _(n):
            rows = rows_of((first + n * (second - first)) * block, block)
            a = act_full[rows, :]
            cos_t, sin_t = cos_ref[rows, :], sin_ref[rows, :]
            query = dot_nn(a, wbuf[0]).astype(BF16).astype(F32)
            q_ref[rows, :] = (rope(query, cos_t, sin_t) * scale).astype(BF16)
            key = dot_nn(a, wbuf[1]).astype(BF16).astype(F32)
            k_ref[rows, :] = rope(key, cos_t, sin_t).astype(BF16)
            v_ref[rows, :] = dot_nn(a, wbuf[2]).astype(BF16)

    for g, s, own in ((wo_g, wo_s, own_wo), (wq_g, wq_s, own_wq)):
        g.second()
        g.third()
        own.wait()
        s.start()

    act.sibling()
    project(p.me, p.sib)
    act.first()
    grad.start([dout_ref.at[pl.ds(h * (parts // 2), parts // 2)] for h in (0, 1)], dout_ref)
    act.second()
    project(p.left, p.right)
    act.sibling_near()
    project(p.chip_l * 2 + 1 - p.core, p.chip_r * 2 + 1 - p.core)
    act.third()
    act.sibling_far()
    project(p.chip_o * 2 + p.core, p.chip_o * 2 + 1 - p.core)

    row_ids = lax.broadcasted_iota(jnp.int32, (TILE, TILE), 0)
    col_ids = lax.broadcasted_iota(jnp.int32, (TILE, TILE), 1)

    def tile_rows(j):
        return pl.ds(pl.multiple_of(j * TILE, TILE), TILE)

    def lane_groups(v):
        return [v[:, t * lanes:(t + 1) * lanes] for t in range(TILE // lanes)]

    def spread(v):
        return jnp.concatenate([v] * (TILE // lanes), axis=-1)

    diagonal = row_ids >= col_ids

    @pl.loop(0, seq // TILE)
    def _(i):
        rows = tile_rows(i)
        m_scr[...] = jnp.full(m_scr.shape, -1e30, F32)

        def score(j, s):
            dkv_ref[tile_rows(j), :] = s
            m_scr[...] = functools.reduce(jnp.maximum, lane_groups(s), m_scr[...])

        @pl.loop(0, i)
        def _(j):
            score(j, dot_nt(q_ref[rows, :], k_ref[tile_rows(j), :]))

        score(i, jnp.where(diagonal, dot_nt(q_ref[rows, :], k_ref[rows, :]), -1e30))
        m_scr[...] = jnp.broadcast_to(jnp.max(m_scr[...], axis=-1, keepdims=True), m_scr.shape)
        l_scr[...] = jnp.zeros(l_scr.shape, F32)
        acc[...] = jnp.zeros(acc.shape, F32)

        @pl.loop(0, i + 1)
        def _(j):
            prob = jnp.exp(dkv_ref[tile_rows(j), :] - spread(m_scr[...]))
            l_scr[...] = functools.reduce(jnp.add, lane_groups(prob), l_scr[...])
            acc[...] += dot_nn(prob.astype(BF16), v_ref[tile_rows(j), :])

        total = jnp.sum(l_scr[...], axis=-1, keepdims=True)
        lse_ref[rows, :] = m_scr[...] + jnp.log(total)
        o_ref[rows, :] = (acc[...] / total).astype(BF16)

    dkv_ref[...] = jnp.zeros(dkv_ref.shape, F32)

    def backward(first, second, count):
        @pl.loop(0, count)
        def _(n):
            i = first + n * (second - first)
            rows = tile_rows(i)
            do = dot_nt(big[i].reshape(TILE, width), wo_rows()).astype(BF16)
            row_dot = jnp.sum(do.astype(F32) * o_ref[rows, :].astype(F32), axis=-1, keepdims=True)
            m_scr[...] = jnp.broadcast_to(row_dot, m_scr.shape)
            acc[...] = jnp.zeros(acc.shape, F32)
            q = q_ref[rows, :]

            def inner(j, masked):
                cols = tile_rows(j)
                prob = jnp.exp(dot_nt(q, k_ref[cols, :]) - spread(lse_ref[rows, :]))
                if masked:
                    prob = jnp.where(diagonal, prob, 0.0)
                dkv_ref[cols, head:] += dot_tn(prob.astype(BF16), do)
                ds = (prob * (dot_nt(do, v_ref[cols, :]) - spread(m_scr[...]))).astype(BF16)
                dkv_ref[cols, :head] += dot_tn(ds, q)
                acc[...] += dot_nn(ds, k_ref[cols, :])

            @pl.loop(0, i)
            def _(j):
                inner(j, False)
            inner(i, True)

            dq_ref[rows, :] = rope(acc[...] * scale, cos_ref[rows, :], -sin_ref[rows, :]).astype(BF16)

    grad.sibling()
    backward(p.chip, p.chip, 1)
    grad.first()
    o_x.start()
    for s in (wo_s, wq_s):
        s.relay()
    act.finish()

    def strip(n):
        return pl.ds(pl.multiple_of(n * STRIP, STRIP), STRIP)

    @pl.loop(0, width // STRIP)
    def _(i):
        @pl.loop(0, i + 1)
        def _(j):
            upper, lower = act_full[strip(j), strip(i)], act_full[strip(i), strip(j)]
            act_full[strip(i), strip(j)] = upper.T
            act_full[strip(j), strip(i)] = lower.T

    grad.second()
    grad.sibling_near()
    backward(p.chip_l, p.chip_r, 2)
    grad.third()
    grad.sibling_far()
    backward(p.chip_o, p.chip_o, 1)

    kv_r.chip_send()
    o_x.relay()
    kv_r.far()
    kv_r.near_first()
    for s in (wo_s, wq_s):
        s.forward()

    def col_tiles(fn):
        @pl.loop(0, width // COLS)
        def _(n):
            fn(pl.ds(pl.multiple_of(n * COLS, COLS), COLS))

    def big_cols(cols):
        return big[:, :, :, :, cols].reshape(seq, COLS)

    def weight_o(cols):
        dwo_ref[:, cols] = dot_tn(o_ref[...], big_cols(cols))
    col_tiles(weight_o)

    kv_r.near_second()
    dq_x.start()
    grad.finish()
    wo_g.sibling()
    wo_g.sibling_near()
    wo_g.sibling_far()
    wo_s.finish()
    load_wo = pltpu.make_async_copy(wo_full, big, lsem.at[2])
    load_wo.start()

    def weight_q(cols):
        dwq_ref[cols, :] = dot_nn(act_full[cols, :], dq_ref[...])
    col_tiles(weight_q)
    o_x.recv()
    load_wo.wait()

    def finish_out(cols):
        total = dot_nn(jnp.concatenate([o_all[h] for h in range(size)], axis=-1), big_cols(cols))
        out_ref[:, cols] = (x_ref[:, cols].astype(F32) + total).astype(BF16)
    col_tiles(finish_out)

    wq_g.sibling()
    wq_g.sibling_near()
    wq_g.sibling_far()
    wq_s.finish()
    load_wq = pltpu.make_async_copy(wq_full, big, lsem.at[3])
    load_wq.start()

    own = rows_of(p.me * block, block)
    total = kv_r.last()
    dkv_full[own, :head] = rope(total[:, :head], cos_ref[own, :], -sin_ref[own, :]).astype(BF16)
    dkv_full[own, head:] = total[:, head:].astype(BF16)
    dq_x.relay()
    kv_g.start()
    dq_x.recv()
    load_wq.wait()

    def finish_da(cols):
        total = dot_nn(jnp.concatenate([dq_all[h] for h in range(size)], axis=-1), big_cols(cols))
        wide[:, cols] = (total + dot_nt(dkv_full[own, :head], wbuf[1, cols, :])
                         + dot_nt(dkv_full[own, head:], wbuf[2, cols, :]))
    col_tiles(finish_da)
    kv_g.first()

    dw_me[...] = jnp.zeros(dw_me.shape, F32)
    sub = 32

    @pl.loop(0, block // sub)
    def _(n):
        rows = pl.ds(pl.multiple_of(n * sub, sub), sub)
        x_f = x_ref[rows, :].astype(F32)
        inv = lax.rsqrt(jnp.mean(x_f * x_f, axis=-1, keepdims=True) + 1e-6)
        normed = x_f * inv
        da = wide[rows, :]
        dw_me[...] += jnp.sum(da * normed, axis=0, keepdims=True)
        gn = da * gain_ref[...]
        per = part_rows // sub
        dout = dout_ref[n // per, pl.ds(pl.multiple_of(lax.rem(n, per) * sub, sub), sub), :].astype(F32)
        dx_ref[rows, :] = (dout + inv * (gn - normed * jnp.mean(gn * normed, axis=-1, keepdims=True))).astype(BF16)

    for t, cols in enumerate(groups):
        dw_all[p.me, t:t + 1, :] = dw_me[:, cols]
    for d in range(1, size):
        remote(dw_all.at[p.me], dw_all.at[p.me], ss_w.at[d], rs_w.at[d], peers[d - 1]).start()
    kv_g.second()
    kv_g.third()
    for d in range(1, size):
        source = dw_all.at[lax.rem(p.me + size - d, size)]
        remote(source, source, ss_w.at[d], rs_w.at[d], p.sib).wait_recv()
    dw_ref[...] = jnp.sum(dw_all[...], axis=0)
    kv_g.sibling()
    kv_g.sibling_near()
    kv_g.sibling_far()

    for d in range(1, size):
        remote(dw_all.at[0], dw_all.at[0], ss_w.at[d], rs_w.at[d], p.sib).wait_send()
    for g in (wo_g, wq_g, kv_g, kv_r, o_x, dq_x):
        g.finish()


def weight_kernel(out_in, dx_in, dwo_in, dwq_in, dw_in, a_ref, dkv_ref,
                  dwk_ref, dwv_ref, out_ref, dx_ref, dwo_ref, dwq_ref, dw_ref):
    step = pl.program_id(0)
    head = dwk_ref.shape[1]

    def part(rows):
        return pl.ds(pl.multiple_of(step * rows, rows), rows)
    for src, dst in ((out_in, out_ref), (dx_in, dx_ref), (dwo_in, dwo_ref), (dwq_in, dwq_ref)):
        dst[...] = src[part(dst.shape[0]), :]
    dw_ref[...] = dw_in[...]
    a = a_ref[part(dwk_ref.shape[0]), :]
    dwk_ref[...] = dot_nn(a, dkv_ref[:, :head])
    dwv_ref[...] = dot_nn(a, dkv_ref[:, head:])


def local_block(size, stride, hidden, positions, norm_w, w_query, w_key, w_value, w_out, grad_out):
    _, block, width = hidden.shape
    seq = positions.shape[1]
    head = w_key.shape[1]
    half = head // 2
    chips, parts = size // 2, 4
    part_rows = block // parts
    lanes = 128
    x, dout = hidden[0], grad_out[0].reshape(parts, part_rows, width)
    inv_freq = (10000.0 ** (-2.0 * np.arange(half) / head)).astype(np.float32)[None, :]
    vm = pl.BlockSpec(memory_space=pltpu.VMEM)
    hbm = pl.BlockSpec(memory_space=pl.ANY)
    dma = pltpu.SemaphoreType.DMA
    shape = jax.ShapeDtypeStruct
    V = pltpu.VMEM
    full = (chips, 2, parts, part_rows, width)
    kv = 2 * head
    small = (width // lanes, lanes)

    *results, _, _ = pl.pallas_call(
        functools.partial(block_kernel, size, stride),
        out_shape=[V((block, width), BF16), V((block, width), BF16), V((head, width), F32), V((width, head), F32), V(small, F32),
                   V((seq, width), BF16), V((seq, kv), BF16), shape(full, BF16), shape(full, BF16)],
        in_specs=[vm] * 3 + [hbm] * 6,
        out_specs=[vm] * 7 + [hbm] * 2,
        scratch_shapes=[V((block, width), BF16), V((parts, part_rows, width), BF16), V((1, width), F32),
                        V(full, BF16), V((3, width, head), BF16), V((parts, part_rows, width), BF16),
                        V((parts, part_rows, width), BF16)] + [V((seq, head), BF16)] * 5
        + [V((seq, kv), F32), V((size, block, head), BF16), V((size, block, head), BF16),
           V((2, block, head), BF16), V((2, block, head), BF16), V((seq, 128), F32), V((seq, half), F32), V((seq, half), F32),
           V((TILE, 128), F32), V((TILE, 128), F32), V((TILE, head), F32),
           V((4, block, kv), F32), V((3, block, kv), F32), V((block // 2, kv), F32), V((block // 2, kv), F32),
           V((block, kv), F32), V((block, kv), F32), V((head, width), F32), V((1, width), F32),
           V((size, width // 128, 128), F32), dma((8,))]
        + [dma((13,))] * 10 + [dma((8,))] * 4 + [dma((9,))] * 4 + [dma((10,))] * 2 + [dma((size,))] * 2,
        compiler_params=pltpu.CompilerParams(collective_id=0, has_side_effects=True, vmem_limit_bytes=VMEM_LIMIT - KEPT),
        name='attention_block',
    )(norm_w.reshape(width // lanes, lanes), positions, inv_freq, x, dout, w_query, w_key, w_value,
      w_out.reshape(parts, part_rows, width))

    steps = width // COLS
    whole = lambda *dims: pl.BlockSpec(dims, lambda n: (0, 0))
    rows = lambda *dims: pl.BlockSpec(dims, lambda n: (n, 0))
    passed = [rows(block // steps, width), rows(block // steps, width), rows(head // steps, width), rows(width // steps, head),
              whole(*small)]
    dwk, dwv, out, dx, dwo, dwq, dw = pl.pallas_call(
        weight_kernel,
        grid=(steps,),
        out_shape=[shape((width, head), F32)] * 2 + [shape((block, width), BF16)] * 2
        + [shape((head, width), F32), shape((width, head), F32), shape(small, F32)],
        in_specs=[vm] * 7,
        out_specs=[rows(width // steps, head)] * 2 + passed,
        compiler_params=pltpu.CompilerParams(vmem_limit_bytes=VMEM_LIMIT - KEPT),
        name='weight_grads',
    )(*[pltpu.with_memory_space_constraint(v, V) for v in results])
    return out[None], dx[None], dwq, dwo, dwk, dwv, dw.reshape(width)


def solution(mesh):
    specs_in = (P('dp', 'tp', None), P('dp', None), P(None), P(None, 'tp'), P(None, None), P(None, None), P('tp', None), P('dp', 'tp', None))
    specs_out = (P('dp', 'tp', None), P('dp', 'tp', None), P('dp', 'tp'), P(('dp', 'tp'), None), P('dp', None), P('dp', None), P('dp'))
    column = [tuple(d.coords) for d in mesh.devices[:, 0]]
    stride = sum(c[1] == column[0][1] for c in column)
    local = functools.partial(local_block, mesh.shape['tp'], stride)
    return jax.shard_map(local, mesh=mesh, in_specs=specs_in, out_specs=specs_out, check_vma=False)
```

```python
import functools

import jax
import jax.numpy as jnp
import numpy as np
from jax import lax
from jax.experimental import pallas as pl
from jax.experimental.pallas import tpu as pltpu
from jax.sharding import PartitionSpec as P

MESH = pl.DeviceIdType.MESH
F32 = jnp.float32
BF16 = jnp.bfloat16
TILE = 512
STRIP = 256
COLS = 512
VMEM_LIMIT = 63 * 1024 * 1024
KEPT = 16 * 1024 * 1024


def dot_nn(a, b):
    return lax.dot_general(a, b, (((1,), (0,)), ((), ())), preferred_element_type=F32)


def dot_nt(a, b):
    return lax.dot_general(a, b, (((1,), (1,)), ((), ())), preferred_element_type=F32)


def dot_tn(a, b):
    return lax.dot_general(a, b, (((0,), (0,)), ((), ())), preferred_element_type=F32)


def rope(u, cos_t, sin_t):
    half = u.shape[-1] // 2
    first, second = u[:, :half], u[:, half:]
    return jnp.concatenate([first * cos_t - second * sin_t, second * cos_t + first * sin_t], axis=-1)


class Place:
    def __init__(self, size, stride):
        n = size // 2
        group = lax.axis_index('dp')
        z, y = lax.rem(group, 2), lax.rem(lax.div(group, stride), 2)
        self.group_z = group + 1 - 2 * z
        self.group_y = group + stride * (1 - 2 * y)
        self.part = 2 * y + z
        self.part_z, self.part_y, self.part_d = 2 * y + 1 - z, 2 * (1 - y) + z, 3 - self.part
        self.me = lax.axis_index('tp')
        self.core = lax.rem(self.me, 2)
        self.chip = lax.div(self.me, 2)
        self.chip_r = lax.rem(self.chip + 1, n)
        self.chip_l = lax.rem(self.chip + n - 1, n)
        self.chip_o = lax.rem(self.chip + 2, n)
        self.right = self.chip_r * 2 + self.core
        self.left = self.chip_l * 2 + self.core
        self.sib = self.chip * 2 + 1 - self.core


def remote(src, dst, ssem, rsem, to):
    return pltpu.make_async_remote_copy(src_ref=src, dst_ref=dst, send_sem=ssem, recv_sem=rsem,
                                        device_id={'tp': to}, device_id_type=MESH)


def rows_of(start, size):
    return pl.ds(pl.multiple_of(start, min(size, 128)), size)


class Gather:
    def __init__(self, place, at, ssem, rsem):
        self.at, self.p, self.ssem, self.rsem = at, place, ssem, rsem
        p = place
        self.own = [at(p.chip, p.core, h) for h in (0, 1)]
        self.own_all = at(p.chip, p.core, None)
        regions = []
        for core in (p.core, 1 - p.core):
            for chip in (p.chip_l, p.chip_r, p.chip_o):
                regions += [at(chip, core, 0), at(chip, core, 1)]
        self.regions = regions[:6] + [at(p.chip, 1 - p.core, None)] + regions[6:]

    def _send(self, sem, src, dst, rsem, to):
        remote(src, dst, self.ssem.at[sem], self.rsem.at[rsem], to).start()

    def start(self, parts=None, whole=None):
        p = self.p
        parts = self.own if parts is None else parts
        whole = self.own_all if whole is None else whole
        self._send(0, parts[0], self.own[0], 0, p.right)
        self._send(3, parts[1], self.own[1], 3, p.left)
        self._send(1, parts[1], self.own[1], 1, p.right)
        self._send(2, parts[0], self.own[0], 2, p.left)
        self._send(6, whole, self.own_all, 6, p.sib)

    def recv(self, *which):
        for k in which:
            ref = self.regions[k]
            remote(ref, ref, self.ssem.at[k], self.rsem.at[k], self.p.sib).wait_recv()

    def _forward_only(self, *which):
        for k in which:
            self._send(7 + k, self.regions[k], self.regions[k], 7 + k, self.p.sib)

    def _forward(self, *which):
        self.recv(*which)
        self._forward_only(*which)

    def first(self):
        self.recv(0, 3)
        self._send(4, self.regions[0], self.regions[0], 4, self.p.right)
        self._send(5, self.regions[3], self.regions[3], 5, self.p.left)
        self._forward_only(0, 3)

    def second(self):
        self._forward(1, 2)

    def third(self):
        self._forward(4, 5)

    def sibling(self):
        self.recv(6)

    def sibling_near(self):
        self.recv(7, 8, 9, 10)

    def sibling_far(self):
        self.recv(11, 12)

    def finish(self):
        for k in range(13):
            ref = self.own_all if k == 6 else self.own[0]
            remote(ref, ref, self.ssem.at[k], self.rsem.at[k], self.p.sib).wait_send()


class Share:
    def __init__(self, place, full, rows, ssem, rsem):
        self.p, self.full, self.rows, self.ssem, self.rsem = place, full, rows, ssem, rsem

    def at(self, part, h=None, other=False):
        core = 1 - self.p.core if other else self.p.core
        if h is None:
            return self.full.at[:, core, part]
        return self.full.at[:, core, part, pl.ds(h * self.rows, self.rows)]

    def _send(self, k, ref, **to):
        pltpu.make_async_remote_copy(src_ref=ref, dst_ref=ref, send_sem=self.ssem.at[k], recv_sem=self.rsem.at[k],
                                     device_id=to, device_id_type=MESH).start()

    def _recv(self, k, ref):
        remote(ref, ref, self.ssem.at[k], self.rsem.at[k], self.p.sib).wait_recv()

    def start(self):
        p = self.p
        self._send(0, self.at(p.part), dp=p.group_z)
        self._send(1, self.at(p.part), dp=p.group_y)

    def relay(self):
        p = self.p
        self._recv(0, self.at(p.part_z))
        self._send(2, self.at(p.part_z, 0), dp=p.group_y)
        self._recv(1, self.at(p.part_y))
        self._send(3, self.at(p.part_y, 1), dp=p.group_z)
        self._send(4, self.at(p.part_z), tp=p.sib)
        self._send(5, self.at(p.part_y), tp=p.sib)

    def forward(self):
        p = self.p
        for h in (0, 1):
            self._recv(2 + h, self.at(p.part_d, h))
            self._send(6 + h, self.at(p.part_d, h), tp=p.sib)

    def finish(self):
        p = self.p
        for k, h in enumerate((None, None, 0, 0, None, None, 0, 0)):
            ref = self.at(p.part, h)
            remote(ref, ref, self.ssem.at[k], self.rsem.at[k], p.sib).wait_send()
        self._recv(4, self.at(p.part_z, None, True))
        self._recv(5, self.at(p.part_y, None, True))
        self._recv(6, self.at(p.part_d, 0, True))
        self._recv(7, self.at(p.part_d, 1, True))


class Exchange:
    def __init__(self, place, block, src, dst, relays, ssem, rsem):
        self.p, self.block, self.src, self.dst, self.relays, self.ssem, self.rsem = place, block, src, dst, relays, ssem, rsem

    def _send(self, sem, src, dst, rsem, to):
        remote(src, dst, self.ssem.at[sem], self.rsem.at[rsem], to).start()

    def part(self, chip, core):
        return self.src.at[rows_of((chip * 2 + core) * self.block, self.block)]

    def start(self):
        p = self.p
        slot = self.dst.at[p.me]
        self._send(0, self.part(p.chip_o, 0), self.relays.at[0], 0, p.right)
        self._send(1, self.part(p.chip_o, 1), self.relays.at[1], 1, p.left)
        for core in (0, 1):
            self._send(2 + core, self.part(p.chip_r, core), slot, 2 + p.core, p.chip_r * 2 + core)
            self._send(4 + core, self.part(p.chip_l, core), slot, 4 + p.core, p.chip_l * 2 + core)
        self._send(8, self.part(p.chip, 1 - p.core), slot, 8, p.sib)
        self.dst[p.me] = self.src[rows_of(p.me * self.block, self.block), :]

    def _recv(self, k, ref):
        remote(ref, ref, self.ssem.at[k], self.rsem.at[k], self.p.sib).wait_recv()

    def relay(self):
        p = self.p
        self._recv(0, self.relays.at[0])
        self._send(6, self.relays.at[0], self.dst.at[p.left], 6 + p.core, p.chip_r * 2)
        self._recv(1, self.relays.at[1])
        self._send(7, self.relays.at[1], self.dst.at[p.right], 6 + p.core, p.chip_l * 2 + 1)

    def recv(self):
        p = self.p
        for core in (0, 1):
            self._recv(2 + core, self.dst.at[p.chip_l * 2 + core])
            self._recv(4 + core, self.dst.at[p.chip_r * 2 + core])
            self._recv(6 + core, self.dst.at[p.chip_o * 2 + core])
        self._recv(8, self.dst.at[p.sib])

    def finish(self):
        for k in range(9):
            ref = self.relays.at[0]
            remote(ref, ref, self.ssem.at[k], self.rsem.at[k], self.p.sib).wait_send()


class Scatter:
    def __init__(self, place, block, src, d2d, sums, top, bot, from_l, from_r, ssem, rsem):
        self.__dict__.update(locals())
        self.half = block // 2

    def rows(self, chip, core, h=None):
        row = (chip * 2 + core) * self.block
        return rows_of(row, self.block) if h is None else rows_of(row + h * self.half, self.half)

    def _send(self, k, src, dst, to):
        remote(src, dst, self.ssem.at[k], self.rsem.at[k], to).start()

    def _recv(self, k, ref):
        remote(ref, ref, self.ssem.at[k], self.rsem.at[k], self.place.sib).wait_recv()

    def chip_send(self):
        p = self.place
        for k, chip in enumerate((p.chip_o, p.chip_r, p.chip_l, p.chip)):
            self._send(k, self.src.at[self.rows(chip, 1 - p.core)], self.d2d.at[k], p.sib)

    def far(self):
        p, half = self.place, self.half
        self._recv(0, self.d2d.at[0])
        self.sums[0] = self.src[self.rows(p.chip_o, p.core), :] + self.d2d[0]
        self._send(4, self.sums.at[0, pl.ds(0, half)], self.top, p.right)
        self._send(5, self.sums.at[0, pl.ds(half, half)], self.bot, p.left)

    def near_half(self, k, h, chip, extra, dst, sem, to):
        rows = pl.ds(h * self.half, self.half)
        total = self.src[self.rows(chip, self.place.core, h), :] + self.d2d[k, rows, :]
        self.sums[k, rows, :] = total if extra is None else total + extra[...]
        self._send(sem, self.sums.at[k, rows], dst.at[rows], to)

    def near_first(self):
        p = self.place
        self._recv(1, self.d2d.at[1])
        self.near_half(1, 1, p.chip_r, None, self.from_l, 6, p.right)
        self._recv(2, self.d2d.at[2])
        self.near_half(2, 0, p.chip_l, None, self.from_r, 8, p.left)

    def near_second(self):
        p = self.place
        self._recv(4, self.top)
        self.near_half(1, 0, p.chip_r, self.top, self.from_l, 7, p.right)
        self._recv(5, self.bot)
        self.near_half(2, 1, p.chip_l, self.bot, self.from_r, 9, p.left)

    def last(self):
        p, half = self.place, self.half
        self._recv(3, self.d2d.at[3])
        for k, ref, h in ((6, self.from_l, 1), (7, self.from_l, 0), (8, self.from_r, 0), (9, self.from_r, 1)):
            self._recv(k, ref.at[pl.ds(h * half, half)])
        return self.src[self.rows(p.chip, p.core), :] + self.d2d[3] + self.from_l[...] + self.from_r[...]

    def finish(self):
        for k in range(10):
            ref = self.d2d.at[0] if k < 4 else self.top
            remote(ref, ref, self.ssem.at[k], self.rsem.at[k], self.place.sib).wait_send()


def block_kernel(size, stride, norm_hbm, pos_hbm, freq_hbm, x_hbm, dout_hbm, wq_hbm, wk_hbm, wv_hbm, wo_hbm,
                 out_ref, dx_ref, dwo_ref, dwq_ref, dw_ref, act_full, dkv_full, wo_full, wq_full,
                 norm_ref, pos_ref, freq_ref, x_ref, dout_ref, gain_ref, big, wbuf, wo, wqt, q_ref, k_ref, v_ref, o_ref, dq_ref, dkv_ref, o_all, dq_all,
                 relay_o, relay_q, lse_ref, cos_ref, sin_ref, m_scr, l_scr, acc,
                 d2d, sums, top, bot, from_l, from_r, wide, dw_me, dw_all, lsem, ssem,
                 ss_a, rs_a, ss_d, rs_d, ss_wo, rs_wo, ss_wq, rs_wq, ss_kv, rs_kv, ss_yo, rs_yo, ss_yq, rs_yq,
                 ss_o, rs_o, ss_q, rs_q, ss_r, rs_r, ss_w, rs_w):
    p = Place(size, stride)
    block, width = x_ref.shape
    seq, head = q_ref.shape
    chips = size // 2
    half = block // 2
    parts, part_rows = wo.shape[:2]
    scale = head ** -0.5
    wo_rows = lambda: wo[...].reshape(head, width)

    barrier = pltpu.get_barrier_semaphore()
    peers = [lax.rem(p.me + d, size) for d in range(1, size)]
    for to in [{'tp': peer} for peer in peers] + [{'dp': p.group_z}, {'dp': p.group_y}]:
        pl.semaphore_signal(barrier, inc=1, device_id=to, device_id_type=MESH)

    load_x, load_wq, load_wo, load_dout, *load_kv = [pltpu.make_async_copy(src, dst, lsem.at[i]) for i, (src, dst) in enumerate(
        ((x_hbm, x_ref), (wq_hbm, wbuf.at[0]), (wo_hbm, wo), (dout_hbm, dout_ref), (wk_hbm, wbuf.at[1]), (wv_hbm, wbuf.at[2])))]
    small = [pltpu.make_async_copy(src, dst, ssem.at[i]) for i, (src, dst) in enumerate(
        ((norm_hbm, norm_ref), (pos_hbm, pos_ref), (freq_hbm, freq_ref)))]
    for copy in (*small, load_x, load_wq, load_wo, load_dout, *load_kv):
        copy.start()
    for copy in small:
        copy.wait()
    lanes = 128
    groups = [slice(t * lanes, (t + 1) * lanes) for t in range(width // lanes)]
    for t, cols in enumerate(groups):
        gain_ref[:, cols] = 1.0 + norm_ref[t:t + 1, :]

    def weight_at(full):
        quarter = part_rows // 2

        def at(chip, core, h):
            if h is None:
                return full.at[chip, core, p.part]
            return full.at[chip, core, p.part, pl.ds(h * quarter, quarter)]
        return at

    def rows_at(full):
        def at(chip, core, h):
            row = (chip * 2 + core) * block
            return full.at[rows_of(row, block) if h is None else rows_of(row + h * half, half)]
        return at

    def grad_at(chip, core, h):
        return big.at[chip, core] if h is None else big.at[chip, core, pl.ds(h * (parts // 2), parts // 2)]

    act = Gather(p, rows_at(act_full), ss_a, rs_a)
    grad = Gather(p, grad_at, ss_d, rs_d)
    wo_g = Gather(p, weight_at(wo_full), ss_wo, rs_wo)
    wq_g = Gather(p, weight_at(wq_full), ss_wq, rs_wq)
    kv_g = Gather(p, rows_at(dkv_full), ss_kv, rs_kv)
    wo_s = Share(p, wo_full, part_rows // 2, ss_yo, rs_yo)
    wq_s = Share(p, wq_full, part_rows // 2, ss_yq, rs_yq)
    o_x = Exchange(p, block, o_ref, o_all, relay_o, ss_o, rs_o)
    dq_x = Exchange(p, block, dq_ref, dq_all, relay_q, ss_q, rs_q)
    kv_r = Scatter(p, block, dkv_ref, d2d, sums, top, bot, from_l, from_r, ss_r, rs_r)

    def start_weight(g, shard, src, sem):
        quarter = part_rows // 2
        g.start([src.at[p.part, pl.ds(h * quarter, quarter)] for h in (0, 1)], src.at[p.part])
        own = pltpu.make_async_copy(shard.at[p.part], g.own_all, lsem.at[sem])
        own.start()
        return own

    pl.semaphore_wait(barrier, size + 1)
    load_wo.wait()
    own_wo = start_weight(wo_g, wo, wo_hbm, 6)
    load_wq.wait()

    @pl.loop(0, width // COLS)
    def _(n):
        rows = pl.ds(pl.multiple_of(n * COLS, COLS), COLS)
        flipped = wbuf[0, rows, :].T
        for g in range(parts):
            wqt[g, :, rows] = flipped[g * part_rows:(g + 1) * part_rows, :]
    own_wq = start_weight(wq_g, wqt, wqt, 7)

    load_x.wait()

    @pl.loop(0, block // 64)
    def _(n):
        rows = pl.ds(pl.multiple_of(n * 64, 64), 64)
        x_f = x_ref[rows, :].astype(F32)
        inv = lax.rsqrt(jnp.mean(x_f * x_f, axis=-1, keepdims=True) + 1e-6)
        act_full[rows_of(p.me * block + n * 64, 64), :] = (x_f * inv * gain_ref[...]).astype(BF16)

    for g in (wo_g, wq_g):
        g.first()
    act.start()

    @pl.loop(0, seq // lanes)
    def _(n):
        rows = pl.ds(pl.multiple_of(n * lanes, lanes), lanes)
        angle = jnp.broadcast_to(pos_ref[:, rows].astype(F32), (lanes, lanes)).T * freq_ref[...]
        cos_ref[rows, :] = jnp.cos(angle)
        sin_ref[rows, :] = jnp.sin(angle)

    load_dout.wait()
    big[p.chip, p.core] = dout_ref[...]
    for copy in load_kv:
        copy.wait()

    def project(first, second):
        @pl.loop(0, 2)
        def _(n):
            rows = rows_of((first + n * (second - first)) * block, block)
            a = act_full[rows, :]
            cos_t, sin_t = cos_ref[rows, :], sin_ref[rows, :]
            query = dot_nn(a, wbuf[0]).astype(BF16).astype(F32)
            q_ref[rows, :] = (rope(query, cos_t, sin_t) * scale).astype(BF16)
            key = dot_nn(a, wbuf[1]).astype(BF16).astype(F32)
            k_ref[rows, :] = rope(key, cos_t, sin_t).astype(BF16)
            v_ref[rows, :] = dot_nn(a, wbuf[2]).astype(BF16)

    for g, s, own in ((wo_g, wo_s, own_wo), (wq_g, wq_s, own_wq)):
        g.second()
        g.third()
        own.wait()
        s.start()

    act.sibling()
    project(p.me, p.sib)
    act.first()
    grad.start([dout_ref.at[pl.ds(h * (parts // 2), parts // 2)] for h in (0, 1)], dout_ref)
    act.second()
    project(p.left, p.right)
    act.sibling_near()
    project(p.chip_l * 2 + 1 - p.core, p.chip_r * 2 + 1 - p.core)
    act.third()
    act.sibling_far()
    project(p.chip_o * 2 + p.core, p.chip_o * 2 + 1 - p.core)

    row_ids = lax.broadcasted_iota(jnp.int32, (TILE, TILE), 0)
    col_ids = lax.broadcasted_iota(jnp.int32, (TILE, TILE), 1)

    def tile_rows(j):
        return pl.ds(pl.multiple_of(j * TILE, TILE), TILE)

    def lane_groups(v):
        return [v[:, t * lanes:(t + 1) * lanes] for t in range(TILE // lanes)]

    def spread(v):
        return jnp.concatenate([v] * (TILE // lanes), axis=-1)

    diagonal = row_ids >= col_ids

    @pl.loop(0, seq // TILE)
    def _(i):
        rows = tile_rows(i)
        m_scr[...] = jnp.full(m_scr.shape, -1e30, F32)

        def score(j, s):
            dkv_ref[tile_rows(j), :] = s
            m_scr[...] = functools.reduce(jnp.maximum, lane_groups(s), m_scr[...])

        @pl.loop(0, i)
        def _(j):
            score(j, dot_nt(q_ref[rows, :], k_ref[tile_rows(j), :]))

        score(i, jnp.where(diagonal, dot_nt(q_ref[rows, :], k_ref[rows, :]), -1e30))
        m_scr[...] = jnp.broadcast_to(jnp.max(m_scr[...], axis=-1, keepdims=True), m_scr.shape)
        l_scr[...] = jnp.zeros(l_scr.shape, F32)
        acc[...] = jnp.zeros(acc.shape, F32)

        @pl.loop(0, i + 1)
        def _(j):
            prob = jnp.exp(dkv_ref[tile_rows(j), :] - spread(m_scr[...]))
            l_scr[...] = functools.reduce(jnp.add, lane_groups(prob), l_scr[...])
            acc[...] += dot_nn(prob.astype(BF16), v_ref[tile_rows(j), :])

        total = jnp.sum(l_scr[...], axis=-1, keepdims=True)
        lse_ref[rows, :] = m_scr[...] + jnp.log(total)
        o_ref[rows, :] = (acc[...] / total).astype(BF16)

    dkv_ref[...] = jnp.zeros(dkv_ref.shape, F32)

    def backward(first, second, count):
        @pl.loop(0, count)
        def _(n):
            i = first + n * (second - first)
            rows = tile_rows(i)
            do = dot_nt(big[i].reshape(TILE, width), wo_rows()).astype(BF16)
            row_dot = jnp.sum(do.astype(F32) * o_ref[rows, :].astype(F32), axis=-1, keepdims=True)
            m_scr[...] = jnp.broadcast_to(row_dot, m_scr.shape)
            acc[...] = jnp.zeros(acc.shape, F32)
            q = q_ref[rows, :]

            def inner(j, masked):
                cols = tile_rows(j)
                prob = jnp.exp(dot_nt(q, k_ref[cols, :]) - spread(lse_ref[rows, :]))
                if masked:
                    prob = jnp.where(diagonal, prob, 0.0)
                dkv_ref[cols, head:] += dot_tn(prob.astype(BF16), do)
                ds = (prob * (dot_nt(do, v_ref[cols, :]) - spread(m_scr[...]))).astype(BF16)
                dkv_ref[cols, :head] += dot_tn(ds, q)
                acc[...] += dot_nn(ds, k_ref[cols, :])

            @pl.loop(0, i)
            def _(j):
                inner(j, False)
            inner(i, True)

            dq_ref[rows, :] = rope(acc[...] * scale, cos_ref[rows, :], -sin_ref[rows, :]).astype(BF16)

    grad.sibling()
    backward(p.chip, p.chip, 1)
    grad.first()
    o_x.start()
    for s in (wo_s, wq_s):
        s.relay()
    act.finish()

    def strip(n):
        return pl.ds(pl.multiple_of(n * STRIP, STRIP), STRIP)

    @pl.loop(0, width // STRIP)
    def _(i):
        @pl.loop(0, i + 1)
        def _(j):
            upper, lower = act_full[strip(j), strip(i)], act_full[strip(i), strip(j)]
            act_full[strip(i), strip(j)] = upper.T
            act_full[strip(j), strip(i)] = lower.T

    grad.second()
    grad.sibling_near()
    backward(p.chip_l, p.chip_r, 2)
    grad.third()
    grad.sibling_far()
    backward(p.chip_o, p.chip_o, 1)

    kv_r.chip_send()
    o_x.relay()
    kv_r.far()
    kv_r.near_first()
    for s in (wo_s, wq_s):
        s.forward()

    def col_tiles(fn):
        @pl.loop(0, width // COLS)
        def _(n):
            fn(pl.ds(pl.multiple_of(n * COLS, COLS), COLS))

    def big_cols(cols):
        return big[:, :, :, :, cols].reshape(seq, COLS)

    def weight_o(cols):
        dwo_ref[:, cols] = dot_tn(o_ref[...], big_cols(cols))
    col_tiles(weight_o)

    kv_r.near_second()
    dq_x.start()
    grad.finish()
    wo_g.sibling()
    wo_g.sibling_near()
    wo_g.sibling_far()
    wo_s.finish()
    load_wo = pltpu.make_async_copy(wo_full, big, lsem.at[2])
    load_wo.start()

    def weight_q(cols):
        dwq_ref[cols, :] = dot_nn(act_full[cols, :], dq_ref[...])
    col_tiles(weight_q)
    o_x.recv()
    load_wo.wait()

    def finish_out(cols):
        total = dot_nn(jnp.concatenate([o_all[h] for h in range(size)], axis=-1), big_cols(cols))
        out_ref[:, cols] = (x_ref[:, cols].astype(F32) + total).astype(BF16)
    col_tiles(finish_out)

    wq_g.sibling()
    wq_g.sibling_near()
    wq_g.sibling_far()
    wq_s.finish()
    load_wq = pltpu.make_async_copy(wq_full, big, lsem.at[3])
    load_wq.start()

    own = rows_of(p.me * block, block)
    total = kv_r.last()
    dkv_full[own, :head] = rope(total[:, :head], cos_ref[own, :], -sin_ref[own, :]).astype(BF16)
    dkv_full[own, head:] = total[:, head:].astype(BF16)
    dq_x.relay()
    kv_g.start()
    dq_x.recv()
    load_wq.wait()

    def finish_da(cols):
        total = dot_nn(jnp.concatenate([dq_all[h] for h in range(size)], axis=-1), big_cols(cols))
        wide[:, cols] = (total + dot_nt(dkv_full[own, :head], wbuf[1, cols, :])
                         + dot_nt(dkv_full[own, head:], wbuf[2, cols, :]))
    col_tiles(finish_da)
    kv_g.first()

    dw_me[...] = jnp.zeros(dw_me.shape, F32)
    sub = 32

    @pl.loop(0, block // sub)
    def _(n):
        rows = pl.ds(pl.multiple_of(n * sub, sub), sub)
        x_f = x_ref[rows, :].astype(F32)
        inv = lax.rsqrt(jnp.mean(x_f * x_f, axis=-1, keepdims=True) + 1e-6)
        normed = x_f * inv
        da = wide[rows, :]
        dw_me[...] += jnp.sum(da * normed, axis=0, keepdims=True)
        gn = da * gain_ref[...]
        per = part_rows // sub
        dout = dout_ref[n // per, pl.ds(pl.multiple_of(lax.rem(n, per) * sub, sub), sub), :].astype(F32)
        dx_ref[rows, :] = (dout + inv * (gn - normed * jnp.mean(gn * normed, axis=-1, keepdims=True))).astype(BF16)

    for t, cols in enumerate(groups):
        dw_all[p.me, t:t + 1, :] = dw_me[:, cols]
    for d in range(1, size):
        remote(dw_all.at[p.me], dw_all.at[p.me], ss_w.at[d], rs_w.at[d], peers[d - 1]).start()
    kv_g.second()
    kv_g.third()
    for d in range(1, size):
        source = dw_all.at[lax.rem(p.me + size - d, size)]
        remote(source, source, ss_w.at[d], rs_w.at[d], p.sib).wait_recv()
    dw_ref[...] = jnp.sum(dw_all[...], axis=0)
    kv_g.sibling()
    kv_g.sibling_near()
    kv_g.sibling_far()

    for d in range(1, size):
        remote(dw_all.at[0], dw_all.at[0], ss_w.at[d], rs_w.at[d], p.sib).wait_send()
    for g in (wo_g, wq_g, kv_g, kv_r, o_x, dq_x):
        g.finish()


def weight_kernel(out_in, dx_in, dwo_in, dwq_in, dw_in, a_ref, dkv_ref,
                  out_ref, dx_ref, dwo_ref, dwq_ref, dw_ref, dwk_ref, dwv_ref, dwk, dwv, sems):
    head = dwk.shape[1]
    copies = []

    def put(src, dst):
        copies.append(pltpu.make_async_copy(src, dst, sems.at[len(copies)]))
        copies[-1].start()

    tiles = [pl.ds(row, STRIP) for row in range(0, dwk.shape[0], STRIP)]
    for src, dst in ((out_in, out_ref), (dx_in, dx_ref), (dwo_in, dwo_ref), (dwq_in, dwq_ref), (dw_in, dw_ref)):
        put(src, dst)
    for rows in tiles:
        a = a_ref[rows, :]
        for grad, cols, dst in ((dwk, slice(0, head), dwk_ref), (dwv, slice(head, 2 * head), dwv_ref)):
            grad[rows, :] = dot_nn(a, dkv_ref[:, cols])
            put(grad.at[rows], dst.at[rows])
    for copy in copies:
        copy.wait()


def local_block(size, stride, hidden, positions, norm_w, w_query, w_key, w_value, w_out, grad_out):
    _, block, width = hidden.shape
    seq = positions.shape[1]
    head = w_key.shape[1]
    half = head // 2
    chips, parts = size // 2, 4
    part_rows = block // parts
    lanes = 128
    x, dout = hidden[0], grad_out[0].reshape(parts, part_rows, width)
    inv_freq = (10000.0 ** (-2.0 * np.arange(half) / head)).astype(np.float32)[None, :]
    vm = pl.BlockSpec(memory_space=pltpu.VMEM)
    hbm = pl.BlockSpec(memory_space=pl.ANY)
    dma = pltpu.SemaphoreType.DMA
    shape = jax.ShapeDtypeStruct
    V = pltpu.VMEM
    full = (chips, 2, parts, part_rows, width)
    kv = 2 * head
    small = (width // lanes, lanes)

    *results, _, _ = pl.pallas_call(
        functools.partial(block_kernel, size, stride),
        out_shape=[V((block, width), BF16), V((block, width), BF16), V((head, width), F32), V((width, head), F32), V(small, F32),
                   V((seq, width), BF16), V((seq, kv), BF16), shape(full, BF16), shape(full, BF16)],
        in_specs=[hbm] * 9,
        out_specs=[vm] * 7 + [hbm] * 2,
        scratch_shapes=[V(small, F32), V((1, seq), jnp.int32), V((1, half), F32),
                        V((block, width), BF16), V((parts, part_rows, width), BF16), V((1, width), F32),
                        V(full, BF16), V((3, width, head), BF16), V((parts, part_rows, width), BF16),
                        V((parts, part_rows, width), BF16)] + [V((seq, head), BF16)] * 5
        + [V((seq, kv), F32), V((size, block, head), BF16), V((size, block, head), BF16),
           V((2, block, head), BF16), V((2, block, head), BF16), V((seq, 128), F32), V((seq, half), F32), V((seq, half), F32),
           V((TILE, 128), F32), V((TILE, 128), F32), V((TILE, head), F32),
           V((4, block, kv), F32), V((3, block, kv), F32), V((block // 2, kv), F32), V((block // 2, kv), F32),
           V((block, kv), F32), V((block, kv), F32), V((head, width), F32), V((1, width), F32),
           V((size, width // 128, 128), F32), dma((8,)), dma((3,))]
        + [dma((13,))] * 10 + [dma((8,))] * 4 + [dma((9,))] * 4 + [dma((10,))] * 2 + [dma((size,))] * 2,
        compiler_params=pltpu.CompilerParams(collective_id=0, has_side_effects=True, vmem_limit_bytes=VMEM_LIMIT - KEPT),
        name='attention_block',
    )(norm_w.reshape(width // lanes, lanes), positions, inv_freq, x, dout, w_query, w_key, w_value,
      w_out.reshape(parts, part_rows, width))

    out, dx, dwo, dwq, dw, dwk, dwv = pl.pallas_call(
        weight_kernel,
        out_shape=[shape((block, width), BF16)] * 2 + [shape((head, width), F32), shape((width, head), F32), shape(small, F32)]
        + [shape((width, head), F32)] * 2,
        in_specs=[vm] * 7,
        out_specs=[hbm] * 7,
        scratch_shapes=[V((width, head), F32), V((width, head), F32), dma((5 + 2 * (width // STRIP),))],
        compiler_params=pltpu.CompilerParams(vmem_limit_bytes=VMEM_LIMIT - KEPT),
        name='weight_grads',
    )(*[pltpu.with_memory_space_constraint(v, V) for v in results])
    return out[None], dx[None], dwq, dwo, dwk, dwv, dw.reshape(width)


def solution(mesh):
    specs_in = (P('dp', 'tp', None), P('dp', None), P(None), P(None, 'tp'), P(None, None), P(None, None), P('tp', None), P('dp', 'tp', None))
    specs_out = (P('dp', 'tp', None), P('dp', 'tp', None), P('dp', 'tp'), P(('dp', 'tp'), None), P('dp', None), P('dp', None), P('dp'))
    column = [tuple(d.coords) for d in mesh.devices[:, 0]]
    stride = sum(c[1] == column[0][1] for c in column)
    local = functools.partial(local_block, mesh.shape['tp'], stride)
    return jax.shard_map(local, mesh=mesh, in_specs=specs_in, out_specs=specs_out, check_vma=False)
```

```python
import functools

import jax
import jax.numpy as jnp
import numpy as np
from jax import lax
from jax.experimental import pallas as pl
from jax.experimental.pallas import tpu as pltpu
from jax.sharding import PartitionSpec as P

MESH = pl.DeviceIdType.MESH
F32 = jnp.float32
BF16 = jnp.bfloat16
TILE = 512
STRIP = 256
COLS = 512
VMEM_LIMIT = 63 * 1024 * 1024
KEPT = 18 * 1024 * 1024


def dot_nn(a, b):
    return lax.dot_general(a, b, (((1,), (0,)), ((), ())), preferred_element_type=F32)


def dot_nt(a, b):
    return lax.dot_general(a, b, (((1,), (1,)), ((), ())), preferred_element_type=F32)


def dot_tn(a, b):
    return lax.dot_general(a, b, (((0,), (0,)), ((), ())), preferred_element_type=F32)


def rope(u, cos_t, sin_t):
    half = u.shape[-1] // 2
    first, second = u[:, :half], u[:, half:]
    return jnp.concatenate([first * cos_t - second * sin_t, second * cos_t + first * sin_t], axis=-1)


class Place:
    def __init__(self, size, stride):
        n = size // 2
        group = lax.axis_index('dp')
        z, y = lax.rem(group, 2), lax.rem(lax.div(group, stride), 2)
        self.group_z = group + 1 - 2 * z
        self.group_y = group + stride * (1 - 2 * y)
        self.part = 2 * y + z
        self.part_z, self.part_y, self.part_d = 2 * y + 1 - z, 2 * (1 - y) + z, 3 - self.part
        self.me = lax.axis_index('tp')
        self.core = lax.rem(self.me, 2)
        self.chip = lax.div(self.me, 2)
        self.chip_r = lax.rem(self.chip + 1, n)
        self.chip_l = lax.rem(self.chip + n - 1, n)
        self.chip_o = lax.rem(self.chip + 2, n)
        self.right = self.chip_r * 2 + self.core
        self.left = self.chip_l * 2 + self.core
        self.sib = self.chip * 2 + 1 - self.core


def remote(src, dst, ssem, rsem, to):
    return pltpu.make_async_remote_copy(src_ref=src, dst_ref=dst, send_sem=ssem, recv_sem=rsem,
                                        device_id={'tp': to}, device_id_type=MESH)


def rows_of(start, size):
    return pl.ds(pl.multiple_of(start, min(size, 128)), size)


class Gather:
    def __init__(self, place, at, ssem, rsem):
        self.at, self.p, self.ssem, self.rsem = at, place, ssem, rsem
        p = place
        self.own = [at(p.chip, p.core, h) for h in (0, 1)]
        self.own_all = at(p.chip, p.core, None)
        regions = []
        for core in (p.core, 1 - p.core):
            for chip in (p.chip_l, p.chip_r, p.chip_o):
                regions += [at(chip, core, 0), at(chip, core, 1)]
        self.regions = regions[:6] + [at(p.chip, 1 - p.core, None)] + regions[6:]

    def _send(self, sem, src, dst, rsem, to):
        remote(src, dst, self.ssem.at[sem], self.rsem.at[rsem], to).start()

    def start(self, parts=None, whole=None):
        p = self.p
        parts = self.own if parts is None else parts
        whole = self.own_all if whole is None else whole
        self._send(0, parts[0], self.own[0], 0, p.right)
        self._send(3, parts[1], self.own[1], 3, p.left)
        self._send(1, parts[1], self.own[1], 1, p.right)
        self._send(2, parts[0], self.own[0], 2, p.left)
        self._send(6, whole, self.own_all, 6, p.sib)

    def recv(self, *which):
        for k in which:
            ref = self.regions[k]
            remote(ref, ref, self.ssem.at[k], self.rsem.at[k], self.p.sib).wait_recv()

    def _forward_only(self, *which):
        for k in which:
            self._send(7 + k, self.regions[k], self.regions[k], 7 + k, self.p.sib)

    def _forward(self, *which):
        self.recv(*which)
        self._forward_only(*which)

    def first(self):
        self.recv(0, 3)
        self._send(4, self.regions[0], self.regions[0], 4, self.p.right)
        self._send(5, self.regions[3], self.regions[3], 5, self.p.left)
        self._forward_only(0, 3)

    def second(self):
        self._forward(1, 2)

    def third(self):
        self._forward(4, 5)

    def sibling(self):
        self.recv(6)

    def sibling_near(self):
        self.recv(7, 8, 9, 10)

    def sibling_far(self):
        self.recv(11, 12)

    def finish(self):
        for k in range(13):
            ref = self.own_all if k == 6 else self.own[0]
            remote(ref, ref, self.ssem.at[k], self.rsem.at[k], self.p.sib).wait_send()


class Share:
    def __init__(self, place, full, rows, ssem, rsem):
        self.p, self.full, self.rows, self.ssem, self.rsem = place, full, rows, ssem, rsem

    def at(self, part, h=None, other=False):
        core = 1 - self.p.core if other else self.p.core
        if h is None:
            return self.full.at[:, core, part]
        return self.full.at[:, core, part, pl.ds(h * self.rows, self.rows)]

    def _send(self, k, ref, **to):
        pltpu.make_async_remote_copy(src_ref=ref, dst_ref=ref, send_sem=self.ssem.at[k], recv_sem=self.rsem.at[k],
                                     device_id=to, device_id_type=MESH).start()

    def _recv(self, k, ref):
        remote(ref, ref, self.ssem.at[k], self.rsem.at[k], self.p.sib).wait_recv()

    def start(self):
        p = self.p
        self._send(0, self.at(p.part), dp=p.group_z)
        self._send(1, self.at(p.part), dp=p.group_y)

    def relay(self):
        p = self.p
        self._recv(0, self.at(p.part_z))
        self._send(2, self.at(p.part_z, 0), dp=p.group_y)
        self._recv(1, self.at(p.part_y))
        self._send(3, self.at(p.part_y, 1), dp=p.group_z)
        self._send(4, self.at(p.part_z), tp=p.sib)
        self._send(5, self.at(p.part_y), tp=p.sib)

    def forward(self):
        p = self.p
        for h in (0, 1):
            self._recv(2 + h, self.at(p.part_d, h))
            self._send(6 + h, self.at(p.part_d, h), tp=p.sib)

    def finish(self):
        p = self.p
        for k, h in enumerate((None, None, 0, 0, None, None, 0, 0)):
            ref = self.at(p.part, h)
            remote(ref, ref, self.ssem.at[k], self.rsem.at[k], p.sib).wait_send()
        self._recv(4, self.at(p.part_z, None, True))
        self._recv(5, self.at(p.part_y, None, True))
        self._recv(6, self.at(p.part_d, 0, True))
        self._recv(7, self.at(p.part_d, 1, True))


class Exchange:
    def __init__(self, place, block, src, dst, relays, ssem, rsem):
        self.p, self.block, self.src, self.dst, self.relays, self.ssem, self.rsem = place, block, src, dst, relays, ssem, rsem

    def _send(self, sem, src, dst, rsem, to):
        remote(src, dst, self.ssem.at[sem], self.rsem.at[rsem], to).start()

    def part(self, chip, core):
        return self.src.at[rows_of((chip * 2 + core) * self.block, self.block)]

    def start(self):
        p = self.p
        slot = self.dst.at[p.me]
        self._send(0, self.part(p.chip_o, 0), self.relays.at[0], 0, p.right)
        self._send(1, self.part(p.chip_o, 1), self.relays.at[1], 1, p.left)
        for core in (0, 1):
            self._send(2 + core, self.part(p.chip_r, core), slot, 2 + p.core, p.chip_r * 2 + core)
            self._send(4 + core, self.part(p.chip_l, core), slot, 4 + p.core, p.chip_l * 2 + core)
        self._send(8, self.part(p.chip, 1 - p.core), slot, 8, p.sib)
        self.dst[p.me] = self.src[rows_of(p.me * self.block, self.block), :]

    def _recv(self, k, ref):
        remote(ref, ref, self.ssem.at[k], self.rsem.at[k], self.p.sib).wait_recv()

    def relay(self):
        p = self.p
        self._recv(0, self.relays.at[0])
        self._send(6, self.relays.at[0], self.dst.at[p.left], 6 + p.core, p.chip_r * 2)
        self._recv(1, self.relays.at[1])
        self._send(7, self.relays.at[1], self.dst.at[p.right], 6 + p.core, p.chip_l * 2 + 1)

    def recv(self):
        p = self.p
        for core in (0, 1):
            self._recv(2 + core, self.dst.at[p.chip_l * 2 + core])
            self._recv(4 + core, self.dst.at[p.chip_r * 2 + core])
            self._recv(6 + core, self.dst.at[p.chip_o * 2 + core])
        self._recv(8, self.dst.at[p.sib])

    def finish(self):
        for k in range(9):
            ref = self.relays.at[0]
            remote(ref, ref, self.ssem.at[k], self.rsem.at[k], self.p.sib).wait_send()


class Scatter:
    def __init__(self, place, block, src, d2d, sums, top, bot, from_l, from_r, ssem, rsem):
        self.__dict__.update(locals())
        self.half = block // 2

    def rows(self, chip, core, h=None):
        row = (chip * 2 + core) * self.block
        return rows_of(row, self.block) if h is None else rows_of(row + h * self.half, self.half)

    def _send(self, k, src, dst, to):
        remote(src, dst, self.ssem.at[k], self.rsem.at[k], to).start()

    def _recv(self, k, ref):
        remote(ref, ref, self.ssem.at[k], self.rsem.at[k], self.place.sib).wait_recv()

    def chip_send(self):
        p = self.place
        for k, chip in enumerate((p.chip_o, p.chip_r, p.chip_l, p.chip)):
            self._send(k, self.src.at[self.rows(chip, 1 - p.core)], self.d2d.at[k], p.sib)

    def far(self):
        p, half = self.place, self.half
        self._recv(0, self.d2d.at[0])
        self.sums[0] = self.src[self.rows(p.chip_o, p.core), :] + self.d2d[0]
        self._send(4, self.sums.at[0, pl.ds(0, half)], self.top, p.right)
        self._send(5, self.sums.at[0, pl.ds(half, half)], self.bot, p.left)

    def near_half(self, k, h, chip, extra, dst, sem, to):
        rows = pl.ds(h * self.half, self.half)
        total = self.src[self.rows(chip, self.place.core, h), :] + self.d2d[k, rows, :]
        self.sums[k, rows, :] = total if extra is None else total + extra[...]
        self._send(sem, self.sums.at[k, rows], dst.at[rows], to)

    def near_first(self):
        p = self.place
        self._recv(1, self.d2d.at[1])
        self.near_half(1, 1, p.chip_r, None, self.from_l, 6, p.right)
        self._recv(2, self.d2d.at[2])
        self.near_half(2, 0, p.chip_l, None, self.from_r, 8, p.left)

    def near_second(self):
        p = self.place
        self._recv(4, self.top)
        self.near_half(1, 0, p.chip_r, self.top, self.from_l, 7, p.right)
        self._recv(5, self.bot)
        self.near_half(2, 1, p.chip_l, self.bot, self.from_r, 9, p.left)

    def last(self):
        p, half = self.place, self.half
        self._recv(3, self.d2d.at[3])
        for k, ref, h in ((6, self.from_l, 1), (7, self.from_l, 0), (8, self.from_r, 0), (9, self.from_r, 1)):
            self._recv(k, ref.at[pl.ds(h * half, half)])
        return self.src[self.rows(p.chip, p.core), :] + self.d2d[3] + self.from_l[...] + self.from_r[...]

    def finish(self):
        for k in range(10):
            ref = self.d2d.at[0] if k < 4 else self.top
            remote(ref, ref, self.ssem.at[k], self.rsem.at[k], self.place.sib).wait_send()


def block_kernel(size, stride, norm_hbm, pos_hbm, freq_hbm, x_hbm, dout_hbm, wq_hbm, wk_hbm, wv_hbm, wo_hbm,
                 out_ref, dx_ref, dwo_ref, dwq_ref, dw_ref, act_full, dkv_full, dwv_ref, wo_full, wq_full,
                 norm_ref, pos_ref, freq_ref, x_ref, dout_ref, gain_ref, big, wbuf, wo, wqt, q_ref, k_ref, v_ref, o_ref, dq_ref, dkv_ref, o_all, dq_all,
                 relay_o, relay_q, lse_ref, cos_ref, sin_ref, m_scr, l_scr, acc,
                 d2d, sums, top, bot, from_l, from_r, wide, dw_me, dw_all, lsem, ssem,
                 ss_a, rs_a, ss_d, rs_d, ss_wo, rs_wo, ss_wq, rs_wq, ss_kv, rs_kv, ss_yo, rs_yo, ss_yq, rs_yq,
                 ss_o, rs_o, ss_q, rs_q, ss_r, rs_r, ss_w, rs_w):
    p = Place(size, stride)
    block, width = x_ref.shape
    seq, head = q_ref.shape
    chips = size // 2
    half = block // 2
    parts, part_rows = wo.shape[:2]
    scale = head ** -0.5
    wo_rows = lambda: wo[...].reshape(head, width)

    barrier = pltpu.get_barrier_semaphore()
    peers = [lax.rem(p.me + d, size) for d in range(1, size)]
    for to in [{'tp': peer} for peer in peers] + [{'dp': p.group_z}, {'dp': p.group_y}]:
        pl.semaphore_signal(barrier, inc=1, device_id=to, device_id_type=MESH)

    load_x, load_wq, load_wo, load_dout, *load_kv = [pltpu.make_async_copy(src, dst, lsem.at[i]) for i, (src, dst) in enumerate(
        ((x_hbm, x_ref), (wq_hbm, wbuf.at[0]), (wo_hbm, wo), (dout_hbm, dout_ref), (wk_hbm, wbuf.at[1]), (wv_hbm, wbuf.at[2])))]
    small = [pltpu.make_async_copy(src, dst, ssem.at[i]) for i, (src, dst) in enumerate(
        ((norm_hbm, norm_ref), (pos_hbm, pos_ref), (freq_hbm, freq_ref)))]
    for copy in (load_wq, load_wo, load_x, *small, load_dout, *load_kv):
        copy.start()
    lanes = 128
    groups = [slice(t * lanes, (t + 1) * lanes) for t in range(width // lanes)]
    def weight_at(full):
        quarter = part_rows // 2

        def at(chip, core, h):
            if h is None:
                return full.at[chip, core, p.part]
            return full.at[chip, core, p.part, pl.ds(h * quarter, quarter)]
        return at

    def rows_at(full):
        def at(chip, core, h):
            row = (chip * 2 + core) * block
            return full.at[rows_of(row, block) if h is None else rows_of(row + h * half, half)]
        return at

    def grad_at(chip, core, h):
        return big.at[chip, core] if h is None else big.at[chip, core, pl.ds(h * (parts // 2), parts // 2)]

    act = Gather(p, rows_at(act_full), ss_a, rs_a)
    grad = Gather(p, grad_at, ss_d, rs_d)
    wo_g = Gather(p, weight_at(wo_full), ss_wo, rs_wo)
    wq_g = Gather(p, weight_at(wq_full), ss_wq, rs_wq)
    kv_g = Gather(p, rows_at(dkv_full), ss_kv, rs_kv)
    wo_s = Share(p, wo_full, part_rows // 2, ss_yo, rs_yo)
    wq_s = Share(p, wq_full, part_rows // 2, ss_yq, rs_yq)
    o_x = Exchange(p, block, o_ref, o_all, relay_o, ss_o, rs_o)
    dq_x = Exchange(p, block, dq_ref, dq_all, relay_q, ss_q, rs_q)
    kv_r = Scatter(p, block, dkv_ref, d2d, sums, top, bot, from_l, from_r, ss_r, rs_r)

    def start_weight(g, shard, src, sem, load):
        quarter = part_rows // 2
        g.start([src.at[p.part, pl.ds(h * quarter, quarter)] for h in (0, 1)], src.at[p.part])
        load.wait()
        own = pltpu.make_async_copy(shard.at[p.part], g.own_all, lsem.at[sem])
        own.start()
        return own

    pl.semaphore_wait(barrier, size + 1)
    own_wo = start_weight(wo_g, wo, wo_hbm, 6, load_wo)
    load_wq.wait()

    @pl.loop(0, width // COLS)
    def _(n):
        rows = pl.ds(pl.multiple_of(n * COLS, COLS), COLS)
        flipped = wbuf[0, rows, :].T
        for g in range(parts):
            wqt[g, :, rows] = flipped[g * part_rows:(g + 1) * part_rows, :]
    own_wq = start_weight(wq_g, wqt, wqt, 7, load_x)
    for copy in small:
        copy.wait()
    for t, cols in enumerate(groups):
        gain_ref[:, cols] = 1.0 + norm_ref[t:t + 1, :]

    @pl.loop(0, block // 64)
    def _(n):
        rows = pl.ds(pl.multiple_of(n * 64, 64), 64)
        x_f = x_ref[rows, :].astype(F32)
        inv = lax.rsqrt(jnp.mean(x_f * x_f, axis=-1, keepdims=True) + 1e-6)
        act_full[rows_of(p.me * block + n * 64, 64), :] = (x_f * inv * gain_ref[...]).astype(BF16)

    for g in (wo_g, wq_g):
        g.first()
    act.start()

    @pl.loop(0, seq // lanes)
    def _(n):
        rows = pl.ds(pl.multiple_of(n * lanes, lanes), lanes)
        angle = jnp.broadcast_to(pos_ref[:, rows].astype(F32), (lanes, lanes)).T * freq_ref[...]
        cos_ref[rows, :] = jnp.cos(angle)
        sin_ref[rows, :] = jnp.sin(angle)

    load_dout.wait()
    big[p.chip, p.core] = dout_ref[...]
    for copy in load_kv:
        copy.wait()

    def project(first, second):
        @pl.loop(0, 2)
        def _(n):
            rows = rows_of((first + n * (second - first)) * block, block)
            a = act_full[rows, :]
            cos_t, sin_t = cos_ref[rows, :], sin_ref[rows, :]
            query = dot_nn(a, wbuf[0]).astype(BF16).astype(F32)
            q_ref[rows, :] = (rope(query, cos_t, sin_t) * scale).astype(BF16)
            key = dot_nn(a, wbuf[1]).astype(BF16).astype(F32)
            k_ref[rows, :] = rope(key, cos_t, sin_t).astype(BF16)
            v_ref[rows, :] = dot_nn(a, wbuf[2]).astype(BF16)

    for g, s, own in ((wo_g, wo_s, own_wo), (wq_g, wq_s, own_wq)):
        g.second()
        g.third()
        own.wait()
        s.start()

    act.sibling()
    project(p.me, p.sib)
    act.first()
    grad.start([dout_ref.at[pl.ds(h * (parts // 2), parts // 2)] for h in (0, 1)], dout_ref)
    act.second()
    project(p.left, p.right)
    act.sibling_near()
    project(p.chip_l * 2 + 1 - p.core, p.chip_r * 2 + 1 - p.core)
    act.third()
    act.sibling_far()
    project(p.chip_o * 2 + p.core, p.chip_o * 2 + 1 - p.core)

    row_ids = lax.broadcasted_iota(jnp.int32, (TILE, TILE), 0)
    col_ids = lax.broadcasted_iota(jnp.int32, (TILE, TILE), 1)

    def tile_rows(j):
        return pl.ds(pl.multiple_of(j * TILE, TILE), TILE)

    def lane_groups(v):
        return [v[:, t * lanes:(t + 1) * lanes] for t in range(TILE // lanes)]

    def spread(v):
        return jnp.concatenate([v] * (TILE // lanes), axis=-1)

    diagonal = row_ids >= col_ids

    @pl.loop(0, seq // TILE)
    def _(i):
        rows = tile_rows(i)
        m_scr[...] = jnp.full(m_scr.shape, -1e30, F32)

        def score(j, s):
            dkv_ref[tile_rows(j), :] = s
            m_scr[...] = functools.reduce(jnp.maximum, lane_groups(s), m_scr[...])

        @pl.loop(0, i)
        def _(j):
            score(j, dot_nt(q_ref[rows, :], k_ref[tile_rows(j), :]))

        score(i, jnp.where(diagonal, dot_nt(q_ref[rows, :], k_ref[rows, :]), -1e30))
        m_scr[...] = jnp.broadcast_to(jnp.max(m_scr[...], axis=-1, keepdims=True), m_scr.shape)
        l_scr[...] = jnp.zeros(l_scr.shape, F32)
        acc[...] = jnp.zeros(acc.shape, F32)

        @pl.loop(0, i + 1)
        def _(j):
            prob = jnp.exp(dkv_ref[tile_rows(j), :] - spread(m_scr[...]))
            l_scr[...] = functools.reduce(jnp.add, lane_groups(prob), l_scr[...])
            acc[...] += dot_nn(prob.astype(BF16), v_ref[tile_rows(j), :])

        total = jnp.sum(l_scr[...], axis=-1, keepdims=True)
        lse_ref[rows, :] = m_scr[...] + jnp.log(total)
        o_ref[rows, :] = (acc[...] / total).astype(BF16)

    dkv_ref[...] = jnp.zeros(dkv_ref.shape, F32)

    def backward(first, second, count):
        @pl.loop(0, count)
        def _(n):
            i = first + n * (second - first)
            rows = tile_rows(i)
            do = dot_nt(big[i].reshape(TILE, width), wo_rows()).astype(BF16)
            row_dot = jnp.sum(do.astype(F32) * o_ref[rows, :].astype(F32), axis=-1, keepdims=True)
            m_scr[...] = jnp.broadcast_to(row_dot, m_scr.shape)
            acc[...] = jnp.zeros(acc.shape, F32)
            q = q_ref[rows, :]

            def inner(j, masked):
                cols = tile_rows(j)
                prob = jnp.exp(dot_nt(q, k_ref[cols, :]) - spread(lse_ref[rows, :]))
                if masked:
                    prob = jnp.where(diagonal, prob, 0.0)
                dkv_ref[cols, head:] += dot_tn(prob.astype(BF16), do)
                ds = (prob * (dot_nt(do, v_ref[cols, :]) - spread(m_scr[...]))).astype(BF16)
                dkv_ref[cols, :head] += dot_tn(ds, q)
                acc[...] += dot_nn(ds, k_ref[cols, :])

            @pl.loop(0, i)
            def _(j):
                inner(j, False)
            inner(i, True)

            dq_ref[rows, :] = rope(acc[...] * scale, cos_ref[rows, :], -sin_ref[rows, :]).astype(BF16)

    grad.sibling()
    backward(p.chip, p.chip, 1)
    grad.first()
    o_x.start()
    for s in (wo_s, wq_s):
        s.relay()
    act.finish()

    def strip(n):
        return pl.ds(pl.multiple_of(n * STRIP, STRIP), STRIP)

    @pl.loop(0, width // STRIP)
    def _(i):
        @pl.loop(0, i + 1)
        def _(j):
            upper, lower = act_full[strip(j), strip(i)], act_full[strip(i), strip(j)]
            act_full[strip(i), strip(j)] = upper.T
            act_full[strip(j), strip(i)] = lower.T

    grad.second()
    grad.sibling_near()
    backward(p.chip_l, p.chip_r, 2)
    grad.third()
    grad.sibling_far()
    backward(p.chip_o, p.chip_o, 1)

    kv_r.chip_send()
    o_x.relay()
    kv_r.far()
    kv_r.near_first()
    for s in (wo_s, wq_s):
        s.forward()

    def col_tiles(fn):
        @pl.loop(0, width // COLS)
        def _(n):
            fn(pl.ds(pl.multiple_of(n * COLS, COLS), COLS))

    def big_cols(cols):
        return big[:, :, :, :, cols].reshape(seq, COLS)

    def weight_o(cols):
        dwo_ref[:, cols] = dot_tn(o_ref[...], big_cols(cols))
    col_tiles(weight_o)

    kv_r.near_second()
    dq_x.start()
    grad.finish()
    wo_g.sibling()
    wo_g.sibling_near()
    wo_g.sibling_far()
    wo_s.finish()
    load_wo = pltpu.make_async_copy(wo_full, big, lsem.at[2])
    load_wo.start()

    def weight_q(cols):
        dwq_ref[cols, :] = dot_nn(act_full[cols, :], dq_ref[...])
    col_tiles(weight_q)
    o_x.recv()
    load_wo.wait()

    def finish_out(cols):
        total = dot_nn(jnp.concatenate([o_all[h] for h in range(size)], axis=-1), big_cols(cols))
        out_ref[:, cols] = (x_ref[:, cols].astype(F32) + total).astype(BF16)
    col_tiles(finish_out)

    wq_g.sibling()
    wq_g.sibling_near()
    wq_g.sibling_far()
    wq_s.finish()
    load_wq = pltpu.make_async_copy(wq_full, big, lsem.at[3])
    load_wq.start()

    own = rows_of(p.me * block, block)
    total = kv_r.last()
    dkv_full[own, :head] = rope(total[:, :head], cos_ref[own, :], -sin_ref[own, :]).astype(BF16)
    dkv_full[own, head:] = total[:, head:].astype(BF16)
    dq_x.relay()
    kv_g.start()
    dq_x.recv()
    load_wq.wait()

    def finish_da(cols):
        total = dot_nn(jnp.concatenate([dq_all[h] for h in range(size)], axis=-1), big_cols(cols))
        wide[:, cols] = (total + dot_nt(dkv_full[own, :head], wbuf[1, cols, :])
                         + dot_nt(dkv_full[own, head:], wbuf[2, cols, :]))
    col_tiles(finish_da)
    kv_g.first()

    dw_me[...] = jnp.zeros(dw_me.shape, F32)
    sub = 32

    @pl.loop(0, block // sub)
    def _(n):
        rows = pl.ds(pl.multiple_of(n * sub, sub), sub)
        x_f = x_ref[rows, :].astype(F32)
        inv = lax.rsqrt(jnp.mean(x_f * x_f, axis=-1, keepdims=True) + 1e-6)
        normed = x_f * inv
        da = wide[rows, :]
        dw_me[...] += jnp.sum(da * normed, axis=0, keepdims=True)
        gn = da * gain_ref[...]
        per = part_rows // sub
        dout = dout_ref[n // per, pl.ds(pl.multiple_of(lax.rem(n, per) * sub, sub), sub), :].astype(F32)
        dx_ref[rows, :] = (dout + inv * (gn - normed * jnp.mean(gn * normed, axis=-1, keepdims=True))).astype(BF16)

    for t, cols in enumerate(groups):
        dw_all[p.me, t:t + 1, :] = dw_me[:, cols]
    for d in range(1, size):
        remote(dw_all.at[p.me], dw_all.at[p.me], ss_w.at[d], rs_w.at[d], peers[d - 1]).start()
    kv_g.second()
    kv_g.sibling_near()

    def weight_v(cols):
        dwv_ref[cols, :] = sum(dot_nn(act_full[cols, tokens], dkv_full[tokens, head:])
                               for tokens in (rows_of(chip * TILE, TILE) for chip in (p.chip_l, p.chip_r)))
    col_tiles(weight_v)
    kv_g.third()
    for d in range(1, size):
        source = dw_all.at[lax.rem(p.me + size - d, size)]
        remote(source, source, ss_w.at[d], rs_w.at[d], p.sib).wait_recv()
    dw_ref[...] = jnp.sum(dw_all[...], axis=0)
    kv_g.sibling()
    kv_g.sibling_far()

    for d in range(1, size):
        remote(dw_all.at[0], dw_all.at[0], ss_w.at[d], rs_w.at[d], p.sib).wait_send()
    for g in (wo_g, wq_g, kv_g, kv_r, o_x, dq_x):
        g.finish()


def weight_kernel(chips, out_in, dx_in, dwo_in, dwq_in, dw_in, a_ref, dkv_ref, dwv_in,
                  out_ref, dx_ref, dwo_ref, dwq_ref, dw_ref, dwk_ref, dwv_ref, dwk, dwv, sems):
    head = dwk.shape[1]
    chip = lax.div(lax.axis_index('tp'), 2)
    left_out = [rows_of(c * TILE, TILE) for c in (chip, lax.rem(chip + 2, chips))]
    copies = []

    def put(src, dst):
        copies.append(pltpu.make_async_copy(src, dst, sems.at[len(copies)]))
        copies[-1].start()

    tiles = [pl.ds(row, STRIP) for row in range(0, dwk.shape[0], STRIP)]
    for src, dst in ((out_in, out_ref), (dx_in, dx_ref), (dwo_in, dwo_ref), (dwq_in, dwq_ref), (dw_in, dw_ref)):
        put(src, dst)
    for rows in tiles:
        dwk[rows, :] = dot_nn(a_ref[rows, :], dkv_ref[:, :head])
        put(dwk.at[rows], dwk_ref.at[rows])
        dwv[rows, :] = dwv_in[rows, :] + sum(dot_nn(a_ref[rows, tokens], dkv_ref[tokens, head:]) for tokens in left_out)
        put(dwv.at[rows], dwv_ref.at[rows])
    for copy in copies:
        copy.wait()


def local_block(size, stride, hidden, positions, norm_w, w_query, w_key, w_value, w_out, grad_out):
    _, block, width = hidden.shape
    seq = positions.shape[1]
    head = w_key.shape[1]
    half = head // 2
    chips, parts = size // 2, 4
    part_rows = block // parts
    lanes = 128
    x, dout = hidden[0], grad_out[0].reshape(parts, part_rows, width)
    inv_freq = (10000.0 ** (-2.0 * np.arange(half) / head)).astype(np.float32)[None, :]
    vm = pl.BlockSpec(memory_space=pltpu.VMEM)
    hbm = pl.BlockSpec(memory_space=pl.ANY)
    dma = pltpu.SemaphoreType.DMA
    shape = jax.ShapeDtypeStruct
    V = pltpu.VMEM
    full = (chips, 2, parts, part_rows, width)
    kv = 2 * head
    small = (width // lanes, lanes)

    *results, _, _ = pl.pallas_call(
        functools.partial(block_kernel, size, stride),
        out_shape=[V((block, width), BF16), V((block, width), BF16), V((head, width), F32), V((width, head), F32), V(small, F32),
                   V((seq, width), BF16), V((seq, kv), BF16), V((width, head), F32), shape(full, BF16), shape(full, BF16)],
        in_specs=[hbm] * 9,
        out_specs=[vm] * 8 + [hbm] * 2,
        scratch_shapes=[V(small, F32), V((1, seq), jnp.int32), V((1, half), F32),
                        V((block, width), BF16), V((parts, part_rows, width), BF16), V((1, width), F32),
                        V(full, BF16), V((3, width, head), BF16), V((parts, part_rows, width), BF16),
                        V((parts, part_rows, width), BF16)] + [V((seq, head), BF16)] * 5
        + [V((seq, kv), F32), V((size, block, head), BF16), V((size, block, head), BF16),
           V((2, block, head), BF16), V((2, block, head), BF16), V((seq, 128), F32), V((seq, half), F32), V((seq, half), F32),
           V((TILE, 128), F32), V((TILE, 128), F32), V((TILE, head), F32),
           V((4, block, kv), F32), V((3, block, kv), F32), V((block // 2, kv), F32), V((block // 2, kv), F32),
           V((block, kv), F32), V((block, kv), F32), V((head, width), F32), V((1, width), F32),
           V((size, width // 128, 128), F32), dma((8,)), dma((3,))]
        + [dma((13,))] * 10 + [dma((8,))] * 4 + [dma((9,))] * 4 + [dma((10,))] * 2 + [dma((size,))] * 2,
        compiler_params=pltpu.CompilerParams(collective_id=0, has_side_effects=True, vmem_limit_bytes=VMEM_LIMIT - KEPT),
        name='attention_block',
    )(norm_w.reshape(width // lanes, lanes), positions, inv_freq, x, dout, w_query, w_key, w_value,
      w_out.reshape(parts, part_rows, width))

    out, dx, dwo, dwq, dw, dwk, dwv = pl.pallas_call(
        functools.partial(weight_kernel, chips),
        out_shape=[shape((block, width), BF16)] * 2 + [shape((head, width), F32), shape((width, head), F32), shape(small, F32)]
        + [shape((width, head), F32)] * 2,
        in_specs=[vm] * 8,
        out_specs=[hbm] * 7,
        scratch_shapes=[V((width, head), F32), V((width, head), F32), dma((5 + 2 * (width // STRIP),))],
        compiler_params=pltpu.CompilerParams(vmem_limit_bytes=VMEM_LIMIT - KEPT),
        name='weight_grads',
    )(*[pltpu.with_memory_space_constraint(v, V) for v in results])
    return out[None], dx[None], dwq, dwo, dwk, dwv, dw.reshape(width)


def solution(mesh):
    specs_in = (P('dp', 'tp', None), P('dp', None), P(None), P(None, 'tp'), P(None, None), P(None, None), P('tp', None), P('dp', 'tp', None))
    specs_out = (P('dp', 'tp', None), P('dp', 'tp', None), P('dp', 'tp'), P(('dp', 'tp'), None), P('dp', None), P('dp', None), P('dp'))
    column = [tuple(d.coords) for d in mesh.devices[:, 0]]
    stride = sum(c[1] == column[0][1] for c in column)
    local = functools.partial(local_block, mesh.shape['tp'], stride)
    return jax.shard_map(local, mesh=mesh, in_specs=specs_in, out_specs=specs_out, check_vma=False)
```

```python
import functools

import jax
import jax.numpy as jnp
import numpy as np
from jax import lax
from jax.experimental import pallas as pl
from jax.experimental.pallas import tpu as pltpu
from jax.sharding import PartitionSpec as P

MESH = pl.DeviceIdType.MESH
F32 = jnp.float32
BF16 = jnp.bfloat16
TILE = 512
STRIP = 256
COLS = 512
VMEM_LIMIT = 63 * 1024 * 1024
KEPT = 20 * 1024 * 1024


def dot_nn(a, b):
    return lax.dot_general(a, b, (((1,), (0,)), ((), ())), preferred_element_type=F32)


def dot_nt(a, b):
    return lax.dot_general(a, b, (((1,), (1,)), ((), ())), preferred_element_type=F32)


def dot_tn(a, b):
    return lax.dot_general(a, b, (((0,), (0,)), ((), ())), preferred_element_type=F32)


def rope(u, cos_t, sin_t):
    half = u.shape[-1] // 2
    first, second = u[:, :half], u[:, half:]
    return jnp.concatenate([first * cos_t - second * sin_t, second * cos_t + first * sin_t], axis=-1)


class Place:
    def __init__(self, size, stride):
        n = size // 2
        group = lax.axis_index('dp')
        z, y = lax.rem(group, 2), lax.rem(lax.div(group, stride), 2)
        self.group_z = group + 1 - 2 * z
        self.group_y = group + stride * (1 - 2 * y)
        self.part = 2 * y + z
        self.part_z, self.part_y, self.part_d = 2 * y + 1 - z, 2 * (1 - y) + z, 3 - self.part
        self.me = lax.axis_index('tp')
        self.core = lax.rem(self.me, 2)
        self.chip = lax.div(self.me, 2)
        self.chip_r = lax.rem(self.chip + 1, n)
        self.chip_l = lax.rem(self.chip + n - 1, n)
        self.chip_o = lax.rem(self.chip + 2, n)
        self.right = self.chip_r * 2 + self.core
        self.left = self.chip_l * 2 + self.core
        self.sib = self.chip * 2 + 1 - self.core


def remote(src, dst, ssem, rsem, to):
    return pltpu.make_async_remote_copy(src_ref=src, dst_ref=dst, send_sem=ssem, recv_sem=rsem,
                                        device_id={'tp': to}, device_id_type=MESH)


def rows_of(start, size):
    return pl.ds(pl.multiple_of(start, min(size, 128)), size)


class Gather:
    def __init__(self, place, at, ssem, rsem):
        self.at, self.p, self.ssem, self.rsem = at, place, ssem, rsem
        p = place
        self.own = [at(p.chip, p.core, h) for h in (0, 1)]
        self.own_all = at(p.chip, p.core, None)
        regions = []
        for core in (p.core, 1 - p.core):
            for chip in (p.chip_l, p.chip_r, p.chip_o):
                regions += [at(chip, core, 0), at(chip, core, 1)]
        self.regions = regions[:6] + [at(p.chip, 1 - p.core, None)] + regions[6:]

    def _send(self, sem, src, dst, rsem, to):
        remote(src, dst, self.ssem.at[sem], self.rsem.at[rsem], to).start()

    def start(self, parts=None, whole=None):
        p = self.p
        parts = self.own if parts is None else parts
        whole = self.own_all if whole is None else whole
        self._send(0, parts[0], self.own[0], 0, p.right)
        self._send(3, parts[1], self.own[1], 3, p.left)
        self._send(1, parts[1], self.own[1], 1, p.right)
        self._send(2, parts[0], self.own[0], 2, p.left)
        self._send(6, whole, self.own_all, 6, p.sib)

    def recv(self, *which):
        for k in which:
            ref = self.regions[k]
            remote(ref, ref, self.ssem.at[k], self.rsem.at[k], self.p.sib).wait_recv()

    def _forward_only(self, *which):
        for k in which:
            self._send(7 + k, self.regions[k], self.regions[k], 7 + k, self.p.sib)

    def _forward(self, *which):
        for k in which:
            self.recv(k)
            self._forward_only(k)

    def first(self):
        self.recv(0, 3)
        self._send(4, self.regions[0], self.regions[0], 4, self.p.right)
        self._send(5, self.regions[3], self.regions[3], 5, self.p.left)
        self._forward_only(0, 3)

    def second(self):
        self._forward(1, 2)

    def third(self):
        self._forward(4, 5)

    def sibling(self):
        self.recv(6)

    def sibling_near(self):
        self.recv(7, 8, 9, 10)

    def sibling_far(self):
        self.recv(11, 12)

    def finish(self):
        for k in range(13):
            ref = self.own_all if k == 6 else self.own[0]
            remote(ref, ref, self.ssem.at[k], self.rsem.at[k], self.p.sib).wait_send()


class Share:
    def __init__(self, place, full, rows, ssem, rsem):
        self.p, self.full, self.rows, self.ssem, self.rsem = place, full, rows, ssem, rsem

    def at(self, part, h=None, other=False):
        core = 1 - self.p.core if other else self.p.core
        if h is None:
            return self.full.at[:, core, part]
        return self.full.at[:, core, part, pl.ds(h * self.rows, self.rows)]

    def _send(self, k, ref, **to):
        pltpu.make_async_remote_copy(src_ref=ref, dst_ref=ref, send_sem=self.ssem.at[k], recv_sem=self.rsem.at[k],
                                     device_id=to, device_id_type=MESH).start()

    def _recv(self, k, ref):
        remote(ref, ref, self.ssem.at[k], self.rsem.at[k], self.p.sib).wait_recv()

    def start(self):
        p = self.p
        self._send(0, self.at(p.part), dp=p.group_z)
        self._send(1, self.at(p.part), dp=p.group_y)

    def relay(self):
        p = self.p
        self._recv(0, self.at(p.part_z))
        self._send(2, self.at(p.part_z, 0), dp=p.group_y)
        self._recv(1, self.at(p.part_y))
        self._send(3, self.at(p.part_y, 1), dp=p.group_z)
        self._send(4, self.at(p.part_z), tp=p.sib)
        self._send(5, self.at(p.part_y), tp=p.sib)

    def forward(self):
        p = self.p
        for h in (0, 1):
            self._recv(2 + h, self.at(p.part_d, h))
            self._send(6 + h, self.at(p.part_d, h), tp=p.sib)

    def finish(self):
        p = self.p
        for k, h in enumerate((None, None, 0, 0, None, None, 0, 0)):
            ref = self.at(p.part, h)
            remote(ref, ref, self.ssem.at[k], self.rsem.at[k], p.sib).wait_send()
        self._recv(4, self.at(p.part_z, None, True))
        self._recv(5, self.at(p.part_y, None, True))
        self._recv(6, self.at(p.part_d, 0, True))
        self._recv(7, self.at(p.part_d, 1, True))


class Exchange:
    def __init__(self, place, block, src, dst, relays, ssem, rsem):
        self.p, self.block, self.src, self.dst, self.relays, self.ssem, self.rsem = place, block, src, dst, relays, ssem, rsem

    def _send(self, sem, src, dst, rsem, to):
        remote(src, dst, self.ssem.at[sem], self.rsem.at[rsem], to).start()

    def part(self, chip, core):
        return self.src.at[rows_of((chip * 2 + core) * self.block, self.block)]

    def start(self):
        p = self.p
        slot = self.dst.at[p.me]
        self._send(0, self.part(p.chip_o, 0), self.relays.at[0], 0, p.right)
        self._send(1, self.part(p.chip_o, 1), self.relays.at[1], 1, p.left)
        for core in (0, 1):
            self._send(2 + core, self.part(p.chip_r, core), slot, 2 + p.core, p.chip_r * 2 + core)
            self._send(4 + core, self.part(p.chip_l, core), slot, 4 + p.core, p.chip_l * 2 + core)
        self._send(8, self.part(p.chip, 1 - p.core), slot, 8, p.sib)
        self.dst[p.me] = self.src[rows_of(p.me * self.block, self.block), :]

    def _recv(self, k, ref):
        remote(ref, ref, self.ssem.at[k], self.rsem.at[k], self.p.sib).wait_recv()

    def relay(self):
        p = self.p
        self._recv(0, self.relays.at[0])
        self._send(6, self.relays.at[0], self.dst.at[p.left], 6 + p.core, p.chip_r * 2)
        self._recv(1, self.relays.at[1])
        self._send(7, self.relays.at[1], self.dst.at[p.right], 6 + p.core, p.chip_l * 2 + 1)

    def recv(self):
        p = self.p
        for core in (0, 1):
            self._recv(2 + core, self.dst.at[p.chip_l * 2 + core])
            self._recv(4 + core, self.dst.at[p.chip_r * 2 + core])
            self._recv(6 + core, self.dst.at[p.chip_o * 2 + core])
        self._recv(8, self.dst.at[p.sib])

    def finish(self):
        for k in range(9):
            ref = self.relays.at[0]
            remote(ref, ref, self.ssem.at[k], self.rsem.at[k], self.p.sib).wait_send()


class Scatter:
    def __init__(self, place, block, src, d2d, sums, top, bot, from_l, from_r, ssem, rsem):
        self.__dict__.update(locals())
        self.half = block // 2

    def rows(self, chip, core, h=None):
        row = (chip * 2 + core) * self.block
        return rows_of(row, self.block) if h is None else rows_of(row + h * self.half, self.half)

    def _send(self, k, src, dst, to):
        remote(src, dst, self.ssem.at[k], self.rsem.at[k], to).start()

    def _recv(self, k, ref):
        remote(ref, ref, self.ssem.at[k], self.rsem.at[k], self.place.sib).wait_recv()

    def chip_send(self):
        p = self.place
        for k, chip in enumerate((p.chip_o, p.chip_r, p.chip_l, p.chip)):
            self._send(k, self.src.at[self.rows(chip, 1 - p.core)], self.d2d.at[k], p.sib)

    def far(self):
        p, half = self.place, self.half
        self._recv(0, self.d2d.at[0])
        self.sums[0] = self.src[self.rows(p.chip_o, p.core), :] + self.d2d[0]
        self._send(4, self.sums.at[0, pl.ds(0, half)], self.top, p.right)
        self._send(5, self.sums.at[0, pl.ds(half, half)], self.bot, p.left)

    def near_half(self, k, h, chip, extra, dst, sem, to):
        rows = pl.ds(h * self.half, self.half)
        total = self.src[self.rows(chip, self.place.core, h), :] + self.d2d[k, rows, :]
        self.sums[k, rows, :] = total if extra is None else total + extra[...]
        self._send(sem, self.sums.at[k, rows], dst.at[rows], to)

    def near_first(self):
        p = self.place
        self._recv(1, self.d2d.at[1])
        self.near_half(1, 1, p.chip_r, None, self.from_l, 6, p.right)
        self._recv(2, self.d2d.at[2])
        self.near_half(2, 0, p.chip_l, None, self.from_r, 8, p.left)

    def near_second(self):
        p = self.place
        self._recv(4, self.top)
        self.near_half(1, 0, p.chip_r, self.top, self.from_l, 7, p.right)
        self._recv(5, self.bot)
        self.near_half(2, 1, p.chip_l, self.bot, self.from_r, 9, p.left)

    def last(self):
        p, half = self.place, self.half
        self._recv(3, self.d2d.at[3])
        for k, ref, h in ((6, self.from_l, 1), (7, self.from_l, 0), (8, self.from_r, 0), (9, self.from_r, 1)):
            self._recv(k, ref.at[pl.ds(h * half, half)])
        return self.src[self.rows(p.chip, p.core), :] + self.d2d[3] + self.from_l[...] + self.from_r[...]

    def finish(self):
        for k in range(10):
            ref = self.d2d.at[0] if k < 4 else self.top
            remote(ref, ref, self.ssem.at[k], self.rsem.at[k], self.place.sib).wait_send()


def block_kernel(size, stride, norm_hbm, pos_hbm, freq_hbm, x_hbm, dout_hbm, wq_hbm, wk_hbm, wv_hbm, wo_hbm,
                 out_ref, dx_ref, dwo_ref, dwq_ref, dw_ref, act_full, dkv_full, dwkv_ref, wo_full, wq_full,
                 norm_ref, pos_ref, freq_ref, x_ref, dout_ref, gain_ref, big, wbuf, wo, wqt, q_ref, k_ref, v_ref, o_ref, dq_ref, dkv_ref, o_all, dq_all,
                 relay_o, relay_q, lse_ref, cos_ref, sin_ref, m_scr, l_scr, acc,
                 d2d, sums, top, bot, from_l, from_r, wide, dw_me, dw_all, lsem, ssem,
                 ss_a, rs_a, ss_d, rs_d, ss_wo, rs_wo, ss_wq, rs_wq, ss_kv, rs_kv, ss_yo, rs_yo, ss_yq, rs_yq,
                 ss_o, rs_o, ss_q, rs_q, ss_r, rs_r, ss_w, rs_w):
    p = Place(size, stride)
    block, width = x_ref.shape
    seq, head = q_ref.shape
    chips = size // 2
    half = block // 2
    parts, part_rows = wo.shape[:2]
    scale = head ** -0.5
    wo_rows = lambda: wo[...].reshape(head, width)

    barrier = pltpu.get_barrier_semaphore()
    peers = [lax.rem(p.me + d, size) for d in range(1, size)]
    for to in [{'tp': peer} for peer in peers] + [{'dp': p.group_z}, {'dp': p.group_y}]:
        pl.semaphore_signal(barrier, inc=1, device_id=to, device_id_type=MESH)

    load_x, load_wq, load_wo, load_dout, *load_kv = [pltpu.make_async_copy(src, dst, lsem.at[i]) for i, (src, dst) in enumerate(
        ((x_hbm, x_ref), (wq_hbm, wbuf.at[0]), (wo_hbm, wo), (dout_hbm, dout_ref), (wk_hbm, wbuf.at[1]), (wv_hbm, wbuf.at[2])))]
    small = [pltpu.make_async_copy(src, dst, ssem.at[i]) for i, (src, dst) in enumerate(
        ((norm_hbm, norm_ref), (pos_hbm, pos_ref), (freq_hbm, freq_ref)))]
    for copy in (load_wq, load_wo, load_x, *small, load_dout, *load_kv):
        copy.start()
    lanes = 128
    groups = [slice(t * lanes, (t + 1) * lanes) for t in range(width // lanes)]
    def weight_at(full):
        quarter = part_rows // 2

        def at(chip, core, h):
            if h is None:
                return full.at[chip, core, p.part]
            return full.at[chip, core, p.part, pl.ds(h * quarter, quarter)]
        return at

    def rows_at(full):
        def at(chip, core, h):
            row = (chip * 2 + core) * block
            return full.at[rows_of(row, block) if h is None else rows_of(row + h * half, half)]
        return at

    def grad_at(chip, core, h):
        return big.at[chip, core] if h is None else big.at[chip, core, pl.ds(h * (parts // 2), parts // 2)]

    act = Gather(p, rows_at(act_full), ss_a, rs_a)
    grad = Gather(p, grad_at, ss_d, rs_d)
    wo_g = Gather(p, weight_at(wo_full), ss_wo, rs_wo)
    wq_g = Gather(p, weight_at(wq_full), ss_wq, rs_wq)
    kv_g = Gather(p, rows_at(dkv_full), ss_kv, rs_kv)
    wo_s = Share(p, wo_full, part_rows // 2, ss_yo, rs_yo)
    wq_s = Share(p, wq_full, part_rows // 2, ss_yq, rs_yq)
    o_x = Exchange(p, block, o_ref, o_all, relay_o, ss_o, rs_o)
    dq_x = Exchange(p, block, dq_ref, dq_all, relay_q, ss_q, rs_q)
    kv_r = Scatter(p, block, dkv_ref, d2d, sums, top, bot, from_l, from_r, ss_r, rs_r)

    def start_weight(g, shard, src, sem, load):
        quarter = part_rows // 2
        g.start([src.at[p.part, pl.ds(h * quarter, quarter)] for h in (0, 1)], src.at[p.part])
        load.wait()
        own = pltpu.make_async_copy(shard.at[p.part], g.own_all, lsem.at[sem])
        own.start()
        return own

    pl.semaphore_wait(barrier, size + 1)
    own_wo = start_weight(wo_g, wo, wo_hbm, 6, load_wo)
    load_wq.wait()

    @pl.loop(0, width // COLS)
    def _(n):
        rows = pl.ds(pl.multiple_of(n * COLS, COLS), COLS)
        flipped = wbuf[0, rows, :].T
        for g in range(parts):
            wqt[g, :, rows] = flipped[g * part_rows:(g + 1) * part_rows, :]
    own_wq = start_weight(wq_g, wqt, wqt, 7, load_x)
    for copy in small:
        copy.wait()
    for t, cols in enumerate(groups):
        gain_ref[:, cols] = 1.0 + norm_ref[t:t + 1, :]

    @pl.loop(0, block // 64)
    def _(n):
        rows = pl.ds(pl.multiple_of(n * 64, 64), 64)
        x_f = x_ref[rows, :].astype(F32)
        inv = lax.rsqrt(jnp.mean(x_f * x_f, axis=-1, keepdims=True) + 1e-6)
        act_full[rows_of(p.me * block + n * 64, 64), :] = (x_f * inv * gain_ref[...]).astype(BF16)

    for g in (wo_g, wq_g):
        g.first()
    act.start()

    @pl.loop(0, seq // lanes)
    def _(n):
        rows = pl.ds(pl.multiple_of(n * lanes, lanes), lanes)
        angle = jnp.broadcast_to(pos_ref[:, rows].astype(F32), (lanes, lanes)).T * freq_ref[...]
        cos_ref[rows, :] = jnp.cos(angle)
        sin_ref[rows, :] = jnp.sin(angle)

    load_dout.wait()
    big[p.chip, p.core] = dout_ref[...]
    for copy in load_kv:
        copy.wait()

    def project(first, second):
        @pl.loop(0, 2)
        def _(n):
            rows = rows_of((first + n * (second - first)) * block, block)
            a = act_full[rows, :]
            cos_t, sin_t = cos_ref[rows, :], sin_ref[rows, :]
            query = dot_nn(a, wbuf[0]).astype(BF16).astype(F32)
            q_ref[rows, :] = (rope(query, cos_t, sin_t) * scale).astype(BF16)
            key = dot_nn(a, wbuf[1]).astype(BF16).astype(F32)
            k_ref[rows, :] = rope(key, cos_t, sin_t).astype(BF16)
            v_ref[rows, :] = dot_nn(a, wbuf[2]).astype(BF16)

    for g, s, own in ((wo_g, wo_s, own_wo), (wq_g, wq_s, own_wq)):
        g.second()
        g.third()
        own.wait()
        s.start()

    act.sibling()
    project(p.me, p.sib)
    act.first()
    grad.start([dout_ref.at[pl.ds(h * (parts // 2), parts // 2)] for h in (0, 1)], dout_ref)
    act.second()
    project(p.left, p.right)
    act.sibling_near()
    project(p.chip_l * 2 + 1 - p.core, p.chip_r * 2 + 1 - p.core)
    act.third()
    act.sibling_far()
    project(p.chip_o * 2 + p.core, p.chip_o * 2 + 1 - p.core)

    row_ids = lax.broadcasted_iota(jnp.int32, (TILE, TILE), 0)
    col_ids = lax.broadcasted_iota(jnp.int32, (TILE, TILE), 1)

    def tile_rows(j):
        return pl.ds(pl.multiple_of(j * TILE, TILE), TILE)

    def lane_groups(v):
        return [v[:, t * lanes:(t + 1) * lanes] for t in range(TILE // lanes)]

    def spread(v):
        return jnp.concatenate([v] * (TILE // lanes), axis=-1)

    diagonal = row_ids >= col_ids

    @pl.loop(0, seq // TILE)
    def _(i):
        rows = tile_rows(i)
        m_scr[...] = jnp.full(m_scr.shape, -1e30, F32)

        def score(j, s):
            dkv_ref[tile_rows(j), :] = s
            m_scr[...] = functools.reduce(jnp.maximum, lane_groups(s), m_scr[...])

        @pl.loop(0, i)
        def _(j):
            score(j, dot_nt(q_ref[rows, :], k_ref[tile_rows(j), :]))

        score(i, jnp.where(diagonal, dot_nt(q_ref[rows, :], k_ref[rows, :]), -1e30))
        m_scr[...] = jnp.broadcast_to(jnp.max(m_scr[...], axis=-1, keepdims=True), m_scr.shape)
        l_scr[...] = jnp.zeros(l_scr.shape, F32)
        acc[...] = jnp.zeros(acc.shape, F32)

        @pl.loop(0, i + 1)
        def _(j):
            prob = jnp.exp(dkv_ref[tile_rows(j), :] - spread(m_scr[...]))
            l_scr[...] = functools.reduce(jnp.add, lane_groups(prob), l_scr[...])
            acc[...] += dot_nn(prob.astype(BF16), v_ref[tile_rows(j), :])

        total = jnp.sum(l_scr[...], axis=-1, keepdims=True)
        lse_ref[rows, :] = m_scr[...] + jnp.log(total)
        o_ref[rows, :] = (acc[...] / total).astype(BF16)

    dkv_ref[...] = jnp.zeros(dkv_ref.shape, F32)

    def backward(first, second, count):
        @pl.loop(0, count)
        def _(n):
            i = first + n * (second - first)
            rows = tile_rows(i)
            do = dot_nt(big[i].reshape(TILE, width), wo_rows()).astype(BF16)
            row_dot = jnp.sum(do.astype(F32) * o_ref[rows, :].astype(F32), axis=-1, keepdims=True)
            m_scr[...] = jnp.broadcast_to(row_dot, m_scr.shape)
            acc[...] = jnp.zeros(acc.shape, F32)
            q = q_ref[rows, :]

            def inner(j, masked):
                cols = tile_rows(j)
                prob = jnp.exp(dot_nt(q, k_ref[cols, :]) - spread(lse_ref[rows, :]))
                if masked:
                    prob = jnp.where(diagonal, prob, 0.0)
                dkv_ref[cols, head:] += dot_tn(prob.astype(BF16), do)
                ds = (prob * (dot_nt(do, v_ref[cols, :]) - spread(m_scr[...]))).astype(BF16)
                dkv_ref[cols, :head] += dot_tn(ds, q)
                acc[...] += dot_nn(ds, k_ref[cols, :])

            @pl.loop(0, i)
            def _(j):
                inner(j, False)
            inner(i, True)

            dq_ref[rows, :] = rope(acc[...] * scale, cos_ref[rows, :], -sin_ref[rows, :]).astype(BF16)

    grad.sibling()
    backward(p.chip, p.chip, 1)
    grad.first()
    o_x.start()
    for s in (wo_s, wq_s):
        s.relay()
    act.finish()

    def strip(n):
        return pl.ds(pl.multiple_of(n * STRIP, STRIP), STRIP)

    @pl.loop(0, width // STRIP)
    def _(i):
        @pl.loop(0, i + 1)
        def _(j):
            upper, lower = act_full[strip(j), strip(i)], act_full[strip(i), strip(j)]
            act_full[strip(i), strip(j)] = upper.T
            act_full[strip(j), strip(i)] = lower.T

    grad.second()
    grad.sibling_near()
    backward(p.chip_l, p.chip_r, 2)
    grad.third()
    grad.sibling_far()
    backward(p.chip_o, p.chip_o, 1)

    kv_r.chip_send()
    o_x.relay()
    kv_r.far()
    kv_r.near_first()
    for s in (wo_s, wq_s):
        s.forward()

    def col_tiles(fn):
        @pl.loop(0, width // COLS)
        def _(n):
            fn(pl.ds(pl.multiple_of(n * COLS, COLS), COLS))

    def big_cols(cols):
        return big[:, :, :, :, cols].reshape(seq, COLS)

    def weight_o(cols):
        dwo_ref[:, cols] = dot_tn(o_ref[...], big_cols(cols))
    col_tiles(weight_o)

    kv_r.near_second()
    dq_x.start()
    grad.finish()
    wo_g.sibling()
    wo_g.sibling_near()
    wo_g.sibling_far()
    wo_s.finish()
    load_wo = pltpu.make_async_copy(wo_full, big, lsem.at[2])
    load_wo.start()

    def weight_q(cols):
        dwq_ref[cols, :] = dot_nn(act_full[cols, :], dq_ref[...])
    col_tiles(weight_q)
    o_x.recv()
    load_wo.wait()

    def finish_out(cols):
        total = dot_nn(jnp.concatenate([o_all[h] for h in range(size)], axis=-1), big_cols(cols))
        out_ref[:, cols] = (x_ref[:, cols].astype(F32) + total).astype(BF16)
    col_tiles(finish_out)

    wq_g.sibling()
    wq_g.sibling_near()
    wq_g.sibling_far()
    wq_s.finish()
    load_wq = pltpu.make_async_copy(wq_full, big, lsem.at[3])
    load_wq.start()

    own = rows_of(p.me * block, block)
    total = kv_r.last()
    dkv_full[own, :head] = rope(total[:, :head], cos_ref[own, :], -sin_ref[own, :]).astype(BF16)
    dkv_full[own, head:] = total[:, head:].astype(BF16)
    dq_x.relay()
    kv_g.start()
    dq_x.recv()
    load_wq.wait()

    def finish_da(cols):
        total = dot_nn(jnp.concatenate([dq_all[h] for h in range(size)], axis=-1), big_cols(cols))
        wide[:, cols] = (total + dot_nt(dkv_full[own, :head], wbuf[1, cols, :])
                         + dot_nt(dkv_full[own, head:], wbuf[2, cols, :]))
    col_tiles(finish_da)
    kv_g.first()

    dw_me[...] = jnp.zeros(dw_me.shape, F32)
    sub = 32

    @pl.loop(0, block // sub)
    def _(n):
        rows = pl.ds(pl.multiple_of(n * sub, sub), sub)
        x_f = x_ref[rows, :].astype(F32)
        inv = lax.rsqrt(jnp.mean(x_f * x_f, axis=-1, keepdims=True) + 1e-6)
        normed = x_f * inv
        da = wide[rows, :]
        dw_me[...] += jnp.sum(da * normed, axis=0, keepdims=True)
        gn = da * gain_ref[...]
        per = part_rows // sub
        dout = dout_ref[n // per, pl.ds(pl.multiple_of(lax.rem(n, per) * sub, sub), sub), :].astype(F32)
        dx_ref[rows, :] = (dout + inv * (gn - normed * jnp.mean(gn * normed, axis=-1, keepdims=True))).astype(BF16)

    for t, cols in enumerate(groups):
        dw_all[p.me, t:t + 1, :] = dw_me[:, cols]
    for d in range(1, size):
        remote(dw_all.at[p.me], dw_all.at[p.me], ss_w.at[d], rs_w.at[d], peers[d - 1]).start()
    kv_g.second()
    kv_g.sibling_near()

    def weight_kv(cols):
        dwkv_ref[cols, :] = sum(dot_nn(act_full[cols, tokens], dkv_full[tokens, :])
                                for tokens in (rows_of(chip * TILE, TILE) for chip in (p.chip_l, p.chip_r)))
    col_tiles(weight_kv)
    kv_g.third()
    for d in range(1, size):
        source = dw_all.at[lax.rem(p.me + size - d, size)]
        remote(source, source, ss_w.at[d], rs_w.at[d], p.sib).wait_recv()
    dw_ref[...] = jnp.sum(dw_all[...], axis=0)
    kv_g.sibling()
    kv_g.sibling_far()

    for d in range(1, size):
        remote(dw_all.at[0], dw_all.at[0], ss_w.at[d], rs_w.at[d], p.sib).wait_send()
    for g in (wo_g, wq_g, kv_g, kv_r, o_x, dq_x):
        g.finish()


def weight_kernel(chips, out_in, dx_in, dwo_in, dwq_in, dw_in, a_ref, dkv_ref, dwkv_in,
                  out_ref, dx_ref, dwo_ref, dwq_ref, dw_ref, dwk_ref, dwv_ref, dwk, dwv, sems):
    head = dwk.shape[1]
    chip = lax.div(lax.axis_index('tp'), 2)
    left_out = [rows_of(c * TILE, TILE) for c in (chip, lax.rem(chip + 2, chips))]
    copies = []

    def put(src, dst):
        copies.append(pltpu.make_async_copy(src, dst, sems.at[len(copies)]))
        copies[-1].start()

    tiles = [pl.ds(row, STRIP) for row in range(0, dwk.shape[0], STRIP)]
    for src, dst in ((out_in, out_ref), (dx_in, dx_ref), (dwo_in, dwo_ref), (dwq_in, dwq_ref), (dw_in, dw_ref)):
        put(src, dst)
    for rows in tiles:
        dwk[rows, :] = dwkv_in[rows, :head] + sum(dot_nn(a_ref[rows, tokens], dkv_ref[tokens, :head]) for tokens in left_out)
        put(dwk.at[rows], dwk_ref.at[rows])
        dwv[rows, :] = dwkv_in[rows, head:] + sum(dot_nn(a_ref[rows, tokens], dkv_ref[tokens, head:]) for tokens in left_out)
        put(dwv.at[rows], dwv_ref.at[rows])
    for copy in copies:
        copy.wait()


def local_block(size, stride, hidden, positions, norm_w, w_query, w_key, w_value, w_out, grad_out):
    _, block, width = hidden.shape
    seq = positions.shape[1]
    head = w_key.shape[1]
    half = head // 2
    chips, parts = size // 2, 4
    part_rows = block // parts
    lanes = 128
    x, dout = hidden[0], grad_out[0].reshape(parts, part_rows, width)
    inv_freq = (10000.0 ** (-2.0 * np.arange(half) / head)).astype(np.float32)[None, :]
    vm = pl.BlockSpec(memory_space=pltpu.VMEM)
    hbm = pl.BlockSpec(memory_space=pl.ANY)
    dma = pltpu.SemaphoreType.DMA
    shape = jax.ShapeDtypeStruct
    V = pltpu.VMEM
    full = (chips, 2, parts, part_rows, width)
    kv = 2 * head
    small = (width // lanes, lanes)

    *results, _, _ = pl.pallas_call(
        functools.partial(block_kernel, size, stride),
        out_shape=[V((block, width), BF16), V((block, width), BF16), V((head, width), F32), V((width, head), F32), V(small, F32),
                   V((seq, width), BF16), V((seq, kv), BF16), V((width, kv), F32), shape(full, BF16), shape(full, BF16)],
        in_specs=[hbm] * 9,
        out_specs=[vm] * 8 + [hbm] * 2,
        scratch_shapes=[V(small, F32), V((1, seq), jnp.int32), V((1, half), F32),
                        V((block, width), BF16), V((parts, part_rows, width), BF16), V((1, width), F32),
                        V(full, BF16), V((3, width, head), BF16), V((parts, part_rows, width), BF16),
                        V((parts, part_rows, width), BF16)] + [V((seq, head), BF16)] * 5
        + [V((seq, kv), F32), V((size, block, head), BF16), V((size, block, head), BF16),
           V((2, block, head), BF16), V((2, block, head), BF16), V((seq, 128), F32), V((seq, half), F32), V((seq, half), F32),
           V((TILE, 128), F32), V((TILE, 128), F32), V((TILE, head), F32),
           V((4, block, kv), F32), V((3, block, kv), F32), V((block // 2, kv), F32), V((block // 2, kv), F32),
           V((block, kv), F32), V((block, kv), F32), V((head, width), F32), V((1, width), F32),
           V((size, width // 128, 128), F32), dma((8,)), dma((3,))]
        + [dma((13,))] * 10 + [dma((8,))] * 4 + [dma((9,))] * 4 + [dma((10,))] * 2 + [dma((size,))] * 2,
        compiler_params=pltpu.CompilerParams(collective_id=0, has_side_effects=True, vmem_limit_bytes=VMEM_LIMIT - KEPT),
        name='attention_block',
    )(norm_w.reshape(width // lanes, lanes), positions, inv_freq, x, dout, w_query, w_key, w_value,
      w_out.reshape(parts, part_rows, width))

    out, dx, dwo, dwq, dw, dwk, dwv = pl.pallas_call(
        functools.partial(weight_kernel, chips),
        out_shape=[shape((block, width), BF16)] * 2 + [shape((head, width), F32), shape((width, head), F32), shape(small, F32)]
        + [shape((width, head), F32)] * 2,
        in_specs=[vm] * 8,
        out_specs=[hbm] * 7,
        scratch_shapes=[V((width, head), F32), V((width, head), F32), dma((5 + 2 * (width // STRIP),))],
        compiler_params=pltpu.CompilerParams(vmem_limit_bytes=VMEM_LIMIT - KEPT),
        name='weight_grads',
    )(*[pltpu.with_memory_space_constraint(v, V) for v in results])
    return out[None], dx[None], dwq, dwo, dwk, dwv, dw.reshape(width)


def solution(mesh):
    specs_in = (P('dp', 'tp', None), P('dp', None), P(None), P(None, 'tp'), P(None, None), P(None, None), P('tp', None), P('dp', 'tp', None))
    specs_out = (P('dp', 'tp', None), P('dp', 'tp', None), P('dp', 'tp'), P(('dp', 'tp'), None), P('dp', None), P('dp', None), P('dp'))
    column = [tuple(d.coords) for d in mesh.devices[:, 0]]
    stride = sum(c[1] == column[0][1] for c in column)
    local = functools.partial(local_block, mesh.shape['tp'], stride)
    return jax.shard_map(local, mesh=mesh, in_specs=specs_in, out_specs=specs_out, check_vma=False)
```
